32 devices in a mesh: rep: 4 (over y, x), shard: 4 (over z), tp: 2 (over core).
Axes of the slice: x: 2, y: 2, z: 4, core: 2. Of those that a mesh axis runs over, the one named last changes fastest.
Arguments:
- x_in: bfloat16 [4, 1536, 1536], P('rep', 'shard'), may hold values from -6 to 6
- query_key_value_weight: bfloat16 [2, 1536, 2048], P(None, 'shard', 'tp'), may hold values from -0.15625 to 0.15625
- qkv_bias: bfloat16 [2, 2048], P(None, 'tp'), may hold values from -3 to 3
- output_weight: bfloat16 [2, 1536, 1536], P(None, 'shard', 'tp'), may hold values from -0.875 to 0.875
- feedforward_entry_matrix: bfloat16 [2, 1536, 2, 8960], P(None, 'shard', None, 'tp'), may hold values from -0.15625 to 0.15625
- down_weight: bfloat16 [2, 1536, 8960], P(None, 'shard', 'tp'), may hold values from -0.125 to 0.125
- norm_gains: bfloat16 [2, 2, 1536], replicated, may hold values from 0.5 to 1.5
- piece_starts: int32 [4, 2], P('rep'), may hold values from 0 to 1280, as said below
- seq_lengths: int32 [4], P('rep'), may hold values from 1 to 1536, 4608 in all
- grad_out: bfloat16 [4, 1536, 1536], P('rep', 'shard'), may hold values from -6 to 6
Outputs:
- out_act: bfloat16 [4, 1536, 1536], P('rep', 'shard')
- grad_input: float32 [4, 1536, 1536], P('rep', 'shard')
- grad_qkv: float32 [2, 1536, 2048], P(None, 'shard', 'tp')
- grad_bias: float32 [2, 2048], P(None, 'tp')
- grad_out_proj: float32 [2, 1536, 1536], P(None, 'shard', 'tp')
- grad_gate_up: float32 [2, 1536, 2, 8960], P(None, 'shard', None, 'tp')
- grad_down: float32 [2, 1536, 8960], P(None, 'shard', 'tp')
- grad_gains: float32 [2, 2, 1536], replicated
The draws below stay inside these ranges and needn't reach their ends.
Inputs may be any that keep to these rules, and one draw needn't show every extreme that they name: `piece_starts`: piece k of a sequence starts between k * 768 and (k + 1) * 768 - 256, so pieces never intersect.
All inputs are finite; a program needn't handle non-finite values. No bound on the sum of `seq_lengths` on one device may be relied on, other than what follows from the above.
Results may differ from the reference program's by a relative error of at most 0.017.
Values may be sent and summed in bfloat16 or wider, within the bound.
A program may use at most 512 MiB of HBM per device.

```python
import math
import jax
import jax.numpy as jnp
import numpy as np
from jax import lax

D = 1536
QUERY_HEADS = 12
KEY_VALUE_HEADS = 2
HEAD_SIZE = 128
FF = 8960
LAYERS = 2
SEQUENCE_LENGTH = 1536
PIECE = 256
PIECES = 2
SEQUENCE_TOTAL = 4
QKVW = 2048


def draw_piece_starts(key, part):
    half = SEQUENCE_LENGTH // PIECES
    offsets = jax.random.randint(key, (SEQUENCE_TOTAL, PIECES), 0, half - PIECE + 1).astype(jnp.int32)
    offsets = offsets.at[0, 0].set(0).at[0, PIECES - 1].set(half - PIECE)
    return (jnp.arange(PIECES, dtype=jnp.int32)[None, :] * half + offsets).astype(jnp.int32)


def levels(key, extent, split, low, largest):
    gain = 1.0
    for position, blocks in split:
        draws = jax.random.uniform(jax.random.fold_in(jax.random.fold_in(key, 6), position), (blocks,), jnp.float32, low / len(split), largest / len(split))
        gain = gain * jnp.repeat(jnp.exp(draws), extent[position] // blocks).reshape((-1,) + (1,) * (len(extent) - 1 - position))
    return gain


def split_up(count, total, reach, slope):
    portions = [(1 << 20) // math.isqrt(standing ** slope) + 1 for standing in range(2, count + 1)]
    spare, holding = total - reach - (count - 1), [1] * (count - 1)
    while spare > 0:
        candidates = [i for i in range(count - 1) if holding[i] < reach]
        whole, remaining = sum([portions[i] for i in candidates]), spare
        for i in candidates:
            more = min(reach - holding[i], max(1, remaining * portions[i] // whole), spare)
            holding[i] = holding[i] + more
            spare = spare - more
    return np.array([reach] + holding)


def uneven_parts(rng, number_of, total, most, lean):
    if number_of == 2:
        one = jax.random.randint(rng, (), max(1, total - most), min(most, total - 1) + 1)
        return jnp.stack([one, total - one])
    sizes = jnp.asarray(split_up(number_of, total, most, lean), jnp.int32)
    pairs = (number_of - 1) // 2
    giver, sink = sizes[1:1 + 2 * pairs:2], sizes[2:2 + 2 * pairs:2]
    room = jnp.minimum(giver - 1, most - sink)
    passed = jax.random.randint(jax.random.fold_in(rng, 1), (pairs,), 0, 1 << 20) % (room + 1)
    sizes = sizes.at[1:1 + 2 * pairs:2].set(giver - passed).at[2:2 + 2 * pairs:2].set(sink + passed)
    return sizes[jax.random.permutation(jax.random.fold_in(rng, 2), number_of)]


def gaussian(key, dims, scale, bound, pieces=(), kind=jnp.bfloat16):
    entries = scale * jax.random.normal(key, dims, jnp.float32)
    if pieces:
        entries = entries * levels(key, dims, pieces, -0.22, 0.18)
    return jnp.clip(entries, -bound, bound).astype(kind)


def setup_inputs(seed: int = 0) -> dict:
    key_of = jax.random.split(jax.random.key(seed), 11)
    x_in = gaussian(key_of[0], (SEQUENCE_TOTAL, SEQUENCE_LENGTH, D), 1.0, 6.0, ((0, 4), (1, 4)))
    query_key_value_weight = gaussian(key_of[1], (LAYERS, D, QKVW), D ** -0.5, 0.15625, ((1, 4), (2, 2)))
    qkv_bias = gaussian(key_of[2], (LAYERS, QKVW), 0.5, 3.0, ((1, 2),))
    output_weight = gaussian(key_of[3], (LAYERS, D, QUERY_HEADS * HEAD_SIZE), (QUERY_HEADS * HEAD_SIZE // 32) ** -0.5, 0.875, ((1, 4), (2, 2)))
    feedforward_entry_matrix = gaussian(key_of[4], (LAYERS, D, 2, FF), D ** -0.5, 0.15625, ((1, 4), (3, 2)))
    down_weight = gaussian(key_of[5], (LAYERS, D, FF), (FF // 4) ** -0.5, 0.125, ((1, 4), (2, 2)))
    norm_gains = jnp.clip(1.0 + 0.1 * jax.random.normal(key_of[6], (LAYERS, 2, D), jnp.float32), 0.5, 1.5).astype(jnp.bfloat16)
    piece_starts = draw_piece_starts(jax.random.fold_in(key_of[10], 71), 0)
    seq_lengths = uneven_parts(key_of[8], SEQUENCE_TOTAL, SEQUENCE_TOTAL * SEQUENCE_LENGTH * 3 // 4, SEQUENCE_LENGTH, 1).astype(jnp.int32)
    grad_out = gaussian(key_of[9], (SEQUENCE_TOTAL, SEQUENCE_LENGTH, D), 1.0, 6.0, ((0, 4), (1, 4)))
    return {"x_in": x_in, "query_key_value_weight": query_key_value_weight, "qkv_bias": qkv_bias, "output_weight": output_weight, "feedforward_entry_matrix": feedforward_entry_matrix, "down_weight": down_weight, "norm_gains": norm_gains, "piece_starts": piece_starts, "seq_lengths": seq_lengths, "grad_out": grad_out}


EPS = 1e-06
THETA = 1000000.0
EXACT_ARITHMETIC = lax.Precision.HIGHEST

@jax.custom_vjp
def low(v):
    return lax.optimization_barrier(v.astype(jnp.bfloat16)).astype(jnp.float32)

@jax.custom_vjp
def reduced_chain_rule(v):
    return v

def low_keep(v):
    return (low(v), None)

def low_pass(kept, grad):
    return (grad,)

def back_keep(v):
    return (v, None)

def back_low(kept, grad):
    return (low(grad),)
low.defvjp(low_keep, low_pass)
reduced_chain_rule.defvjp(back_keep, back_low)

def rope_tables(positions):
    freq = jnp.exp(jnp.arange(HEAD_SIZE // 2, dtype=jnp.float32) * (-2.0 * math.log(THETA) / HEAD_SIZE))
    angle = positions.astype(jnp.float32)[:, None] * freq[None, :]
    angle = jnp.concatenate([angle, angle], axis=1)
    return (jnp.cos(angle), jnp.sin(angle))

def rotate(content_entries, cosine, sine):
    half = content_entries.shape[-1] // 2
    turned = jnp.concatenate([-content_entries[..., half:], content_entries[..., :half]], axis=-1)
    return content_entries * cosine + turned * sine

def piece_ids(positions, starts):
    inside = (positions[..., :, None] >= starts[..., None, :]) & (positions[..., :, None] < starts[..., None, :] + PIECE)
    labels = jnp.arange(1, PIECES + 1, dtype=jnp.int32)
    return lax.optimization_barrier(jnp.sum(jnp.where(inside, labels, 0), axis=-1)).astype(jnp.int32)

def norm_scale(content_entries):
    return lax.rsqrt(lax.optimization_barrier(jnp.mean(content_entries * content_entries, axis=-1, keepdims=True)) + EPS)

def attend(query_rows, keys, content_entries, seq_len, starts):
    positions = jnp.arange(SEQUENCE_LENGTH, dtype=jnp.int32)
    labels = piece_ids(positions, starts)
    seen = (positions[None, :] < seq_len) & ((positions[None, :] <= positions[:, None]) | (labels[:, None] == labels[None, :]) & (labels[:, None] > 0))
    group_index = QUERY_HEADS // KEY_VALUE_HEADS
    grouped_heads = query_rows.reshape(SEQUENCE_LENGTH, KEY_VALUE_HEADS, group_index, HEAD_SIZE)
    attention_logits = jnp.einsum('ihgd,jhd->hgij', grouped_heads, keys, precision=EXACT_ARITHMETIC) / math.sqrt(HEAD_SIZE)
    attention_logits = jnp.where(seen[None, None], reduced_chain_rule(attention_logits), -1e+30)
    log_total = jax.nn.logsumexp(attention_logits, axis=-1, keepdims=True)
    shares = low(jnp.exp(attention_logits - log_total))
    mixed_output = jnp.einsum('hgij,jhd->ihgd', shares, content_entries, precision=EXACT_ARITHMETIC)
    return low(reduced_chain_rule(mixed_output)).reshape(SEQUENCE_LENGTH, QUERY_HEADS * HEAD_SIZE)

def layer(residual_state, weights, lengths, starts):
    query_key_value_weight, bias_vector, output_weight, feedforward_entry_matrix, down_weight, gains = weights
    cosine, sine = rope_tables(jnp.arange(SEQUENCE_LENGTH, dtype=jnp.int32))
    group_index = QUERY_HEADS // KEY_VALUE_HEADS
    first_normed = low(residual_state * norm_scale(residual_state) * gains[0])
    joined_output = reduced_chain_rule(jnp.einsum('rog,gt->rot', first_normed, query_key_value_weight, precision=EXACT_ARITHMETIC) + bias_vector)
    joined_output = joined_output.reshape(SEQUENCE_TOTAL, SEQUENCE_LENGTH, KEY_VALUE_HEADS, group_index + 2, HEAD_SIZE)
    query_rows = low(rotate(joined_output[:, :, :, :group_index], cosine[None, :, None, None, :], sine[None, :, None, None, :]))
    query_rows = query_rows.reshape(SEQUENCE_TOTAL, SEQUENCE_LENGTH, QUERY_HEADS, HEAD_SIZE)
    keys = low(rotate(joined_output[:, :, :, group_index], cosine[None, :, None, :], sine[None, :, None, :]))
    content_entries = low(joined_output[:, :, :, group_index + 1])
    mixed_output = lax.map(lambda item: jax.checkpoint(attend)(*item), (query_rows, keys, content_entries, lengths, starts))
    middle_state = residual_state + reduced_chain_rule(jnp.einsum('vwn,xn->vwx', mixed_output, output_weight, precision=EXACT_ARITHMETIC))
    rescaled_after_attention = low(middle_state * norm_scale(middle_state) * gains[1])
    swiglu_input_pair = reduced_chain_rule(jnp.einsum('fhe,elw->fhlw', rescaled_after_attention, feedforward_entry_matrix, precision=EXACT_ARITHMETIC))
    hidden_state = low(jax.nn.silu(swiglu_input_pair[:, :, 0]) * swiglu_input_pair[:, :, 1])
    return middle_state + reduced_chain_rule(jnp.einsum('cqr,jr->cqj', hidden_state, down_weight, precision=EXACT_ARITHMETIC))

def reference(x_in, query_key_value_weight, qkv_bias, output_weight, feedforward_entry_matrix, down_weight, norm_gains, piece_starts, seq_lengths, grad_out):
    stacks = tuple((w.astype(jnp.float32) for w in (query_key_value_weight, qkv_bias, output_weight, feedforward_entry_matrix, down_weight, norm_gains)))

    def forward(residual_state, *weights):
        for index in range(LAYERS):
            residual_state = jax.checkpoint(layer)(residual_state, tuple((w[index] for w in weights)), seq_lengths, piece_starts)
        return residual_state
    result, pull = jax.vjp(forward, x_in.astype(jnp.float32), *stacks)
    grads = pull(grad_out.astype(jnp.float32))
    return (result.astype(jnp.bfloat16), grads[0], grads[1], grads[2], grads[3], grads[4], grads[5], grads[6])
```

```python
import math

import jax
import jax.numpy as jnp
from jax import lax
from jax.sharding import PartitionSpec as P

QUERY_HEADS = 12
KEY_VALUE_HEADS = 2
HEAD_SIZE = 128
LAYERS = 2
PIECE = 256
PIECES = 2
LANES = 128


EPS = 1e-06
THETA = 1000000.0


def rope_tables(positions):
    freq = jnp.exp(
        jnp.arange(HEAD_SIZE // 2, dtype=jnp.float32) * (-2.0 * math.log(THETA) / HEAD_SIZE)
    )
    angle = positions.astype(jnp.float32)[:, None] * freq[None, :]
    angle = jnp.concatenate([angle, angle], axis=1)
    return (jnp.cos(angle), jnp.sin(angle))


def rotate(content_entries, cosine, sine):
    half = content_entries.shape[-1] // 2
    turned = jnp.concatenate([-content_entries[..., half:], content_entries[..., :half]], axis=-1)
    return content_entries * cosine + turned * sine


def rotate_back(grads, cosine, sine):
    half = grads.shape[-1] // 2
    shifted = grads * sine
    return grads * cosine + jnp.concatenate([shifted[..., half:], -shifted[..., :half]], axis=-1)


def piece_ids(positions, starts):
    inside = (positions[..., :, None] >= starts[..., None, :]) & (
        positions[..., :, None] < starts[..., None, :] + PIECE
    )
    labels = jnp.arange(1, PIECES + 1, dtype=jnp.int32)
    return jnp.sum(jnp.where(inside, labels, 0), axis=-1)


def norm_scale(content_entries):
    return lax.rsqrt(jnp.mean(content_entries * content_entries, axis=-1, keepdims=True) + EPS)


def norm_back(content_entries, scale, gain, grad_normed):
    inner = jnp.mean(grad_normed * gain * content_entries, axis=-1, keepdims=True)
    grad_values = scale * gain * grad_normed - content_entries * (scale * scale * scale) * inner
    gain_grad = jnp.sum(grad_normed * content_entries * scale, axis=0)
    return (grad_values, gain_grad)


def masked_scores(query_rows, keys_all, seen, root):
    raw = (
        jnp.einsum("sqgjd,skgd->sgjqk", query_rows, keys_all, preferred_element_type=jnp.float32)
        / root
    )
    return jnp.where(seen[:, None, None], raw, -1e30)


def left_product(left, right):
    return lax.dot_general(
        left, right, (((0,), (0,)), ((), ())), preferred_element_type=jnp.float32
    ).astype(jnp.bfloat16)


def layer_weights(qkv, out, gate_up, down, first_unit, block):
    depth = qkv.shape[0]
    part = depth // lax.axis_size("rep")
    first_row = lax.axis_index("rep") * part

    def whole(weight):
        rows = lax.dynamic_slice_in_dim(weight, first_row, part, axis=0)
        return lax.all_gather(rows, ("shard", "rep"), axis=0, tiled=True)

    gate_up_block = lax.dynamic_slice_in_dim(gate_up, first_unit, block, axis=2)
    down_block = lax.dynamic_slice_in_dim(down, first_unit, block, axis=1)
    return (
        whole(qkv),
        whole(out),
        lax.all_gather(gate_up_block.reshape(depth, 2 * block), "shard", axis=0, tiled=True),
        lax.all_gather(down_block, "shard", axis=0, tiled=True),
    )


def plane_sum(terms):
    part = lax.psum_scatter(terms.astype(jnp.bfloat16), "rep", scatter_dimension=0, tiled=True)
    return lax.psum(part, "tp").astype(jnp.float32)


def spread_block(grad):
    part = lax.psum_scatter(grad, "shard", scatter_dimension=0, tiled=True)
    return lax.all_gather(part, "rep", axis=0, tiled=False)


def join_blocks(blocks, width):
    reps, block = blocks.shape[0], blocks.shape[-1]
    parts = []
    for index in range(reps):
        skip = max(index * block - (width - block), 0)
        if skip < block:
            parts.append(blocks[index, ..., skip:])
    return jnp.concatenate(parts, axis=-1).astype(jnp.float32)


def sum_all(grad):
    part = lax.psum_scatter(grad, ("shard", "rep"), scatter_dimension=0, tiled=True)
    return lax.all_gather(part, "rep", axis=0, tiled=True)


def right_product(left, right):
    return lax.dot_general(
        left, right, (((1,), (1,)), ((), ())), preferred_element_type=jnp.float32
    )


def body(
    x_in,
    query_key_value_weight,
    qkv_bias,
    output_weight,
    feedforward_entry_matrix,
    down_weight,
    norm_gains,
    piece_starts,
    seq_lengths,
    grad_out,
):
    seqs, span, width = x_in.shape
    shards = lax.axis_size("shard")
    place = lax.axis_index("shard")
    length = span * shards
    rows = seqs * span
    group_index = QUERY_HEADS // KEY_VALUE_HEADS
    joined_width = query_key_value_weight.shape[2]
    local_groups = joined_width // ((group_index + 2) * HEAD_SIZE)
    heads_width = output_weight.shape[2]
    hidden_width = down_weight.shape[2]
    reps = lax.axis_size("rep")
    block = -(-hidden_width // (reps * LANES)) * LANES
    first_owned = lax.axis_index("rep") * block
    first_unit = jnp.minimum(first_owned, hidden_width - block)
    owned = first_unit + jnp.arange(block, dtype=jnp.int32)[None, :] >= first_owned
    root = math.sqrt(HEAD_SIZE)
    own_pos = place * span + jnp.arange(span, dtype=jnp.int32)
    all_pos = jnp.arange(length, dtype=jnp.int32)
    cosine, sine = rope_tables(own_pos)
    cos_query = cosine[None, :, None, None, :]
    sin_query = sine[None, :, None, None, :]
    cos_key = cosine[None, :, None, :]
    sin_key = sine[None, :, None, :]
    own_ids = piece_ids(jnp.broadcast_to(own_pos, (seqs, span)), piece_starts)
    all_ids = piece_ids(jnp.broadcast_to(all_pos, (seqs, length)), piece_starts)
    same_piece = (own_ids[:, :, None] == all_ids[:, None, :]) & (own_ids[:, :, None] > 0)
    seen = (all_pos[None, None, :] < seq_lengths[:, None, None]) & (
        (all_pos[None, None, :] <= own_pos[None, :, None]) | same_piece
    )
    residual_state = x_in.astype(jnp.float32).reshape(rows, width)
    saved = []
    for index in range(LAYERS):
        full_qkv, full_out, part_gate_up, part_down = layer_weights(
            query_key_value_weight[index],
            output_weight[index],
            feedforward_entry_matrix[index],
            down_weight[index],
            first_unit,
            block,
        )
        gains = norm_gains[index].astype(jnp.float32)
        scale_one = norm_scale(residual_state)
        first_normed = (residual_state * scale_one * gains[0]).astype(jnp.bfloat16)
        joined_output = jnp.dot(
            first_normed, full_qkv, preferred_element_type=jnp.float32
        ) + qkv_bias[index].astype(jnp.float32)
        joined_output = joined_output.reshape(seqs, span, local_groups, group_index + 2, HEAD_SIZE)
        query_rows = rotate(joined_output[:, :, :, :group_index], cos_query, sin_query).astype(
            jnp.bfloat16
        )
        keys = rotate(joined_output[:, :, :, group_index], cos_key, sin_key).astype(jnp.bfloat16)
        content_entries = joined_output[:, :, :, group_index + 1].astype(jnp.bfloat16)
        keys_all, values_all = (
            lax.all_gather(keys, "shard", axis=1, tiled=True),
            lax.all_gather(content_entries, "shard", axis=1, tiled=True),
        )
        attention_logits = masked_scores(query_rows, keys_all, seen, root)
        log_total = jax.nn.logsumexp(attention_logits, axis=-1, keepdims=True)
        shares = jnp.exp(attention_logits - log_total).astype(jnp.bfloat16)
        mixed_output = jnp.einsum(
            "sgjqk,skgd->sqgjd", shares, values_all, preferred_element_type=jnp.float32
        )
        mixed_output = mixed_output.astype(jnp.bfloat16).reshape(rows, heads_width)
        middle_state = residual_state + lax.psum(right_product(mixed_output, full_out), "tp")
        scale_two = norm_scale(middle_state)
        rescaled_after_attention = (middle_state * scale_two * gains[1]).astype(jnp.bfloat16)
        plane_rows = lax.all_gather(rescaled_after_attention, "rep", axis=0, tiled=True)
        gate = jnp.dot(plane_rows, part_gate_up[:, :block], preferred_element_type=jnp.float32)
        upper = jnp.dot(plane_rows, part_gate_up[:, block:], preferred_element_type=jnp.float32)
        hidden_state = jnp.where(owned, jax.nn.silu(gate) * upper, 0.0).astype(jnp.bfloat16)
        saved.append(
            (
                residual_state,
                scale_one,
                first_normed,
                query_rows,
                keys_all,
                values_all,
                log_total,
                mixed_output,
                middle_state,
                scale_two,
                plane_rows,
                gate,
                upper,
                hidden_state,
                full_qkv,
                full_out,
                part_gate_up,
                part_down,
            )
        )
        residual_state = middle_state + plane_sum(right_product(hidden_state, part_down))
    out_act = residual_state.astype(jnp.bfloat16).reshape(seqs, span, width)
    flow = grad_out.astype(jnp.float32).reshape(rows, width)
    gate_pieces = [None] * LAYERS
    down_pieces = [None] * LAYERS
    qkv_pieces = [None] * LAYERS
    out_pieces = [None] * LAYERS
    gain_grads = [None] * LAYERS
    bias_grads = [None] * LAYERS
    for index in reversed(range(LAYERS)):
        (
            residual_state,
            scale_one,
            first_normed,
            query_rows,
            keys_all,
            values_all,
            log_total,
            mixed_output,
            middle_state,
            scale_two,
            plane_rows,
            gate,
            upper,
            hidden_state,
            full_qkv,
            full_out,
            part_gate_up,
            part_down,
        ) = saved[index]
        gains = norm_gains[index].astype(jnp.float32)
        down_grad = flow.astype(jnp.bfloat16)
        plane_grad = lax.all_gather(down_grad, "rep", axis=0, tiled=True)
        hidden_grad = jnp.dot(plane_grad, part_down, preferred_element_type=jnp.float32)
        sigmoid = jax.nn.sigmoid(gate)
        gate_grad = hidden_grad * upper * (sigmoid + gate * sigmoid * (1.0 - sigmoid))
        up_grad = hidden_grad * (gate * sigmoid)
        gate_grad = jnp.where(owned, gate_grad, 0.0).astype(jnp.bfloat16)
        up_grad = jnp.where(owned, up_grad, 0.0).astype(jnp.bfloat16)
        normed_two_grad = plane_sum(
            right_product(gate_grad, part_gate_up[:, :block])
            + right_product(up_grad, part_gate_up[:, block:])
        )
        middle_grad, gain_two = norm_back(middle_state, scale_two, gains[1], normed_two_grad)
        middle_grad = flow + middle_grad
        out_grad = middle_grad.astype(jnp.bfloat16)
        mixed_grad = jnp.dot(out_grad, full_out, preferred_element_type=jnp.float32).astype(
            jnp.bfloat16
        )
        mixed_grad = mixed_grad.reshape(seqs, span, local_groups, group_index, HEAD_SIZE)
        attention_logits = masked_scores(query_rows, keys_all, seen, root)
        exact = jnp.exp(attention_logits - log_total)
        shares = exact.astype(jnp.bfloat16)
        share_grad = jnp.einsum(
            "sqgjd,skgd->sgjqk", mixed_grad, values_all, preferred_element_type=jnp.float32
        )
        centre = jnp.sum(exact * share_grad, axis=-1, keepdims=True)
        score_grad = (exact * (share_grad - centre)).astype(jnp.bfloat16)
        query_grad = (
            jnp.einsum(
                "sgjqk,skgd->sqgjd", score_grad, keys_all, preferred_element_type=jnp.float32
            )
            / root
        )
        key_grad = (
            jnp.einsum(
                "sgjqk,sqgjd->skgd", score_grad, query_rows, preferred_element_type=jnp.float32
            )
            / root
        )
        value_grad = jnp.einsum(
            "sgjqk,sqgjd->skgd", shares, mixed_grad, preferred_element_type=jnp.float32
        )
        key_own, value_own = (
            lax.psum_scatter(
                key_grad.astype(jnp.bfloat16), "shard", scatter_dimension=1, tiled=True
            ).astype(jnp.float32),
            lax.psum_scatter(
                value_grad.astype(jnp.bfloat16), "shard", scatter_dimension=1, tiled=True
            ).astype(jnp.float32),
        )
        unrotated_asks = rotate_back(query_grad, cos_query, sin_query)
        key_raw = rotate_back(key_own, cos_key, sin_key)
        joined_grad = jnp.concatenate(
            [unrotated_asks, key_raw[:, :, :, None], value_own[:, :, :, None]], axis=3
        )
        joined_grad = joined_grad.reshape(rows, joined_width).astype(jnp.bfloat16)
        bias_grads[index] = jnp.sum(joined_grad, axis=0, dtype=jnp.float32)
        normed_one_grad = lax.psum(
            right_product(joined_grad, full_qkv).astype(jnp.bfloat16), "tp"
        ).astype(jnp.float32)
        input_grad, gain_one = norm_back(residual_state, scale_one, gains[0], normed_one_grad)
        gain_grads[index] = jnp.stack([gain_one, gain_two])
        flow = middle_grad + input_grad
        gate_pieces[index] = spread_block(
            jnp.stack([left_product(plane_rows, gate_grad), left_product(plane_rows, up_grad)], 1)
        )
        down_pieces[index] = spread_block(left_product(plane_grad, hidden_state))
        qkv_pieces[index] = sum_all(left_product(first_normed, joined_grad))
        out_pieces[index] = sum_all(left_product(out_grad, mixed_output))
    grad_gate_up = jnp.stack([join_blocks(g, hidden_width) for g in gate_pieces])
    grad_down = jnp.stack([join_blocks(g, hidden_width) for g in down_pieces])
    grad_qkv = jnp.stack(qkv_pieces).astype(jnp.float32)
    grad_out_proj = jnp.stack(out_pieces).astype(jnp.float32)
    bias = jnp.stack(bias_grads)
    slots = jnp.arange(lax.axis_size("tp"), dtype=jnp.int32)[:, None, None] == lax.axis_index("tp")
    bias_slots = jnp.where(slots, bias[None], 0.0)
    gains_own = jnp.where(lax.axis_index("tp") == 0, jnp.stack(gain_grads), 0.0)
    gains_total, bias_slots = lax.psum((gains_own, bias_slots), ("rep", "shard", "tp"))
    bias_total = lax.dynamic_index_in_dim(bias_slots, lax.axis_index("tp"), 0, keepdims=False)
    grad_input = flow.reshape(seqs, span, width)
    return (
        out_act,
        grad_input,
        grad_qkv,
        bias_total,
        grad_out_proj,
        grad_gate_up,
        grad_down,
        gains_total,
    )


def solution(mesh):
    return jax.shard_map(
        body,
        mesh=mesh,
        in_specs=(
            P("rep", "shard", None),
            P(None, "shard", "tp"),
            P(None, "tp"),
            P(None, "shard", "tp"),
            P(None, "shard", None, "tp"),
            P(None, "shard", "tp"),
            P(),
            P("rep", None),
            P("rep"),
            P("rep", "shard", None),
        ),
        out_specs=(
            P("rep", "shard", None),
            P("rep", "shard", None),
            P(None, "shard", "tp"),
            P(None, "tp"),
            P(None, "shard", "tp"),
            P(None, "shard", None, "tp"),
            P(None, "shard", "tp"),
            P(),
        ),
        check_vma=False,
    )
```

```python
import math

import jax
import jax.numpy as jnp
from jax import lax
from jax.sharding import PartitionSpec as P

QUERY_HEADS = 12
KEY_VALUE_HEADS = 2
HEAD_SIZE = 128
LAYERS = 2
PIECE = 256
PIECES = 2
LANES = 128


EPS = 1e-06
THETA = 1000000.0


def rope_tables(positions):
    freq = jnp.exp(
        jnp.arange(HEAD_SIZE // 2, dtype=jnp.float32) * (-2.0 * math.log(THETA) / HEAD_SIZE)
    )
    angle = positions.astype(jnp.float32)[:, None] * freq[None, :]
    angle = jnp.concatenate([angle, angle], axis=1)
    return (jnp.cos(angle), jnp.sin(angle))


def rotate(content_entries, cosine, sine):
    half = content_entries.shape[-1] // 2
    turned = jnp.concatenate([-content_entries[..., half:], content_entries[..., :half]], axis=-1)
    return content_entries * cosine + turned * sine


def rotate_back(grads, cosine, sine):
    half = grads.shape[-1] // 2
    shifted = grads * sine
    return grads * cosine + jnp.concatenate([shifted[..., half:], -shifted[..., :half]], axis=-1)


def piece_ids(positions, starts):
    inside = (positions[..., :, None] >= starts[..., None, :]) & (
        positions[..., :, None] < starts[..., None, :] + PIECE
    )
    labels = jnp.arange(1, PIECES + 1, dtype=jnp.int32)
    return jnp.sum(jnp.where(inside, labels, 0), axis=-1)


def norm_scale(content_entries):
    return lax.rsqrt(jnp.mean(content_entries * content_entries, axis=-1, keepdims=True) + EPS)


def norm_back(content_entries, scale, gain, grad_normed):
    inner = jnp.mean(grad_normed * gain * content_entries, axis=-1, keepdims=True)
    grad_values = scale * gain * grad_normed - content_entries * (scale * scale * scale) * inner
    gain_grad = jnp.sum(grad_normed * content_entries * scale, axis=0)
    return (grad_values, gain_grad)


def masked_scores(query_rows, keys_all, seen, root):
    raw = (
        jnp.einsum("sqgjd,skgd->sgjqk", query_rows, keys_all, preferred_element_type=jnp.float32)
        / root
    )
    return jnp.where(seen[:, None, None], raw, -1e30)


def left_product(left, right):
    return lax.dot_general(
        left, right, (((0,), (0,)), ((), ())), preferred_element_type=jnp.float32
    ).astype(jnp.bfloat16)


def right_product(left, right):
    return lax.dot_general(
        left, right, (((1,), (1,)), ((), ())), preferred_element_type=jnp.float32
    )


def product(left, right):
    return jnp.dot(left, right, preferred_element_type=jnp.float32)


def peer_pairs(count, step):
    if count & (count - 1) == 0:
        return [(i, i ^ step) for i in range(count)], [(i, i ^ step) for i in range(count)]
    return (
        [((i + step) % count, i) for i in range(count)],
        [(i, (i + step) % count) for i in range(count)],
    )


def from_peer(values, axis, step):
    return lax.ppermute(values, axis, peer_pairs(lax.axis_size(axis), step)[0])


def to_peer(values, axis, step):
    return lax.ppermute(values, axis, peer_pairs(lax.axis_size(axis), step)[1])


def from_ring(values, axis, step):
    count = lax.axis_size(axis)
    return lax.ppermute(values, axis, [((i + step) % count, i) for i in range(count)])


def to_ring(values, axis, step):
    count = lax.axis_size(axis)
    return lax.ppermute(values, axis, [(i, (i + step) % count) for i in range(count)])


def ring_gather(values, axis, dim):
    blocks = [values]
    for step in range(1, lax.axis_size(axis)):
        blocks.append(from_ring(values, axis, step))
    return jnp.concatenate(blocks, axis=dim)


def ring_scatter(terms, axis, dim):
    count = lax.axis_size(axis)
    blocks = jnp.split(terms, count, axis=dim)
    arrived = [
        to_ring(blocks[step].astype(jnp.bfloat16), axis, step).astype(jnp.float32)
        for step in range(1, count)
    ]
    total = blocks[0].astype(jnp.float32)
    for block in arrived:
        total = total + block
    return total


def line_gather(values):
    count = lax.axis_size("shard")
    place = lax.axis_index("shard")
    up, down = [values], [values]
    for step in range(1, count):
        up.append(lax.ppermute(up[-1], "shard", [(i, i + 1) for i in range(step - 1, count - 1)]))
        down.append(lax.ppermute(down[-1], "shard", [(i, i - 1) for i in range(1, count - step + 1)]))
    blocks = [values]
    for step in range(1, count):
        blocks.append(jnp.where(place + step < count, down[step], up[count - step]))
    return jnp.concatenate(blocks, axis=0)


def line_scatter(terms):
    count = lax.axis_size("shard")
    blocks = jnp.split(terms, count, axis=0)
    up = down = None
    for far in range(count - 1, 0, -1):
        rising, falling = blocks[far], blocks[count - far]
        if up is not None:
            rising = (rising.astype(jnp.float32) + up.astype(jnp.float32)).astype(jnp.bfloat16)
            falling = (falling.astype(jnp.float32) + down.astype(jnp.float32)).astype(jnp.bfloat16)
        up = lax.ppermute(rising, "shard", [(i, i + 1) for i in range(count - far)])
        down = lax.ppermute(falling, "shard", [(i, i - 1) for i in range(far, count)])
    total = blocks[0].astype(jnp.float32)
    if up is not None:
        total = total + up.astype(jnp.float32) + down.astype(jnp.float32)
    return total.astype(jnp.bfloat16)


def plane_gather(rows):
    reps = lax.axis_size("rep")
    near = [rows] + [from_peer(rows, "rep", step) for step in range(1, reps)]
    blocks = list(near)
    for step in range(1, lax.axis_size("tp")):
        blocks.extend([from_ring(block, "tp", step) for block in near])
    return jnp.concatenate(blocks, axis=0)


def plane_scatter(product_of, reps):
    cores = lax.axis_size("tp")
    arrived = []
    for step in range(1, cores):
        far = product_of(step).astype(jnp.bfloat16)
        arrived.append([to_ring(block, "tp", step) for block in jnp.split(far, reps, axis=0)])
    near = jnp.split(product_of(0), reps, axis=0)
    sums = []
    for place in range(reps):
        total = near[place]
        for blocks in arrived:
            total = total + blocks[place].astype(jnp.float32)
        sums.append(total)
    total = sums[0]
    for step in range(1, reps):
        total = total + to_peer(sums[step].astype(jnp.bfloat16), "rep", step).astype(jnp.float32)
    return total


def rolled(values, shift, dim):
    extent = values.shape[dim]
    return lax.dynamic_slice_in_dim(
        jnp.concatenate([values, values], axis=dim), shift, extent, axis=dim
    )


def whole_weight(weight):
    part = weight.shape[0] // lax.axis_size("rep")
    rows = lax.dynamic_slice_in_dim(weight, lax.axis_index("rep") * part, part, axis=0)
    return lax.all_gather(rows, ("shard", "rep"), axis=0, tiled=True)


def join_blocks(blocks, width):
    reps, block = blocks.shape[0], blocks.shape[-1]
    parts = []
    for index in range(reps):
        skip = max(index * block - (width - block), 0)
        if skip < block:
            parts.append(blocks[index, ..., skip:])
    return jnp.concatenate(parts, axis=-1).astype(jnp.float32)


def sum_all(grad):
    part = lax.psum_scatter(grad, ("shard", "rep"), scatter_dimension=0, tiled=True)
    return lax.all_gather(part, "rep", axis=0, tiled=True)


def body(
    x_in,
    query_key_value_weight,
    qkv_bias,
    output_weight,
    feedforward_entry_matrix,
    down_weight,
    norm_gains,
    piece_starts,
    seq_lengths,
    grad_out,
):
    seqs, span, width = x_in.shape
    shards = lax.axis_size("shard")
    place = lax.axis_index("shard")
    cores = lax.axis_size("tp")
    core = lax.axis_index("tp")
    reps = lax.axis_size("rep")
    length = span * shards
    half = span // cores
    rows = seqs * span
    own_rows = seqs * half
    depth = width // shards
    group_index = QUERY_HEADS // KEY_VALUE_HEADS
    joined_width = query_key_value_weight.shape[2]
    local_groups = joined_width // ((group_index + 2) * HEAD_SIZE)
    heads_width = output_weight.shape[2]
    hidden_width = down_weight.shape[2]
    block = -(-hidden_width // (reps * LANES)) * LANES
    first_owned = lax.axis_index("rep") * block
    first_unit = jnp.minimum(first_owned, hidden_width - block)
    owned = first_unit + jnp.arange(block, dtype=jnp.int32)[None, :] >= first_owned
    root = math.sqrt(HEAD_SIZE)
    inner_pos = rolled(jnp.arange(span, dtype=jnp.int32), core * half, 0)
    own_pos = place * span + inner_pos
    all_pos = jnp.concatenate(
        [lax.rem(place + step, shards) * span + inner_pos for step in range(shards)]
    )
    cosine, sine = rope_tables(own_pos)
    cos_query = cosine[None, :, None, None, :]
    sin_query = sine[None, :, None, None, :]
    cos_key = cosine[None, :, None, :]
    sin_key = sine[None, :, None, :]
    own_ids = piece_ids(jnp.broadcast_to(own_pos, (seqs, span)), piece_starts)
    all_ids = piece_ids(jnp.broadcast_to(all_pos, (seqs, length)), piece_starts)
    same_piece = (own_ids[:, :, None] == all_ids[:, None, :]) & (own_ids[:, :, None] > 0)
    seen = (all_pos[None, None, :] < seq_lengths[:, None, None]) & (
        (all_pos[None, None, :] <= own_pos[None, :, None]) | same_piece
    )

    def turned(values):
        return rolled(values, place * depth, values.ndim - 1)

    def turned_back(values):
        return rolled(values, lax.rem(shards - place, shards) * depth, values.ndim - 1)

    def own_block(weight):
        part = lax.dynamic_slice_in_dim(weight, first_unit, block, axis=1)
        return jnp.where(owned, part, jnp.zeros_like(part))

    def core_gather(values):
        tall = ring_gather(values.reshape(seqs, half, -1), "tp", 1)
        return tall.reshape(rows, -1)

    def core_scatter(values):
        return ring_scatter(values.reshape(seqs, span, -1), "tp", 1).reshape(own_rows, -1)

    def whole_turned(weight):
        return rolled(whole_weight(weight), place * depth, 0)

    gains_all = turned(norm_gains.astype(jnp.float32))
    x_tall = turned(rolled(x_in, core * half, 1)).astype(jnp.float32)
    residual_state = x_tall[:, :half].reshape(own_rows, width)
    x_tall = x_tall.reshape(rows, width)
    first_normed = (x_tall * norm_scale(x_tall) * gains_all[0, 0]).astype(jnp.bfloat16)
    saved = []
    for index in range(LAYERS):
        full_qkv = whole_turned(query_key_value_weight[index])
        full_out = whole_turned(output_weight[index])
        part_gate = line_gather(own_block(feedforward_entry_matrix[index, :, 0]))
        part_up = line_gather(own_block(feedforward_entry_matrix[index, :, 1]))
        part_down = line_gather(own_block(down_weight[index]))
        gains = gains_all[index]
        scale_one = norm_scale(residual_state)
        if index:
            first_normed = core_gather(
                (residual_state * scale_one * gains[0]).astype(jnp.bfloat16)
            )
        joined_output = product(first_normed, full_qkv) + qkv_bias[index].astype(jnp.float32)
        joined_output = joined_output.reshape(seqs, span, local_groups, group_index + 2, HEAD_SIZE)
        query_rows = rotate(joined_output[:, :, :, :group_index], cos_query, sin_query).astype(
            jnp.bfloat16
        )
        keys = rotate(joined_output[:, :, :, group_index], cos_key, sin_key).astype(jnp.bfloat16)
        content_entries = joined_output[:, :, :, group_index + 1].astype(jnp.bfloat16)
        pair_all = ring_gather(jnp.stack([keys, content_entries]), "shard", 2)
        keys_all, values_all = pair_all[0], pair_all[1]
        attention_logits = masked_scores(query_rows, keys_all, seen, root)
        log_total = jax.nn.logsumexp(attention_logits, axis=-1, keepdims=True)
        shares = jnp.exp(attention_logits - log_total).astype(jnp.bfloat16)
        mixed_output = jnp.einsum(
            "sgjqk,skgd->sqgjd", shares, values_all, preferred_element_type=jnp.float32
        )
        mixed_output = mixed_output.astype(jnp.bfloat16).reshape(rows, heads_width)
        middle_state = residual_state + core_scatter(right_product(mixed_output, full_out))
        scale_two = norm_scale(middle_state)
        plane_rows = plane_gather((middle_state * scale_two * gains[1]).astype(jnp.bfloat16))
        gate = product(plane_rows, part_gate)
        upper = product(plane_rows, part_up)
        hidden_state = (jax.nn.silu(gate) * upper).astype(jnp.bfloat16)
        saved.append(
            (
                residual_state,
                scale_one,
                first_normed,
                query_rows,
                keys_all,
                values_all,
                log_total,
                mixed_output,
                middle_state,
                scale_two,
                plane_rows,
                gate,
                upper,
                hidden_state,
                full_qkv,
                full_out,
                part_gate,
                part_up,
                part_down,
            )
        )
        near_rows = reps * own_rows

        def down_product(step):
            return right_product(
                hidden_state[step * near_rows : (step + 1) * near_rows], part_down
            )

        residual_state = middle_state + plane_scatter(down_product, reps)
    out_own = residual_state.astype(jnp.bfloat16)
    grad_tall = turned(rolled(grad_out, core * half, 1)[:, :half])
    flow = grad_tall.astype(jnp.float32).reshape(own_rows, width)
    gate_pieces = [None] * LAYERS
    down_pieces = [None] * LAYERS
    qkv_pieces = [None] * LAYERS
    out_pieces = [None] * LAYERS
    gain_grads = [None] * LAYERS
    bias_grads = [None] * LAYERS
    for index in reversed(range(LAYERS)):
        (
            residual_state,
            scale_one,
            first_normed,
            query_rows,
            keys_all,
            values_all,
            log_total,
            mixed_output,
            middle_state,
            scale_two,
            plane_rows,
            gate,
            upper,
            hidden_state,
            full_qkv,
            full_out,
            part_gate,
            part_up,
            part_down,
        ) = saved[index]
        gains = gains_all[index]
        plane_grad = plane_gather(flow.astype(jnp.bfloat16))
        hidden_grad = product(plane_grad, part_down)
        sigmoid = jax.nn.sigmoid(gate)
        gate_grad = hidden_grad * upper * (sigmoid + gate * sigmoid * (1.0 - sigmoid))
        up_grad = hidden_grad * (gate * sigmoid)
        gate_grad = gate_grad.astype(jnp.bfloat16)
        up_grad = up_grad.astype(jnp.bfloat16)

        def entry_product(step):
            some = slice(step * near_rows, (step + 1) * near_rows)
            return right_product(gate_grad[some], part_gate) + right_product(
                up_grad[some], part_up
            )

        normed_two_grad = plane_scatter(entry_product, reps)
        down_own = line_scatter(left_product(plane_grad, hidden_state))
        gate_own = line_scatter(left_product(plane_rows, gate_grad))
        up_own = line_scatter(left_product(plane_rows, up_grad))
        down_pieces[index] = lax.all_gather(down_own, "rep", axis=0, tiled=False)
        gate_pieces[index] = lax.all_gather(
            jnp.stack([gate_own, up_own], 1), "rep", axis=0, tiled=False
        )
        middle_grad, gain_two = norm_back(middle_state, scale_two, gains[1], normed_two_grad)
        middle_grad = flow + middle_grad
        out_grad = core_gather(middle_grad.astype(jnp.bfloat16))
        mixed_grad = product(out_grad, full_out).astype(jnp.bfloat16)
        mixed_grad = mixed_grad.reshape(seqs, span, local_groups, group_index, HEAD_SIZE)
        attention_logits = masked_scores(query_rows, keys_all, seen, root)
        exact = jnp.exp(attention_logits - log_total)
        shares = exact.astype(jnp.bfloat16)
        share_grad = jnp.einsum(
            "sqgjd,skgd->sgjqk", mixed_grad, values_all, preferred_element_type=jnp.float32
        )
        centre = jnp.sum(exact * share_grad, axis=-1, keepdims=True)
        score_grad = (exact * (share_grad - centre)).astype(jnp.bfloat16)
        query_grad = (
            jnp.einsum(
                "sgjqk,skgd->sqgjd", score_grad, keys_all, preferred_element_type=jnp.float32
            )
            / root
        )
        key_grad = (
            jnp.einsum(
                "sgjqk,sqgjd->skgd", score_grad, query_rows, preferred_element_type=jnp.float32
            )
            / root
        )
        value_grad = jnp.einsum(
            "sgjqk,sqgjd->skgd", shares, mixed_grad, preferred_element_type=jnp.float32
        )
        pair_own = ring_scatter(jnp.stack([key_grad, value_grad]), "shard", 2)
        key_own, value_own = pair_own[0], pair_own[1]
        unrotated_asks = rotate_back(query_grad, cos_query, sin_query)
        key_raw = rotate_back(key_own, cos_key, sin_key)
        joined_grad = jnp.concatenate(
            [unrotated_asks, key_raw[:, :, :, None], value_own[:, :, :, None]], axis=3
        )
        joined_grad = joined_grad.reshape(rows, joined_width).astype(jnp.bfloat16)
        bias_grads[index] = jnp.sum(joined_grad, axis=0, dtype=jnp.float32)
        normed_one_grad = core_scatter(right_product(joined_grad, full_qkv))
        input_grad, gain_one = norm_back(residual_state, scale_one, gains[0], normed_one_grad)
        gain_grads[index] = jnp.stack([gain_one, gain_two])
        flow = middle_grad + input_grad
        back = lax.rem(shards - place, shards) * depth
        qkv_pieces[index] = sum_all(rolled(left_product(first_normed, joined_grad), back, 0))
        out_pieces[index] = sum_all(rolled(left_product(out_grad, mixed_output), back, 0))
    grad_gate_up = jnp.stack([join_blocks(g, hidden_width) for g in gate_pieces])
    grad_down = jnp.stack([join_blocks(g, hidden_width) for g in down_pieces])
    grad_qkv = jnp.stack(qkv_pieces).astype(jnp.float32)
    grad_out_proj = jnp.stack(out_pieces).astype(jnp.float32)
    bias = jnp.stack(bias_grads)
    slots = jnp.arange(cores, dtype=jnp.int32)[:, None, None] == core
    bias_slots = jnp.where(slots, bias[None], 0.0)
    gains_own = turned_back(jnp.stack(gain_grads))
    gains_total, bias_slots = lax.psum((gains_own, bias_slots), ("rep", "shard", "tp"))
    bias_total = lax.dynamic_index_in_dim(bias_slots, core, 0, keepdims=False)

    def whole_rows(values):
        tall = turned_back(core_gather(values)).reshape(seqs, span, width)
        return rolled(tall, lax.rem(cores - core, cores) * half, 1)

    return (
        whole_rows(out_own),
        whole_rows(flow),
        grad_qkv,
        bias_total,
        grad_out_proj,
        grad_gate_up,
        grad_down,
        gains_total,
    )


def solution(mesh):
    return jax.shard_map(
        body,
        mesh=mesh,
        in_specs=(
            P("rep", "shard", None),
            P(None, "shard", "tp"),
            P(None, "tp"),
            P(None, "shard", "tp"),
            P(None, "shard", None, "tp"),
            P(None, "shard", "tp"),
            P(),
            P("rep", None),
            P("rep"),
            P("rep", "shard", None),
        ),
        out_specs=(
            P("rep", "shard", None),
            P("rep", "shard", None),
            P(None, "shard", "tp"),
            P(None, "tp"),
            P(None, "shard", "tp"),
            P(None, "shard", None, "tp"),
            P(None, "shard", "tp"),
            P(),
        ),
        check_vma=False,
    )
```

```python
import functools
import math

import jax
import jax.numpy as jnp
from jax import lax
from jax.experimental import pallas as pl
from jax.experimental.pallas import tpu as pltpu
from jax.sharding import PartitionSpec as P

QUERY_HEADS = 12
KEY_VALUE_HEADS = 2
HEAD_SIZE = 128
LAYERS = 2
PIECE = 256
PIECES = 2
LANES = 128


EPS = 1e-06
THETA = 1000000.0


def rope_tables(positions):
    freq = jnp.exp(
        jnp.arange(HEAD_SIZE // 2, dtype=jnp.float32) * (-2.0 * math.log(THETA) / HEAD_SIZE)
    )
    angle = positions.astype(jnp.float32)[:, None] * freq[None, :]
    angle = jnp.concatenate([angle, angle], axis=1)
    return (jnp.cos(angle), jnp.sin(angle))


def rotate(content_entries, cosine, sine):
    half = content_entries.shape[-1] // 2
    turned = jnp.concatenate([-content_entries[..., half:], content_entries[..., :half]], axis=-1)
    return content_entries * cosine + turned * sine


def rotate_back(grads, cosine, sine):
    half = grads.shape[-1] // 2
    shifted = grads * sine
    return grads * cosine + jnp.concatenate([shifted[..., half:], -shifted[..., :half]], axis=-1)


def piece_ids(positions, starts):
    inside = (positions[..., :, None] >= starts[..., None, :]) & (
        positions[..., :, None] < starts[..., None, :] + PIECE
    )
    labels = jnp.arange(1, PIECES + 1, dtype=jnp.int32)
    return jnp.sum(jnp.where(inside, labels, 0), axis=-1)


def norm_scale(content_entries):
    return lax.rsqrt(jnp.mean(content_entries * content_entries, axis=-1, keepdims=True) + EPS)


def norm_back(content_entries, scale, gain, grad_normed):
    inner = jnp.mean(grad_normed * gain * content_entries, axis=-1, keepdims=True)
    grad_values = scale * gain * grad_normed - content_entries * (scale * scale * scale) * inner
    gain_grad = jnp.sum(grad_normed * content_entries * scale, axis=0)
    return (grad_values, gain_grad)


def masked_scores(query_rows, keys_all, seen, root):
    raw = (
        jnp.einsum("sqgjd,skgd->sgjqk", query_rows, keys_all, preferred_element_type=jnp.float32)
        / root
    )
    return jnp.where(seen[:, None, None], raw, -1e30)


MESH = pl.DeviceIdType.MESH
FAST_BYTES_PER_US = 3_000_000


def left_product(left, right):
    return lax.dot_general(
        left, right, (((0,), (0,)), ((), ())), preferred_element_type=jnp.float32
    ).astype(jnp.bfloat16)


def right_product(left, right):
    return lax.dot_general(
        left, right, (((1,), (1,)), ((), ())), preferred_element_type=jnp.float32
    )


def product(left, right):
    return jnp.dot(left, right, preferred_element_type=jnp.float32)


def next_on(axis, step):
    return {axis: lax.rem(lax.axis_index(axis) + step, lax.axis_size(axis))}


def greet(sizes):
    barrier = pltpu.get_barrier_semaphore()
    for axis, count in sizes:
        for step in range(1, count):
            pl.semaphore_signal(
                barrier, inc=1, device_id=next_on(axis, step), device_id_type=MESH
            )
    pl.semaphore_wait(barrier, sum(count - 1 for _, count in sizes))


def start_copy(source, target, sent, received, device):
    copy = pltpu.make_async_remote_copy(
        src_ref=source,
        dst_ref=target,
        send_sem=sent,
        recv_sem=received,
        device_id=device,
        device_id_type=MESH,
    )
    copy.start()
    return copy


def by_rows(rows, update):
    size = math.gcd(rows, 32)

    def step(index, carry):
        update(pl.ds(pl.multiple_of(index * size, size), size))
        return carry

    lax.fori_loop(0, rows // size, step, 0)


def call_kernel(kernel, name, out_shape, scratch, operands, micros):
    return pl.pallas_call(
        kernel,
        out_shape=out_shape,
        in_specs=[pl.BlockSpec(memory_space=pltpu.VMEM)] * len(operands),
        out_specs=pl.BlockSpec(memory_space=pltpu.VMEM),
        scratch_shapes=scratch,
        compiler_params=pltpu.CompilerParams(
            collective_id=name, has_side_effects=True, vmem_limit_bytes=40 * 1024 * 1024
        ),
        cost_estimate=pl.CostEstimate(
            flops=0, bytes_accessed=int(micros * FAST_BYTES_PER_US), transcendentals=0
        ),
    )(*operands)


def ring_gather_kernel(axis, count, x_ref, out_ref, sent, received):
    greet(((axis, count),))
    copies = [
        start_copy(
            x_ref,
            out_ref.at[count - step],
            sent.at[step],
            received.at[count - step],
            next_on(axis, step),
        )
        for step in range(1, count)
    ]
    out_ref[0] = x_ref[...]
    for copy in copies:
        copy.wait()


def ring_gather(values, axis, name, micros):
    count = lax.axis_size(axis)
    if count == 1:
        return values[None]
    return call_kernel(
        functools.partial(ring_gather_kernel, axis, count),
        name,
        jax.ShapeDtypeStruct((count, *values.shape), values.dtype),
        [pltpu.SemaphoreType.DMA((count,)), pltpu.SemaphoreType.DMA((count,))],
        (values,),
        micros,
    )


def ring_scatter_kernel(axis, count, far_ref, near_ref, out_ref, arrived, sent, received):
    greet(((axis, count),))
    copies = [
        start_copy(
            far_ref.at[step - 1],
            arrived.at[step - 1],
            sent.at[step],
            received.at[step],
            next_on(axis, step),
        )
        for step in range(1, count)
    ]
    for copy in copies:
        copy.wait()

    def add(some):
        total = near_ref[some, :]
        for step in range(1, count):
            total = total + arrived[step - 1, some, :].astype(jnp.float32)
        out_ref[some, :] = total

    by_rows(near_ref.shape[0], add)


def ring_scatter(far, near, axis, name, micros):
    count = lax.axis_size(axis)
    if count == 1:
        return near
    return call_kernel(
        functools.partial(ring_scatter_kernel, axis, count),
        name,
        jax.ShapeDtypeStruct(near.shape, jnp.float32),
        [
            pltpu.VMEM(far.shape, far.dtype),
            pltpu.SemaphoreType.DMA((count,)),
            pltpu.SemaphoreType.DMA((count,)),
        ],
        (far, near),
        micros,
    )


def plane_gather_kernel(reps, cores, x_ref, out_ref, sent, received, sent_on, received_on):
    greet((("rep", reps), ("tp", cores)))
    copies = [
        start_copy(
            x_ref,
            out_ref.at[0, reps - step],
            sent.at[step],
            received.at[reps - step],
            next_on("rep", step),
        )
        for step in range(1, reps)
    ]
    passed = []

    def pass_on(source, slot):
        for step in range(1, cores):
            passed.append(
                start_copy(
                    source,
                    out_ref.at[cores - step, slot],
                    sent_on.at[step, slot],
                    received_on.at[cores - step, slot],
                    next_on("tp", step),
                )
            )

    pass_on(x_ref, 0)
    out_ref[0, 0] = x_ref[...]
    for copy, step in zip(copies, range(1, reps)):
        copy.wait_recv()
        pass_on(out_ref.at[0, reps - step], reps - step)
    for copy in copies:
        copy.wait_send()
    for copy in passed:
        copy.wait()


def plane_gather(rows):
    reps, cores = lax.axis_size("rep"), lax.axis_size("tp")
    gathered = call_kernel(
        functools.partial(plane_gather_kernel, reps, cores),
        1,
        jax.ShapeDtypeStruct((cores, reps, *rows.shape), rows.dtype),
        [
            pltpu.SemaphoreType.DMA((reps,)),
            pltpu.SemaphoreType.DMA((reps,)),
            pltpu.SemaphoreType.DMA((cores, reps)),
            pltpu.SemaphoreType.DMA((cores, reps)),
        ],
        (rows,),
        30,
    )
    return gathered.reshape(cores * reps * rows.shape[0], rows.shape[1])


def plane_scatter_kernel(
    reps,
    cores,
    far_ref,
    near_ref,
    out_ref,
    arrived,
    staged,
    landed,
    sent,
    received,
    sent_on,
    received_on,
):
    greet((("rep", reps), ("tp", cores)))
    rows = near_ref.shape[1]
    order = list(range(1, reps)) + [0]
    first = {}
    for slot in order:
        for step in range(1, cores):
            first[step, slot] = start_copy(
                far_ref.at[step - 1, slot],
                arrived.at[step - 1, slot],
                sent.at[step, slot],
                received.at[step, slot],
                next_on("tp", step),
            )

    def near_sum(slot, some):
        total = near_ref[slot, some, :]
        for step in range(1, cores):
            total = total + arrived[step - 1, slot, some, :].astype(jnp.float32)
        return total

    second = []
    for slot in order:
        for step in range(1, cores):
            first[step, slot].wait_recv()
        if slot:

            def stage(some, slot=slot):
                staged[slot - 1, some, :] = near_sum(slot, some).astype(jnp.bfloat16)

            by_rows(rows, stage)
            second.append(
                start_copy(
                    staged.at[slot - 1],
                    landed.at[slot - 1],
                    sent_on.at[slot],
                    received_on.at[slot],
                    next_on("rep", slot),
                )
            )
    for copy in first.values():
        copy.wait_send()
    for copy in second:
        copy.wait()

    def finish(some):
        total = near_sum(0, some)
        for slot in range(1, reps):
            total = total + landed[slot - 1, some, :].astype(jnp.float32)
        out_ref[some, :] = total

    by_rows(rows, finish)


def plane_scatter(far, near):
    reps, cores = lax.axis_size("rep"), lax.axis_size("tp")
    rows = near.shape[0] // reps
    far = far.reshape(cores - 1, reps, rows, far.shape[1])
    near = near.reshape(reps, rows, near.shape[1])
    return call_kernel(
        functools.partial(plane_scatter_kernel, reps, cores),
        2,
        jax.ShapeDtypeStruct(near.shape[1:], jnp.float32),
        [
            pltpu.VMEM(far.shape, jnp.bfloat16),
            pltpu.VMEM((reps - 1, *near.shape[1:]), jnp.bfloat16),
            pltpu.VMEM((reps - 1, *near.shape[1:]), jnp.bfloat16),
            pltpu.SemaphoreType.DMA((cores, reps)),
            pltpu.SemaphoreType.DMA((cores, reps)),
            pltpu.SemaphoreType.DMA((reps,)),
            pltpu.SemaphoreType.DMA((reps,)),
        ],
        (far, near),
        35,
    )


def sum_kernel(sizes, x_ref, out_ref, *scratch):
    greet(sizes)
    held = x_ref
    for place, (axis, count) in enumerate(sizes):
        total_ref, arrived, sent, received = scratch[4 * place : 4 * place + 4]
        copies = [
            start_copy(
                held, arrived.at[step - 1], sent.at[step], received.at[step], next_on(axis, step)
            )
            for step in range(1, count)
        ]
        for copy in copies:
            copy.wait()
        total = held[...]
        for step in range(1, count):
            total = total + arrived[step - 1]
        total_ref[...] = total
        held = total_ref
    out_ref[...] = held[...]


def sum_everywhere(values, axes, name):
    sizes = tuple((axis, lax.axis_size(axis)) for axis in axes)
    scratch = []
    for _, count in sizes:
        scratch.extend(
            [
                pltpu.VMEM(values.shape, jnp.float32),
                pltpu.VMEM((max(count - 1, 1), *values.shape), jnp.float32),
                pltpu.SemaphoreType.DMA((count,)),
                pltpu.SemaphoreType.DMA((count,)),
            ]
        )
    return call_kernel(
        functools.partial(sum_kernel, sizes),
        name,
        jax.ShapeDtypeStruct(values.shape, jnp.float32),
        scratch,
        (values,),
        8,
    )


def peer_pairs(count, step):
    if count & (count - 1) == 0:
        return [(i, i ^ step) for i in range(count)]
    return [((i + step) % count, i) for i in range(count)]


def replica_blocks(part):
    count = lax.axis_size("rep")
    me = lax.axis_index("rep")
    blocks = [part]
    for step in range(1, count):
        blocks.append(lax.ppermute(part, "rep", peer_pairs(count, step)))
    held = jnp.stack(blocks)
    places = []
    for index in range(count):
        if count & (count - 1) == 0:
            slot = lax.bitwise_xor(jnp.int32(index), me)
        else:
            slot = lax.rem(index - me + count, count)
        places.append(lax.dynamic_index_in_dim(held, slot, 0, keepdims=False))
    return places


def rolled(values, shift, dim):
    extent = values.shape[dim]
    return lax.dynamic_slice_in_dim(
        jnp.concatenate([values, values], axis=dim), shift, extent, axis=dim
    )


def whole_weight(weight):
    part = weight.shape[0] // lax.axis_size("rep")
    rows = lax.dynamic_slice_in_dim(weight, lax.axis_index("rep") * part, part, axis=0)
    return lax.all_gather(rows, ("shard", "rep"), axis=0, tiled=True)


def join_blocks(blocks, width):
    block = blocks[0].shape[-1]
    parts = []
    for index, part in enumerate(blocks):
        skip = max(index * block - (width - block), 0)
        if skip < block:
            parts.append(part[..., skip:])
    return jnp.concatenate(parts, axis=-1).astype(jnp.float32)


def body(
    x_in,
    query_key_value_weight,
    qkv_bias,
    output_weight,
    feedforward_entry_matrix,
    down_weight,
    norm_gains,
    piece_starts,
    seq_lengths,
    grad_out,
):
    seqs, span, width = x_in.shape
    shards = lax.axis_size("shard")
    place = lax.axis_index("shard")
    cores = lax.axis_size("tp")
    core = lax.axis_index("tp")
    reps = lax.axis_size("rep")
    length = span * shards
    half = span // cores
    rows = seqs * span
    own_rows = seqs * half
    depth = width // shards
    group_index = QUERY_HEADS // KEY_VALUE_HEADS
    joined_width = query_key_value_weight.shape[2]
    local_groups = joined_width // ((group_index + 2) * HEAD_SIZE)
    heads_width = output_weight.shape[2]
    hidden_width = down_weight.shape[2]
    block = -(-hidden_width // (reps * LANES)) * LANES
    first_owned = lax.axis_index("rep") * block
    first_unit = jnp.minimum(first_owned, hidden_width - block)
    owned = first_unit + jnp.arange(block, dtype=jnp.int32) >= first_owned
    root = math.sqrt(HEAD_SIZE)
    inner_pos = rolled(jnp.arange(span, dtype=jnp.int32), core * half, 0)
    own_pos = place * span + inner_pos
    all_pos = jnp.concatenate(
        [lax.rem(place + step, shards) * span + inner_pos for step in range(shards)]
    )
    cosine, sine = rope_tables(own_pos)
    cos_query = cosine[None, :, None, None, :]
    sin_query = sine[None, :, None, None, :]
    cos_key = cosine[None, :, None, :]
    sin_key = sine[None, :, None, :]
    own_ids = piece_ids(jnp.broadcast_to(own_pos, (seqs, span)), piece_starts)
    all_ids = piece_ids(jnp.broadcast_to(all_pos, (seqs, length)), piece_starts)
    same_piece = (own_ids[:, :, None] == all_ids[:, None, :]) & (own_ids[:, :, None] > 0)
    seen = (all_pos[None, None, :] < seq_lengths[:, None, None]) & (
        (all_pos[None, None, :] <= own_pos[None, :, None]) | same_piece
    )

    def own_block(weight):
        part = lax.dynamic_slice_in_dim(weight, first_unit, block, axis=weight.ndim - 1)
        return lax.optimization_barrier(jnp.where(owned, part, jnp.zeros_like(part)))

    def core_gather(values, name):
        tall = ring_gather(values, "tp", name, 6).reshape(cores, seqs, half, -1)
        return jnp.moveaxis(tall, 0, 1).reshape(rows, -1)

    def core_scatter(values):
        blocks = jnp.moveaxis(values.reshape(seqs, cores, half, -1), 1, 0)
        blocks = blocks.reshape(cores, own_rows, -1)
        return ring_scatter(blocks[1:].astype(jnp.bfloat16), blocks[0], "tp", 4, 8)

    gains_all = norm_gains.astype(jnp.float32)
    x_tall = rolled(x_in, core * half, 1).astype(jnp.float32)
    residual_state = x_tall[:, :half].reshape(own_rows, width)
    x_tall = x_tall.reshape(rows, width)
    first_normed = (x_tall * norm_scale(x_tall) * gains_all[0, 0]).astype(jnp.bfloat16)
    saved = []
    entry_blocks = own_block(feedforward_entry_matrix)
    down_blocks = own_block(down_weight)
    near_rows = reps * own_rows
    for index in range(LAYERS):
        full_qkv = whole_weight(query_key_value_weight[index])
        full_out = whole_weight(output_weight[index])
        part_entry = lax.all_gather(
            entry_blocks[index].reshape(depth, 2 * block), "shard", axis=0, tiled=True
        )
        part_down = lax.all_gather(down_blocks[index], "shard", axis=0, tiled=True)
        gains = gains_all[index]
        scale_one = norm_scale(residual_state)
        if index:
            first_normed = core_gather(
                (residual_state * scale_one * gains[0]).astype(jnp.bfloat16), 3
            )
        joined_output = product(first_normed, full_qkv) + qkv_bias[index].astype(jnp.float32)
        joined_output = joined_output.reshape(seqs, span, local_groups, group_index + 2, HEAD_SIZE)
        query_rows = rotate(joined_output[:, :, :, :group_index], cos_query, sin_query).astype(
            jnp.bfloat16
        )
        keys = rotate(joined_output[:, :, :, group_index], cos_key, sin_key).astype(jnp.bfloat16)
        content_entries = joined_output[:, :, :, group_index + 1].astype(jnp.bfloat16)
        pair = jnp.stack([keys, content_entries]).reshape(-1, HEAD_SIZE)
        pair_all = ring_gather(pair, "shard", 5, 12)
        pair_all = pair_all.reshape(shards, 2, seqs, span, local_groups, HEAD_SIZE)
        pair_all = jnp.moveaxis(pair_all, 0, 2).reshape(2, seqs, length, local_groups, HEAD_SIZE)
        keys_all, values_all = pair_all[0], pair_all[1]
        attention_logits = masked_scores(query_rows, keys_all, seen, root)
        log_total = jax.nn.logsumexp(attention_logits, axis=-1, keepdims=True)
        shares = jnp.exp(attention_logits - log_total).astype(jnp.bfloat16)
        mixed_output = jnp.einsum(
            "sgjqk,skgd->sqgjd", shares, values_all, preferred_element_type=jnp.float32
        )
        mixed_output = mixed_output.astype(jnp.bfloat16).reshape(rows, heads_width)
        middle_state = residual_state + core_scatter(right_product(mixed_output, full_out))
        scale_two = norm_scale(middle_state)
        plane_rows = plane_gather((middle_state * scale_two * gains[1]).astype(jnp.bfloat16))
        gate = product(plane_rows, part_entry[:, :block])
        upper = product(plane_rows, part_entry[:, block:])
        hidden_state = (jax.nn.silu(gate) * upper).astype(jnp.bfloat16)
        saved.append(
            (
                residual_state,
                scale_one,
                first_normed,
                query_rows,
                keys_all,
                values_all,
                log_total,
                mixed_output,
                middle_state,
                scale_two,
                plane_rows,
                gate,
                upper,
                hidden_state,
                full_qkv,
                full_out,
                part_entry,
                part_down,
            )
        )
        residual_state = middle_state + plane_scatter(
            right_product(hidden_state[near_rows:], part_down).astype(jnp.bfloat16),
            right_product(hidden_state[:near_rows], part_down),
        )
    out_own = residual_state.astype(jnp.bfloat16)
    grad_tall = rolled(grad_out, core * half, 1)[:, :half]
    flow = grad_tall.astype(jnp.float32).reshape(own_rows, width)
    gate_pieces = [None] * LAYERS
    down_pieces = [None] * LAYERS
    qkv_pieces = [None] * LAYERS
    out_pieces = [None] * LAYERS
    gain_grads = [None] * LAYERS
    bias_grads = [None] * LAYERS
    for index in reversed(range(LAYERS)):
        (
            residual_state,
            scale_one,
            first_normed,
            query_rows,
            keys_all,
            values_all,
            log_total,
            mixed_output,
            middle_state,
            scale_two,
            plane_rows,
            gate,
            upper,
            hidden_state,
            full_qkv,
            full_out,
            part_entry,
            part_down,
        ) = saved[index]
        gains = gains_all[index]
        plane_grad = plane_gather(flow.astype(jnp.bfloat16))
        hidden_grad = product(plane_grad, part_down)
        sigmoid = jax.nn.sigmoid(gate)
        gate_grad = hidden_grad * upper * (sigmoid + gate * sigmoid * (1.0 - sigmoid))
        up_grad = hidden_grad * (gate * sigmoid)
        entry_grad = jnp.concatenate([gate_grad, up_grad], axis=1).astype(jnp.bfloat16)
        normed_two_grad = plane_scatter(
            right_product(entry_grad[near_rows:], part_entry).astype(jnp.bfloat16),
            right_product(entry_grad[:near_rows], part_entry),
        )
        down_own = lax.psum_scatter(
            left_product(plane_grad, hidden_state), "shard", scatter_dimension=0, tiled=True
        )
        entry_own = lax.psum_scatter(
            left_product(plane_rows, entry_grad), "shard", scatter_dimension=0, tiled=True
        )
        down_pieces[index] = replica_blocks(down_own)
        gate_pieces[index] = replica_blocks(entry_own)
        middle_grad, gain_two = norm_back(middle_state, scale_two, gains[1], normed_two_grad)
        middle_grad = flow + middle_grad
        out_grad = core_gather(middle_grad.astype(jnp.bfloat16), 3)
        mixed_grad = product(out_grad, full_out).astype(jnp.bfloat16)
        mixed_grad = mixed_grad.reshape(seqs, span, local_groups, group_index, HEAD_SIZE)
        attention_logits = masked_scores(query_rows, keys_all, seen, root)
        exact = jnp.exp(attention_logits - log_total)
        shares = exact.astype(jnp.bfloat16)
        share_grad = jnp.einsum(
            "sqgjd,skgd->sgjqk", mixed_grad, values_all, preferred_element_type=jnp.float32
        )
        centre = jnp.sum(exact * share_grad, axis=-1, keepdims=True)
        score_grad = (exact * (share_grad - centre)).astype(jnp.bfloat16)
        query_grad = (
            jnp.einsum(
                "sgjqk,skgd->sqgjd", score_grad, keys_all, preferred_element_type=jnp.float32
            )
            / root
        )
        key_grad = (
            jnp.einsum(
                "sgjqk,sqgjd->skgd", score_grad, query_rows, preferred_element_type=jnp.float32
            )
            / root
        )
        value_grad = jnp.einsum(
            "sgjqk,sqgjd->skgd", shares, mixed_grad, preferred_element_type=jnp.float32
        )
        pair = jnp.stack([key_grad, value_grad])
        pair = pair.reshape(2, seqs, shards, span, local_groups, HEAD_SIZE)
        pair = jnp.moveaxis(pair, 2, 0).reshape(shards, -1, HEAD_SIZE)
        pair_own = ring_scatter(pair[1:].astype(jnp.bfloat16), pair[0], "shard", 6, 14)
        pair_own = pair_own.reshape(2, seqs, span, local_groups, HEAD_SIZE)
        key_own, value_own = pair_own[0], pair_own[1]
        unrotated_asks = rotate_back(query_grad, cos_query, sin_query)
        key_raw = rotate_back(key_own, cos_key, sin_key)
        joined_grad = jnp.concatenate(
            [unrotated_asks, key_raw[:, :, :, None], value_own[:, :, :, None]], axis=3
        )
        joined_grad = joined_grad.reshape(rows, joined_width).astype(jnp.bfloat16)
        bias_grads[index] = jnp.sum(joined_grad, axis=0, dtype=jnp.float32)
        normed_one_grad = core_scatter(right_product(joined_grad, full_qkv))
        input_grad, gain_one = norm_back(residual_state, scale_one, gains[0], normed_one_grad)
        gain_grads[index] = jnp.stack([gain_one, gain_two])
        flow = middle_grad + input_grad
        both = jnp.concatenate(
            [left_product(first_normed, joined_grad), left_product(out_grad, mixed_output)], axis=1
        )
        part = lax.psum_scatter(both, ("shard", "rep"), scatter_dimension=0, tiled=True)
        qkv_pieces[index] = jnp.concatenate(replica_blocks(part), axis=0).astype(jnp.float32)
    grad_gate_up = []
    for blocks in gate_pieces:
        blocks = [piece.reshape(depth, 2, block) for piece in blocks]
        grad_gate_up.append(join_blocks(blocks, hidden_width))
    grad_gate_up = jnp.stack(grad_gate_up)
    grad_down = jnp.stack([join_blocks(blocks, hidden_width) for blocks in down_pieces])
    grad_both = jnp.stack(qkv_pieces)
    grad_qkv = grad_both[:, :, :joined_width]
    grad_out_proj = grad_both[:, :, joined_width:]
    bias = jnp.stack(bias_grads)
    slots = jnp.arange(cores, dtype=jnp.int32)[:, None, None] == core
    bias_slots = jnp.where(slots, bias[None], 0.0)
    gains_own = jnp.stack(gain_grads)
    small = jnp.concatenate([gains_own.reshape(-1), bias_slots.reshape(-1)])
    small = sum_everywhere(small.reshape(-1, LANES), ("rep", "shard", "tp"), 7).reshape(-1)
    gains_total = small[: gains_own.size].reshape(gains_own.shape)
    bias_slots = small[gains_own.size :].reshape(bias_slots.shape)
    bias_total = lax.dynamic_index_in_dim(bias_slots, core, 0, keepdims=False)

    def whole_rows(values, name):
        tall = core_gather(values, name).reshape(seqs, span, width)
        return rolled(tall, lax.rem(cores - core, cores) * half, 1)

    return (
        whole_rows(out_own, 3),
        whole_rows(flow, 8),
        grad_qkv,
        bias_total,
        grad_out_proj,
        grad_gate_up,
        grad_down,
        gains_total,
    )


def solution(mesh):
    return jax.shard_map(
        body,
        mesh=mesh,
        in_specs=(
            P("rep", "shard", None),
            P(None, "shard", "tp"),
            P(None, "tp"),
            P(None, "shard", "tp"),
            P(None, "shard", None, "tp"),
            P(None, "shard", "tp"),
            P(),
            P("rep", None),
            P("rep"),
            P("rep", "shard", None),
        ),
        out_specs=(
            P("rep", "shard", None),
            P("rep", "shard", None),
            P(None, "shard", "tp"),
            P(None, "tp"),
            P(None, "shard", "tp"),
            P(None, "shard", None, "tp"),
            P(None, "shard", "tp"),
            P(),
        ),
        check_vma=False,
    )
```

```python
import functools
import math

import jax
import jax.numpy as jnp
from jax import lax
from jax.experimental import pallas as pl
from jax.experimental.pallas import tpu as pltpu
from jax.sharding import PartitionSpec as P


QUERY_HEADS = 12
KEY_VALUE_HEADS = 2
HEAD_SIZE = 128
LAYERS = 2
PIECE = 256
PIECES = 2
LANES = 128


EPS = 1e-06
THETA = 1000000.0


def rope_tables(positions):
    freq = jnp.exp(
        jnp.arange(HEAD_SIZE // 2, dtype=jnp.float32) * (-2.0 * math.log(THETA) / HEAD_SIZE)
    )
    angle = positions.astype(jnp.float32)[:, None] * freq[None, :]
    angle = jnp.concatenate([angle, angle], axis=1)
    return (jnp.cos(angle), jnp.sin(angle))


def rotate(content_entries, cosine, sine):
    half = content_entries.shape[-1] // 2
    turned = jnp.concatenate([-content_entries[..., half:], content_entries[..., :half]], axis=-1)
    return content_entries * cosine + turned * sine


def rotate_back(grads, cosine, sine):
    half = grads.shape[-1] // 2
    shifted = grads * sine
    return grads * cosine + jnp.concatenate([shifted[..., half:], -shifted[..., :half]], axis=-1)


def piece_ids(positions, starts):
    inside = (positions[..., :, None] >= starts[..., None, :]) & (
        positions[..., :, None] < starts[..., None, :] + PIECE
    )
    labels = jnp.arange(1, PIECES + 1, dtype=jnp.int32)
    return jnp.sum(jnp.where(inside, labels, 0), axis=-1)


def norm_scale(content_entries):
    return lax.rsqrt(jnp.mean(content_entries * content_entries, axis=-1, keepdims=True) + EPS)


def norm_back(content_entries, scale, gain, grad_normed):
    inner = jnp.mean(grad_normed * gain * content_entries, axis=-1, keepdims=True)
    grad_values = scale * gain * grad_normed - content_entries * (scale * scale * scale) * inner
    gain_grad = jnp.sum(grad_normed * content_entries * scale, axis=0)
    return (grad_values, gain_grad)


def masked_scores(query_rows, keys_all, seen, root):
    raw = (
        jnp.einsum("sqgjd,skgd->sgjqk", query_rows, keys_all, preferred_element_type=jnp.float32)
        / root
    )
    return jnp.where(seen[:, None, None], raw, -1e30)


MESH = pl.DeviceIdType.MESH
FAST_BYTES_PER_US = 3_000_000


def left_product(left, right):
    return lax.dot_general(
        left, right, (((0,), (0,)), ((), ())), preferred_element_type=jnp.float32
    ).astype(jnp.bfloat16)


def right_product(left, right):
    return lax.dot_general(
        left, right, (((1,), (1,)), ((), ())), preferred_element_type=jnp.float32
    )


def product(left, right):
    return jnp.dot(left, right, preferred_element_type=jnp.float32)


def next_on(axis, step):
    return {axis: lax.rem(lax.axis_index(axis) + step, lax.axis_size(axis))}


def greet(sizes):
    barrier = pltpu.get_barrier_semaphore()
    for axis, count in sizes:
        for step in range(1, count):
            pl.semaphore_signal(
                barrier, inc=1, device_id=next_on(axis, step), device_id_type=MESH
            )
    pl.semaphore_wait(barrier, sum(count - 1 for _, count in sizes))


def start_copy(source, target, sent, received, device):
    copy = pltpu.make_async_remote_copy(
        src_ref=source,
        dst_ref=target,
        send_sem=sent,
        recv_sem=received,
        device_id=device,
        device_id_type=MESH,
    )
    copy.start()
    return copy


def by_rows(rows, update):
    size = next((size for size in (32, 16) if rows % size == 0), rows)

    def step(index, carry):
        update(pl.ds(pl.multiple_of(index * size, size), size))
        return carry

    lax.fori_loop(0, rows // size, step, 0)


def call_kernel(kernel, name, out_shape, scratch, operands, micros):
    return pl.pallas_call(
        kernel,
        out_shape=out_shape,
        in_specs=[pl.BlockSpec(memory_space=pltpu.VMEM)] * len(operands),
        out_specs=pl.BlockSpec(memory_space=pltpu.VMEM),
        scratch_shapes=scratch,
        compiler_params=pltpu.CompilerParams(
            collective_id=name, has_side_effects=True, vmem_limit_bytes=40 * 1024 * 1024
        ),
        cost_estimate=pl.CostEstimate(
            flops=0, bytes_accessed=int(micros * FAST_BYTES_PER_US), transcendentals=0
        ),
    )(*operands)


def ring_gather_kernel(axis, count, x_ref, out_ref, sent, received):
    greet(((axis, count),))
    copies = [
        start_copy(
            x_ref,
            out_ref.at[count - step],
            sent.at[step],
            received.at[count - step],
            next_on(axis, step),
        )
        for step in range(1, count)
    ]
    out_ref[0] = x_ref[...]
    for copy in copies:
        copy.wait()


def ring_gather(values, axis, name, micros):
    count = lax.axis_size(axis)
    if count == 1:
        return values[None]
    return call_kernel(
        functools.partial(ring_gather_kernel, axis, count),
        name,
        jax.ShapeDtypeStruct((count, *values.shape), values.dtype),
        [pltpu.SemaphoreType.DMA((count,)), pltpu.SemaphoreType.DMA((count,))],
        (values,),
        micros,
    )


def ring_scatter_kernel(axis, count, far_ref, near_ref, out_ref, arrived, sent, received):
    greet(((axis, count),))
    copies = [
        start_copy(
            far_ref.at[step - 1],
            arrived.at[step - 1],
            sent.at[step],
            received.at[step],
            next_on(axis, step),
        )
        for step in range(1, count)
    ]
    for copy in copies:
        copy.wait()

    def add(some):
        total = near_ref[some, :]
        for step in range(1, count):
            total = total + arrived[step - 1, some, :].astype(jnp.float32)
        out_ref[some, :] = total

    by_rows(near_ref.shape[0], add)


def ring_scatter(far, near, axis, name, micros):
    count = lax.axis_size(axis)
    if count == 1:
        return near
    return call_kernel(
        functools.partial(ring_scatter_kernel, axis, count),
        name,
        jax.ShapeDtypeStruct(near.shape, jnp.float32),
        [
            pltpu.VMEM(far.shape, far.dtype),
            pltpu.SemaphoreType.DMA((count,)),
            pltpu.SemaphoreType.DMA((count,)),
        ],
        (far, near),
        micros,
    )


def plane_gather_kernel(reps, cores, x_ref, out_ref, sent, received, sent_on, received_on):
    greet((("rep", reps), ("tp", cores)))
    copies = [
        start_copy(
            x_ref,
            out_ref.at[0, reps - step],
            sent.at[step],
            received.at[reps - step],
            next_on("rep", step),
        )
        for step in range(1, reps)
    ]
    passed = []

    def pass_on(source, slot):
        for step in range(1, cores):
            passed.append(
                start_copy(
                    source,
                    out_ref.at[cores - step, slot],
                    sent_on.at[step, slot],
                    received_on.at[cores - step, slot],
                    next_on("tp", step),
                )
            )

    pass_on(x_ref, 0)
    out_ref[0, 0] = x_ref[...]
    for copy, step in zip(copies, range(1, reps)):
        copy.wait_recv()
        pass_on(out_ref.at[0, reps - step], reps - step)
    for copy in copies:
        copy.wait_send()
    for copy in passed:
        copy.wait()


def plane_gather(rows):
    reps, cores = lax.axis_size("rep"), lax.axis_size("tp")
    gathered = call_kernel(
        functools.partial(plane_gather_kernel, reps, cores),
        1,
        jax.ShapeDtypeStruct((cores, reps, *rows.shape), rows.dtype),
        [
            pltpu.SemaphoreType.DMA((reps,)),
            pltpu.SemaphoreType.DMA((reps,)),
            pltpu.SemaphoreType.DMA((cores, reps)),
            pltpu.SemaphoreType.DMA((cores, reps)),
        ],
        (rows,),
        30,
    )
    return gathered.reshape(cores * reps * rows.shape[0], rows.shape[1])


def plane_scatter_kernel(
    reps,
    cores,
    far_ref,
    near_ref,
    out_ref,
    arrived,
    staged,
    landed,
    sent,
    received,
    sent_on,
    received_on,
):
    greet((("rep", reps), ("tp", cores)))
    rows = near_ref.shape[1]
    order = list(range(1, reps)) + [0]
    first = {}
    for slot in order:
        for step in range(1, cores):
            first[step, slot] = start_copy(
                far_ref.at[step - 1, slot],
                arrived.at[step - 1, slot],
                sent.at[step, slot],
                received.at[step, slot],
                next_on("tp", step),
            )

    def near_sum(slot, some):
        total = near_ref[slot, some, :]
        for step in range(1, cores):
            total = total + arrived[step - 1, slot, some, :].astype(jnp.float32)
        return total

    second = []
    for slot in order:
        for step in range(1, cores):
            first[step, slot].wait_recv()
        if slot:

            def stage(some, slot=slot):
                staged[slot - 1, some, :] = near_sum(slot, some).astype(jnp.bfloat16)

            by_rows(rows, stage)
            second.append(
                start_copy(
                    staged.at[slot - 1],
                    landed.at[slot - 1],
                    sent_on.at[slot],
                    received_on.at[slot],
                    next_on("rep", slot),
                )
            )
    for copy in first.values():
        copy.wait_send()
    for copy in second:
        copy.wait()

    def finish(some):
        total = near_sum(0, some)
        for slot in range(1, reps):
            total = total + landed[slot - 1, some, :].astype(jnp.float32)
        out_ref[some, :] = total

    by_rows(rows, finish)


def plane_scatter(far, near):
    reps, cores = lax.axis_size("rep"), lax.axis_size("tp")
    rows = near.shape[0] // reps
    far = far.reshape(cores - 1, reps, rows, far.shape[1])
    near = near.reshape(reps, rows, near.shape[1])
    return call_kernel(
        functools.partial(plane_scatter_kernel, reps, cores),
        2,
        jax.ShapeDtypeStruct(near.shape[1:], jnp.float32),
        [
            pltpu.VMEM(far.shape, jnp.bfloat16),
            pltpu.VMEM((reps - 1, *near.shape[1:]), jnp.bfloat16),
            pltpu.VMEM((reps - 1, *near.shape[1:]), jnp.bfloat16),
            pltpu.SemaphoreType.DMA((cores, reps)),
            pltpu.SemaphoreType.DMA((cores, reps)),
            pltpu.SemaphoreType.DMA((reps,)),
            pltpu.SemaphoreType.DMA((reps,)),
        ],
        (far, near),
        35,
    )


def weight_gather_kernel(
    shards, reps, w_ref, out_ref, sent, received, sent_on, received_on
):
    greet((("shard", shards), ("rep", reps)))
    place = lax.axis_index("shard")
    replica = lax.axis_index("rep")
    copies = [
        start_copy(
            w_ref.at[replica],
            out_ref.at[place, replica],
            sent.at[step],
            received.at[step],
            next_on("shard", step),
        )
        for step in range(1, shards)
    ]
    out_ref[place] = w_ref[...]
    passed = []
    for step in range(1, shards):
        copies[step - 1].wait_recv()
        source = out_ref.at[lax.rem(place + shards - step, shards), replica]
        for far in range(1, reps):
            passed.append(
                start_copy(
                    source,
                    source,
                    sent_on.at[step, far],
                    received_on.at[step, far],
                    next_on("rep", far),
                )
            )
    for copy in copies:
        copy.wait_send()
    for copy in passed:
        copy.wait()


def weight_gather(weight):
    shards, reps = lax.axis_size("shard"), lax.axis_size("rep")
    depth, columns = weight.shape
    parts = weight.reshape(reps, depth // reps, columns)
    gathered = call_kernel(
        functools.partial(weight_gather_kernel, shards, reps),
        9,
        jax.ShapeDtypeStruct((shards, *parts.shape), weight.dtype),
        [
            pltpu.SemaphoreType.DMA((shards,)),
            pltpu.SemaphoreType.DMA((shards,)),
            pltpu.SemaphoreType.DMA((shards, reps)),
            pltpu.SemaphoreType.DMA((shards, reps)),
        ],
        (parts,),
        50,
    )
    return gathered.reshape(shards * depth, columns)


def gradient_sum_kernel(
    shards,
    reps,
    grad_ref,
    out_ref,
    arrived,
    staged,
    landed,
    summed,
    sent,
    received,
    sent_far,
    received_far,
    sent_on,
    received_on,
):
    greet((("shard", shards), ("rep", reps)))
    place = lax.axis_index("shard")
    replica = lax.axis_index("rep")
    rows = grad_ref.shape[2]
    order = list(range(1, shards)) + [0]
    first = {}
    for step in order:
        target = lax.rem(place + step, shards)
        for far in range(1, reps):
            first[step, far] = start_copy(
                grad_ref.at[target, lax.rem(replica + far, reps)],
                arrived.at[far - 1, step],
                sent.at[step, far],
                received.at[step, far],
                next_on("rep", far),
            )

    def replica_sum(step, some):
        target = lax.rem(place + step, shards)
        total = grad_ref[target, replica, some, :].astype(jnp.float32)
        for far in range(1, reps):
            total = total + arrived[far - 1, step, some, :].astype(jnp.float32)
        return total

    second = []
    for step in order:
        for far in range(1, reps):
            first[step, far].wait_recv()
        if step:

            def stage(some, step=step):
                staged[step - 1, some, :] = replica_sum(step, some).astype(jnp.bfloat16)

            by_rows(rows, stage)
            second.append(
                start_copy(
                    staged.at[step - 1],
                    landed.at[step - 1],
                    sent_far.at[step],
                    received_far.at[step],
                    next_on("shard", step),
                )
            )
    for copy in second:
        copy.wait()

    def finish(some):
        total = replica_sum(0, some)
        for step in range(1, shards):
            total = total + landed[step - 1, some, :].astype(jnp.float32)
        summed[some, :] = total.astype(jnp.bfloat16)

    by_rows(rows, finish)
    third = [
        start_copy(
            summed,
            out_ref.at[replica],
            sent_on.at[far],
            received_on.at[far],
            next_on("rep", far),
        )
        for far in range(1, reps)
    ]
    out_ref[replica] = summed[...]
    for copy in first.values():
        copy.wait_send()
    for copy in third:
        copy.wait()


def gradient_sum(grad):
    shards, reps = lax.axis_size("shard"), lax.axis_size("rep")
    columns = grad.shape[1]
    depth = grad.shape[0] // shards
    piece = (depth // reps, columns)
    summed = call_kernel(
        functools.partial(gradient_sum_kernel, shards, reps),
        10,
        jax.ShapeDtypeStruct((reps, *piece), grad.dtype),
        [
            pltpu.VMEM((reps - 1, shards, *piece), grad.dtype),
            pltpu.VMEM((shards - 1, *piece), grad.dtype),
            pltpu.VMEM((shards - 1, *piece), grad.dtype),
            pltpu.VMEM(piece, grad.dtype),
            pltpu.SemaphoreType.DMA((shards, reps)),
            pltpu.SemaphoreType.DMA((shards, reps)),
            pltpu.SemaphoreType.DMA((shards,)),
            pltpu.SemaphoreType.DMA((shards,)),
            pltpu.SemaphoreType.DMA((reps,)),
            pltpu.SemaphoreType.DMA((reps,)),
        ],
        (grad.reshape(shards, reps, *piece),),
        90,
    )
    return summed.reshape(depth, columns)


def sum_kernel(sizes, x_ref, out_ref, *scratch):
    greet(sizes)
    held = x_ref
    for place, (axis, count) in enumerate(sizes):
        total_ref, arrived, sent, received = scratch[4 * place : 4 * place + 4]
        copies = [
            start_copy(
                held, arrived.at[step - 1], sent.at[step], received.at[step], next_on(axis, step)
            )
            for step in range(1, count)
        ]
        for copy in copies:
            copy.wait()
        total = held[...]
        for step in range(1, count):
            total = total + arrived[step - 1]
        total_ref[...] = total
        held = total_ref
    out_ref[...] = held[...]


def sum_everywhere(values, axes, name):
    sizes = tuple((axis, lax.axis_size(axis)) for axis in axes)
    scratch = []
    for _, count in sizes:
        scratch.extend(
            [
                pltpu.VMEM(values.shape, jnp.float32),
                pltpu.VMEM((max(count - 1, 1), *values.shape), jnp.float32),
                pltpu.SemaphoreType.DMA((count,)),
                pltpu.SemaphoreType.DMA((count,)),
            ]
        )
    return call_kernel(
        functools.partial(sum_kernel, sizes),
        name,
        jax.ShapeDtypeStruct(values.shape, jnp.float32),
        scratch,
        (values,),
        8,
    )


def peer_pairs(count, step):
    if count & (count - 1) == 0:
        return [(i, i ^ step) for i in range(count)]
    return [((i + step) % count, i) for i in range(count)]


def replica_blocks(part):
    count = lax.axis_size("rep")
    me = lax.axis_index("rep")
    blocks = [part]
    for step in range(1, count):
        blocks.append(lax.ppermute(part, "rep", peer_pairs(count, step)))
    held = jnp.stack(blocks)
    places = []
    for index in range(count):
        if count & (count - 1) == 0:
            slot = lax.bitwise_xor(jnp.int32(index), me)
        else:
            slot = lax.rem(index - me + count, count)
        places.append(lax.dynamic_index_in_dim(held, slot, 0, keepdims=False))
    return places


def rolled(values, shift, dim):
    extent = values.shape[dim]
    return lax.dynamic_slice_in_dim(
        jnp.concatenate([values, values], axis=dim), shift, extent, axis=dim
    )


def gathered(weight):
    return lax.all_gather(weight, "shard", axis=0, tiled=True)


def scattered(grad, axes="shard"):
    return lax.psum_scatter(grad, axes, scatter_dimension=0, tiled=True)


def join_blocks(blocks, width):
    block = blocks[0].shape[-1]
    parts = []
    for index, part in enumerate(blocks):
        skip = max(index * block - (width - block), 0)
        if skip < block:
            parts.append(part[..., skip:])
    return jnp.concatenate(parts, axis=-1).astype(jnp.float32)


def body(
    x_in,
    query_key_value_weight,
    qkv_bias,
    output_weight,
    feedforward_entry_matrix,
    down_weight,
    norm_gains,
    piece_starts,
    seq_lengths,
    grad_out,
):
    seqs, span, width = x_in.shape
    shards = lax.axis_size("shard")
    place = lax.axis_index("shard")
    cores = lax.axis_size("tp")
    core = lax.axis_index("tp")
    reps = lax.axis_size("rep")
    length = span * shards
    half = span // cores
    rows = seqs * span
    own_rows = seqs * half
    depth = width // shards
    group_index = QUERY_HEADS // KEY_VALUE_HEADS
    joined_width = query_key_value_weight.shape[2]
    local_groups = joined_width // ((group_index + 2) * HEAD_SIZE)
    heads_width = output_weight.shape[2]
    hidden_width = down_weight.shape[2]
    block = -(-hidden_width // (reps * LANES)) * LANES
    first_owned = lax.axis_index("rep") * block
    first_unit = jnp.minimum(first_owned, hidden_width - block)
    owned = first_unit + jnp.arange(block, dtype=jnp.int32) >= first_owned
    root = math.sqrt(HEAD_SIZE)
    inner_pos = rolled(jnp.arange(span, dtype=jnp.int32), core * half, 0)
    own_pos = place * span + inner_pos
    all_pos = jnp.concatenate(
        [lax.rem(place + step, shards) * span + inner_pos for step in range(shards)]
    )
    cosine, sine = rope_tables(own_pos)
    cos_query = cosine[None, :, None, None, :]
    sin_query = sine[None, :, None, None, :]
    cos_key = cosine[None, :, None, :]
    sin_key = sine[None, :, None, :]
    own_ids = piece_ids(jnp.broadcast_to(own_pos, (seqs, span)), piece_starts)
    all_ids = piece_ids(jnp.broadcast_to(all_pos, (seqs, length)), piece_starts)
    same_piece = (own_ids[:, :, None] == all_ids[:, None, :]) & (own_ids[:, :, None] > 0)
    seen = (all_pos[None, None, :] < seq_lengths[:, None, None]) & (
        (all_pos[None, None, :] <= own_pos[None, :, None]) | same_piece
    )

    def own_block(weight):
        part = lax.dynamic_slice_in_dim(weight, first_unit, block, axis=weight.ndim - 1)
        return lax.optimization_barrier(jnp.where(owned, part, jnp.zeros_like(part)))

    def core_gather(values, name):
        tall = ring_gather(values, "tp", name, 6).reshape(cores, seqs, half, -1)
        return jnp.moveaxis(tall, 0, 1).reshape(rows, -1)

    def core_scatter(values):
        blocks = jnp.moveaxis(values.reshape(seqs, cores, half, -1), 1, 0)
        blocks = blocks.reshape(cores, own_rows, -1)
        return ring_scatter(blocks[1:].astype(jnp.bfloat16), blocks[0], "tp", 4, 8)

    gains_all = norm_gains.astype(jnp.float32)
    x_tall = rolled(x_in, core * half, 1).astype(jnp.float32)
    residual_state = x_tall[:, :half].reshape(own_rows, width)
    x_tall = x_tall.reshape(rows, width)
    first_normed = (x_tall * norm_scale(x_tall) * gains_all[0, 0]).astype(jnp.bfloat16)
    saved = []
    entry_blocks = own_block(feedforward_entry_matrix)
    down_blocks = own_block(down_weight)
    near_rows = reps * own_rows
    for index in range(LAYERS):
        full_both = weight_gather(
            jnp.concatenate([query_key_value_weight[index], output_weight[index]], axis=1)
        )
        full_qkv, full_out = full_both[:, :joined_width], full_both[:, joined_width:]
        part_entry = gathered(entry_blocks[index].reshape(depth, 2 * block))
        part_down = gathered(down_blocks[index])
        gains = gains_all[index]
        scale_one = norm_scale(residual_state)
        if index:
            first_normed = core_gather(
                (residual_state * scale_one * gains[0]).astype(jnp.bfloat16), 3
            )
        joined_output = product(first_normed, full_qkv) + qkv_bias[index].astype(jnp.float32)
        joined_output = joined_output.reshape(seqs, span, local_groups, group_index + 2, HEAD_SIZE)
        query_rows = rotate(joined_output[:, :, :, :group_index], cos_query, sin_query).astype(
            jnp.bfloat16
        )
        keys = rotate(joined_output[:, :, :, group_index], cos_key, sin_key).astype(jnp.bfloat16)
        content_entries = joined_output[:, :, :, group_index + 1].astype(jnp.bfloat16)
        pair = jnp.stack([keys, content_entries]).reshape(-1, HEAD_SIZE)
        pair_all = ring_gather(pair, "shard", 5, 12)
        pair_all = pair_all.reshape(shards, 2, seqs, span, local_groups, HEAD_SIZE)
        pair_all = jnp.moveaxis(pair_all, 0, 2).reshape(2, seqs, length, local_groups, HEAD_SIZE)
        keys_all, values_all = pair_all[0], pair_all[1]
        attention_logits = masked_scores(query_rows, keys_all, seen, root)
        log_total = jax.nn.logsumexp(attention_logits, axis=-1, keepdims=True)
        shares = jnp.exp(attention_logits - log_total).astype(jnp.bfloat16)
        mixed_output = jnp.einsum(
            "sgjqk,skgd->sqgjd", shares, values_all, preferred_element_type=jnp.float32
        )
        mixed_output = mixed_output.astype(jnp.bfloat16).reshape(rows, heads_width)
        middle_state = residual_state + core_scatter(right_product(mixed_output, full_out))
        scale_two = norm_scale(middle_state)
        plane_rows = plane_gather((middle_state * scale_two * gains[1]).astype(jnp.bfloat16))
        gate = product(plane_rows, part_entry[:, :block])
        upper = product(plane_rows, part_entry[:, block:])
        hidden_state = (jax.nn.silu(gate) * upper).astype(jnp.bfloat16)
        saved.append(
            (
                residual_state,
                scale_one,
                first_normed,
                query_rows,
                keys_all,
                values_all,
                log_total,
                mixed_output,
                middle_state,
                scale_two,
                plane_rows,
                gate,
                upper,
                hidden_state,
                full_qkv,
                full_out,
                part_entry,
                part_down,
            )
        )
        residual_state = middle_state + plane_scatter(
            right_product(hidden_state[near_rows:], part_down).astype(jnp.bfloat16),
            right_product(hidden_state[:near_rows], part_down),
        )
    out_own = residual_state.astype(jnp.bfloat16)
    grad_tall = rolled(grad_out, core * half, 1)[:, :half]
    flow = grad_tall.astype(jnp.float32).reshape(own_rows, width)
    up_pieces = [None] * LAYERS
    gate_pieces = [None] * LAYERS
    down_pieces = [None] * LAYERS
    qkv_pieces = [None] * LAYERS
    gain_grads = [None] * LAYERS
    bias_grads = [None] * LAYERS
    pending = None
    for index in reversed(range(LAYERS)):
        (
            residual_state,
            scale_one,
            first_normed,
            query_rows,
            keys_all,
            values_all,
            log_total,
            mixed_output,
            middle_state,
            scale_two,
            plane_rows,
            gate,
            upper,
            hidden_state,
            full_qkv,
            full_out,
            part_entry,
            part_down,
        ) = saved[index]
        gains = gains_all[index]
        plane_grad = plane_gather(flow.astype(jnp.bfloat16))
        hidden_grad = product(plane_grad, part_down)
        down_total = left_product(plane_grad, hidden_state)
        hidden_grad, down_total = lax.optimization_barrier((hidden_grad, down_total))
        down_own = scattered(down_total)
        sigmoid = jax.nn.sigmoid(gate)
        gate_grad = hidden_grad * upper * (sigmoid + gate * sigmoid * (1.0 - sigmoid))
        up_grad = hidden_grad * (gate * sigmoid)
        entry_grad = jnp.concatenate([gate_grad, up_grad], axis=1).astype(jnp.bfloat16)
        gate_total = left_product(plane_rows, entry_grad[:, :block])
        up_total = left_product(plane_rows, entry_grad[:, block:])
        entry_grad, gate_total, up_total = lax.optimization_barrier(
            (entry_grad, gate_total, up_total)
        )
        own_parts = (down_own, scattered(gate_total), scattered(up_total))
        far_product = right_product(entry_grad[near_rows:], part_entry).astype(jnp.bfloat16)
        near_product = right_product(entry_grad[:near_rows], part_entry)
        normed_two_grad = plane_scatter(far_product, near_product)
        middle_grad, gain_two = norm_back(middle_state, scale_two, gains[1], normed_two_grad)
        middle_grad = flow + middle_grad
        out_grad = core_gather(middle_grad.astype(jnp.bfloat16), 3)
        mixed_grad = product(out_grad, full_out).astype(jnp.bfloat16)
        mixed_grad, pending = lax.optimization_barrier((mixed_grad, pending))
        if pending is not None:
            down_pieces[index + 1], gate_pieces[index + 1], up_pieces[index + 1] = [
                replica_blocks(part) for part in pending
            ]
        pending = own_parts
        mixed_grad = mixed_grad.reshape(seqs, span, local_groups, group_index, HEAD_SIZE)
        attention_logits = masked_scores(query_rows, keys_all, seen, root)
        exact = jnp.exp(attention_logits - log_total)
        shares = exact.astype(jnp.bfloat16)
        share_grad = jnp.einsum(
            "sqgjd,skgd->sgjqk", mixed_grad, values_all, preferred_element_type=jnp.float32
        )
        centre = jnp.sum(exact * share_grad, axis=-1, keepdims=True)
        score_grad = (exact * (share_grad - centre)).astype(jnp.bfloat16)
        query_grad = (
            jnp.einsum(
                "sgjqk,skgd->sqgjd", score_grad, keys_all, preferred_element_type=jnp.float32
            )
            / root
        )
        key_grad = (
            jnp.einsum(
                "sgjqk,sqgjd->skgd", score_grad, query_rows, preferred_element_type=jnp.float32
            )
            / root
        )
        value_grad = jnp.einsum(
            "sgjqk,sqgjd->skgd", shares, mixed_grad, preferred_element_type=jnp.float32
        )
        pair = jnp.stack([key_grad, value_grad])
        pair = pair.reshape(2, seqs, shards, span, local_groups, HEAD_SIZE)
        pair = jnp.moveaxis(pair, 2, 0).reshape(shards, -1, HEAD_SIZE)
        pair_own = ring_scatter(pair[1:].astype(jnp.bfloat16), pair[0], "shard", 6, 14)
        pair_own = pair_own.reshape(2, seqs, span, local_groups, HEAD_SIZE)
        key_own, value_own = pair_own[0], pair_own[1]
        unrotated_asks = rotate_back(query_grad, cos_query, sin_query)
        key_raw = rotate_back(key_own, cos_key, sin_key)
        joined_grad = jnp.concatenate(
            [unrotated_asks, key_raw[:, :, :, None], value_own[:, :, :, None]], axis=3
        )
        joined_grad = joined_grad.reshape(rows, joined_width).astype(jnp.bfloat16)
        bias_grads[index] = jnp.sum(joined_grad, axis=0, dtype=jnp.float32)
        normed_one_grad = core_scatter(right_product(joined_grad, full_qkv))
        input_grad, gain_one = norm_back(residual_state, scale_one, gains[0], normed_one_grad)
        gain_grads[index] = jnp.stack([gain_one, gain_two])
        flow = middle_grad + input_grad
        both = jnp.concatenate(
            [left_product(first_normed, joined_grad), left_product(out_grad, mixed_output)], axis=1
        )
        if index:
            part = scattered(both, ("shard", "rep"))
            both_sum = jnp.concatenate(replica_blocks(part), axis=0)
        else:
            both_sum = gradient_sum(both)
        qkv_pieces[index] = both_sum.astype(jnp.float32)
    down_pieces[0], gate_pieces[0], up_pieces[0] = [replica_blocks(part) for part in pending]
    grad_gate_up = []
    for gates, ups in zip(gate_pieces, up_pieces):
        pairs = [
            lax.optimization_barrier(jnp.concatenate(pair, axis=1)).reshape(depth, 2, block)
            for pair in zip(gates, ups)
        ]
        grad_gate_up.append(join_blocks(pairs, hidden_width))
    grad_gate_up = jnp.stack(grad_gate_up)
    grad_down = jnp.stack([join_blocks(blocks, hidden_width) for blocks in down_pieces])
    grad_both = jnp.stack(qkv_pieces)
    grad_qkv = grad_both[:, :, :joined_width]
    grad_out_proj = grad_both[:, :, joined_width:]
    bias = jnp.stack(bias_grads)
    slots = jnp.arange(cores, dtype=jnp.int32)[:, None, None] == core
    bias_slots = jnp.where(slots, bias[None], 0.0)
    gains_own = jnp.stack(gain_grads)
    small = jnp.concatenate([gains_own.reshape(-1), bias_slots.reshape(-1)])
    small = sum_everywhere(small.reshape(-1, LANES), ("rep", "shard", "tp"), 7).reshape(-1)
    gains_total = small[: gains_own.size].reshape(gains_own.shape)
    bias_slots = small[gains_own.size :].reshape(bias_slots.shape)
    bias_total = lax.dynamic_index_in_dim(bias_slots, core, 0, keepdims=False)

    def whole_rows(values, name):
        tall = core_gather(values, name).reshape(seqs, span, width)
        return rolled(tall, lax.rem(cores - core, cores) * half, 1)

    return (
        whole_rows(out_own, 3),
        whole_rows(flow, 8),
        grad_qkv,
        bias_total,
        grad_out_proj,
        grad_gate_up,
        grad_down,
        gains_total,
    )


def solution(mesh):
    return jax.shard_map(
        body,
        mesh=mesh,
        in_specs=(
            P("rep", "shard", None),
            P(None, "shard", "tp"),
            P(None, "tp"),
            P(None, "shard", "tp"),
            P(None, "shard", None, "tp"),
            P(None, "shard", "tp"),
            P(),
            P("rep", None),
            P("rep"),
            P("rep", "shard", None),
        ),
        out_specs=(
            P("rep", "shard", None),
            P("rep", "shard", None),
            P(None, "shard", "tp"),
            P(None, "tp"),
            P(None, "shard", "tp"),
            P(None, "shard", None, "tp"),
            P(None, "shard", "tp"),
            P(),
        ),
        check_vma=False,
    )
```

```python
import functools
import math

import jax
import jax.numpy as jnp
from jax import lax
from jax.experimental import pallas as pl
from jax.experimental.pallas import tpu as pltpu
from jax.sharding import PartitionSpec as P


QUERY_HEADS = 12
KEY_VALUE_HEADS = 2
HEAD_SIZE = 128
LAYERS = 2
PIECE = 256
PIECES = 2
LANES = 128


EPS = 1e-06
THETA = 1000000.0


def rope_tables(positions):
    freq = jnp.exp(
        jnp.arange(HEAD_SIZE // 2, dtype=jnp.float32) * (-2.0 * math.log(THETA) / HEAD_SIZE)
    )
    angle = positions.astype(jnp.float32)[:, None] * freq[None, :]
    angle = jnp.concatenate([angle, angle], axis=1)
    return (jnp.cos(angle), jnp.sin(angle))


def rotate(content_entries, cosine, sine):
    half = content_entries.shape[-1] // 2
    turned = jnp.concatenate([-content_entries[..., half:], content_entries[..., :half]], axis=-1)
    return content_entries * cosine + turned * sine


def rotate_back(grads, cosine, sine):
    half = grads.shape[-1] // 2
    shifted = grads * sine
    return grads * cosine + jnp.concatenate([shifted[..., half:], -shifted[..., :half]], axis=-1)


def piece_ids(positions, starts):
    inside = (positions[..., :, None] >= starts[..., None, :]) & (
        positions[..., :, None] < starts[..., None, :] + PIECE
    )
    labels = jnp.arange(1, PIECES + 1, dtype=jnp.int32)
    return jnp.sum(jnp.where(inside, labels, 0), axis=-1)


def norm_scale(content_entries):
    return lax.rsqrt(jnp.mean(content_entries * content_entries, axis=-1, keepdims=True) + EPS)


def norm_back(content_entries, scale, gain, grad_normed):
    inner = jnp.mean(grad_normed * gain * content_entries, axis=-1, keepdims=True)
    grad_values = scale * gain * grad_normed - content_entries * (scale * scale * scale) * inner
    gain_grad = jnp.sum(grad_normed * content_entries * scale, axis=0)
    return (grad_values, gain_grad)


def masked_scores(query_rows, keys_all, seen, root):
    raw = (
        jnp.einsum("sqgjd,skgd->sgjqk", query_rows, keys_all, preferred_element_type=jnp.float32)
        / root
    )
    return jnp.where(seen[:, None, None], raw, -1e30)


MESH = pl.DeviceIdType.MESH
FAST_BYTES_PER_US = 3_000_000


def left_product(left, right):
    return lax.dot_general(
        left, right, (((0,), (0,)), ((), ())), preferred_element_type=jnp.float32
    ).astype(jnp.bfloat16)


def right_product(left, right):
    return lax.dot_general(
        left, right, (((1,), (1,)), ((), ())), preferred_element_type=jnp.float32
    )


def product(left, right):
    return jnp.dot(left, right, preferred_element_type=jnp.float32)


def next_on(axis, step):
    return {axis: lax.rem(lax.axis_index(axis) + step, lax.axis_size(axis))}


def greet(sizes):
    barrier = pltpu.get_barrier_semaphore()
    for axis, count in sizes:
        for step in range(1, count):
            pl.semaphore_signal(
                barrier, inc=1, device_id=next_on(axis, step), device_id_type=MESH
            )
    pl.semaphore_wait(barrier, sum(count - 1 for _, count in sizes))


def greet_devices(devices):
    barrier = pltpu.get_barrier_semaphore()
    for device in devices:
        pl.semaphore_signal(barrier, inc=1, device_id=device, device_id_type=MESH)
    pl.semaphore_wait(barrier, len(devices))


def square_peers():
    me = lax.axis_index("rep")
    return me, me + 1 - 2 * lax.rem(me, 2), lax.rem(me + 2, 4)


def slot_of(peer, me):
    return lax.rem(peer - me + 4, 4)


def start_copy(source, target, sent, received, device):
    copy = pltpu.make_async_remote_copy(
        src_ref=source,
        dst_ref=target,
        send_sem=sent,
        recv_sem=received,
        device_id=device,
        device_id_type=MESH,
    )
    copy.start()
    return copy


def by_rows(rows, update, base=0):
    size = next((size for size in (32, 16) if rows % size == 0), rows)

    def step(index, carry):
        update(pl.ds(pl.multiple_of(base + index * size, 16), size))
        return carry

    lax.fori_loop(0, rows // size, step, 0)


def call_kernel(kernel, name, out_shape, scratch, operands, micros):
    return pl.pallas_call(
        kernel,
        out_shape=out_shape,
        in_specs=[pl.BlockSpec(memory_space=pltpu.VMEM)] * len(operands),
        out_specs=pl.BlockSpec(memory_space=pltpu.VMEM),
        scratch_shapes=scratch,
        compiler_params=pltpu.CompilerParams(
            collective_id=name, has_side_effects=True, vmem_limit_bytes=40 * 1024 * 1024
        ),
        cost_estimate=pl.CostEstimate(
            flops=0, bytes_accessed=int(micros * FAST_BYTES_PER_US), transcendentals=0
        ),
    )(*operands)


def ring_gather_kernel(axis, count, x_ref, out_ref, sent, received):
    greet(((axis, count),))
    copies = [
        start_copy(
            x_ref,
            out_ref.at[count - step],
            sent.at[step],
            received.at[count - step],
            next_on(axis, step),
        )
        for step in range(1, count)
    ]
    out_ref[0] = x_ref[...]
    for copy in copies:
        copy.wait()


def ring_gather(values, axis, name, micros):
    count = lax.axis_size(axis)
    if count == 1:
        return values[None]
    return call_kernel(
        functools.partial(ring_gather_kernel, axis, count),
        name,
        jax.ShapeDtypeStruct((count, *values.shape), values.dtype),
        [pltpu.SemaphoreType.DMA((count,)), pltpu.SemaphoreType.DMA((count,))],
        (values,),
        micros,
    )


def ring_scatter_kernel(axis, count, far_ref, near_ref, out_ref, arrived, sent, received):
    greet(((axis, count),))
    copies = [
        start_copy(
            far_ref.at[step - 1],
            arrived.at[step - 1],
            sent.at[step],
            received.at[step],
            next_on(axis, step),
        )
        for step in range(1, count)
    ]
    for copy in copies:
        copy.wait()

    def add(some):
        total = near_ref[some, :]
        for step in range(1, count):
            total = total + arrived[step - 1, some, :].astype(jnp.float32)
        out_ref[some, :] = total

    by_rows(near_ref.shape[0], add)


def ring_scatter(far, near, axis, name, micros):
    count = lax.axis_size(axis)
    if count == 1:
        return near
    return call_kernel(
        functools.partial(ring_scatter_kernel, axis, count),
        name,
        jax.ShapeDtypeStruct(near.shape, jnp.float32),
        [
            pltpu.VMEM(far.shape, far.dtype),
            pltpu.SemaphoreType.DMA((count,)),
            pltpu.SemaphoreType.DMA((count,)),
        ],
        (far, near),
        micros,
    )


def plane_gather_kernel(reps, cores, x_ref, out_ref, sent, received, sent_on, received_on):
    greet((("rep", reps), ("tp", cores)))
    copies = [
        start_copy(
            x_ref,
            out_ref.at[0, reps - step],
            sent.at[step],
            received.at[reps - step],
            next_on("rep", step),
        )
        for step in range(1, reps)
    ]
    passed = []

    def pass_on(source, slot):
        for step in range(1, cores):
            passed.append(
                start_copy(
                    source,
                    out_ref.at[cores - step, slot],
                    sent_on.at[step, slot],
                    received_on.at[cores - step, slot],
                    next_on("tp", step),
                )
            )

    pass_on(x_ref, 0)
    out_ref[0, 0] = x_ref[...]
    for copy, step in zip(copies, range(1, reps)):
        copy.wait_recv()
        pass_on(out_ref.at[0, reps - step], reps - step)
    for copy in copies:
        copy.wait_send()
    for copy in passed:
        copy.wait()


def square_gather_kernel(cores, x_ref, out_ref, sent, received, sent_on, received_on):
    me, beside, above = square_peers()
    ways = {"beside": {"rep": beside}, "above": {"rep": above}}
    greet_devices(list(ways.values()) + [next_on("tp", step) for step in range(1, cores)])
    half = x_ref.shape[0] // 2
    low, high = pl.ds(0, half), pl.ds(half, half)
    by_side = start_copy(
        x_ref, out_ref.at[0, slot_of(me, beside)], sent.at[0], received.at[0], ways["beside"]
    )
    by_top = start_copy(
        x_ref, out_ref.at[0, slot_of(me, above)], sent.at[1], received.at[1], ways["above"]
    )
    passed = []

    def pass_on(source, slot, role):
        for step in range(1, cores):
            passed.append(
                start_copy(
                    source,
                    out_ref.at[cores - step, slot],
                    sent_on.at[step, role],
                    received_on.at[cores - step, role],
                    next_on("tp", step),
                )
            )

    pass_on(x_ref, 0, 0)
    out_ref[0, 0] = x_ref[...]
    side_slot, top_slot = slot_of(beside, me), slot_of(above, me)
    by_side.wait_recv()
    upward = start_copy(
        out_ref.at[0, side_slot, low],
        out_ref.at[0, slot_of(beside, above), low],
        sent.at[2],
        received.at[2],
        ways["above"],
    )
    pass_on(out_ref.at[0, side_slot], side_slot, 1)
    by_top.wait_recv()
    sideward = start_copy(
        out_ref.at[0, top_slot, high],
        out_ref.at[0, slot_of(above, beside), high],
        sent.at[3],
        received.at[3],
        ways["beside"],
    )
    pass_on(out_ref.at[0, top_slot], top_slot, 2)
    upward.wait_recv()
    sideward.wait_recv()
    far_slot = 4 - side_slot
    pass_on(out_ref.at[0, far_slot], far_slot, 3)
    for copy in (by_side, by_top, upward, sideward):
        copy.wait_send()
    for copy in passed:
        copy.wait()


def in_square(reps, rows):
    return reps == 4 and rows % 32 == 0


def plane_gather(rows):
    reps, cores = lax.axis_size("rep"), lax.axis_size("tp")
    gathered = call_kernel(
        (
            functools.partial(square_gather_kernel, cores)
            if in_square(reps, rows.shape[0])
            else functools.partial(plane_gather_kernel, reps, cores)
        ),
        1,
        jax.ShapeDtypeStruct((cores, reps, *rows.shape), rows.dtype),
        [
            pltpu.SemaphoreType.DMA((reps,)),
            pltpu.SemaphoreType.DMA((reps,)),
            pltpu.SemaphoreType.DMA((cores, reps)),
            pltpu.SemaphoreType.DMA((cores, reps)),
        ],
        (rows,),
        30,
    )
    return gathered.reshape(cores * reps * rows.shape[0], rows.shape[1])


def plane_scatter_kernel(
    reps,
    cores,
    far_ref,
    near_ref,
    out_ref,
    arrived,
    staged,
    landed,
    sent,
    received,
    sent_on,
    received_on,
):
    greet((("rep", reps), ("tp", cores)))
    rows = near_ref.shape[1]
    order = list(range(1, reps)) + [0]
    first = {}
    for slot in order:
        for step in range(1, cores):
            first[step, slot] = start_copy(
                far_ref.at[step - 1, slot],
                arrived.at[step - 1, slot],
                sent.at[step, slot],
                received.at[step, slot],
                next_on("tp", step),
            )

    def near_sum(slot, some):
        total = near_ref[slot, some, :]
        for step in range(1, cores):
            total = total + arrived[step - 1, slot, some, :].astype(jnp.float32)
        return total

    second = []
    for slot in order:
        for step in range(1, cores):
            first[step, slot].wait_recv()
        if slot:

            def stage(some, slot=slot):
                staged[slot - 1, some, :] = near_sum(slot, some).astype(jnp.bfloat16)

            by_rows(rows, stage)
            second.append(
                start_copy(
                    staged.at[slot - 1],
                    landed.at[slot - 1],
                    sent_on.at[slot],
                    received_on.at[slot],
                    next_on("rep", slot),
                )
            )
    for copy in first.values():
        copy.wait_send()
    for copy in second:
        copy.wait()

    def finish(some):
        total = near_sum(0, some)
        for slot in range(1, reps):
            total = total + landed[slot - 1, some, :].astype(jnp.float32)
        out_ref[some, :] = total

    by_rows(rows, finish)


def square_scatter_kernel(
    cores,
    far_ref,
    near_ref,
    out_ref,
    arrived,
    staged,
    landed,
    crossed,
    sent,
    received,
    sent_on,
    received_on,
):
    me, beside, above = square_peers()
    ways = {"beside": {"rep": beside}, "above": {"rep": above}}
    greet_devices(list(ways.values()) + [next_on("tp", step) for step in range(1, cores)])
    half = near_ref.shape[1] // 2
    low, high = pl.ds(0, half), pl.ds(half, half)
    side_slot, top_slot = slot_of(beside, me), slot_of(above, me)
    slots = (4 - side_slot, side_slot, top_slot, 0)
    first = {}
    for role, slot in enumerate(slots):
        for step in range(1, cores):
            first[role, step] = start_copy(
                far_ref.at[step - 1, slot],
                arrived.at[step - 1, role],
                sent.at[step, role],
                received.at[step, role],
                next_on("tp", step),
            )

    def near_sum(role, some):
        total = near_ref[slots[role], some, :]
        for step in range(1, cores):
            total = total + arrived[step - 1, role, some, :].astype(jnp.float32)
        return total

    def await_role(role):
        for step in range(1, cores):
            first[role, step].wait_recv()

    def stage(role, base, extra=None):
        def fill(some):
            total = near_sum(role, some)
            if extra is not None:
                inner = pl.ds(some.start - base, some.size)
                total = total + crossed[extra, inner, :].astype(jnp.float32)
            staged[role, some, :] = total.astype(jnp.bfloat16)

        by_rows(half, fill, base)

    def send(role, rows, target, index, way):
        return start_copy(
            staged.at[role, rows], target, sent_on.at[index], received_on.at[index], ways[way]
        )

    await_role(0)
    stage(0, 0)
    corner_low = send(0, low, crossed.at[0], 0, "beside")
    stage(0, half)
    corner_high = send(0, high, crossed.at[1], 1, "above")
    await_role(1)
    stage(1, 0)
    side_low = send(1, low, landed.at[0, low], 2, "beside")
    await_role(2)
    stage(2, half)
    top_high = send(2, high, landed.at[1, high], 3, "above")
    corner_low.wait_recv()
    stage(2, 0, 0)
    top_low = send(2, low, landed.at[1, low], 4, "above")
    corner_high.wait_recv()
    stage(1, half, 1)
    side_high = send(1, high, landed.at[0, high], 5, "beside")
    await_role(3)
    for copy in (side_low, top_high, top_low, side_high):
        copy.wait_recv()

    def finish(some):
        total = near_sum(3, some)
        for way in range(2):
            total = total + landed[way, some, :].astype(jnp.float32)
        out_ref[some, :] = total

    by_rows(near_ref.shape[1], finish)
    for copy in (corner_low, corner_high, side_low, top_high, top_low, side_high):
        copy.wait_send()
    for copy in first.values():
        copy.wait_send()


def plane_scatter(far, near):
    reps, cores = lax.axis_size("rep"), lax.axis_size("tp")
    rows = near.shape[0] // reps
    far = far.reshape(cores - 1, reps, rows, far.shape[1])
    near = near.reshape(reps, rows, near.shape[1])
    if in_square(reps, rows):
        return call_kernel(
            functools.partial(square_scatter_kernel, cores),
            2,
            jax.ShapeDtypeStruct(near.shape[1:], jnp.float32),
            [
                pltpu.VMEM(far.shape, jnp.bfloat16),
                pltpu.VMEM((3, *near.shape[1:]), jnp.bfloat16),
                pltpu.VMEM((2, *near.shape[1:]), jnp.bfloat16),
                pltpu.VMEM((2, rows // 2, near.shape[2]), jnp.bfloat16),
                pltpu.SemaphoreType.DMA((cores, 4)),
                pltpu.SemaphoreType.DMA((cores, 4)),
                pltpu.SemaphoreType.DMA((6,)),
                pltpu.SemaphoreType.DMA((6,)),
            ],
            (far, near),
            28,
        )
    return call_kernel(
        functools.partial(plane_scatter_kernel, reps, cores),
        2,
        jax.ShapeDtypeStruct(near.shape[1:], jnp.float32),
        [
            pltpu.VMEM(far.shape, jnp.bfloat16),
            pltpu.VMEM((reps - 1, *near.shape[1:]), jnp.bfloat16),
            pltpu.VMEM((reps - 1, *near.shape[1:]), jnp.bfloat16),
            pltpu.SemaphoreType.DMA((cores, reps)),
            pltpu.SemaphoreType.DMA((cores, reps)),
            pltpu.SemaphoreType.DMA((reps,)),
            pltpu.SemaphoreType.DMA((reps,)),
        ],
        (far, near),
        35,
    )


def weight_gather_kernel(
    shards, reps, w_ref, out_ref, sent, received, sent_on, received_on
):
    greet((("shard", shards), ("rep", reps)))
    place = lax.axis_index("shard")
    replica = lax.axis_index("rep")
    copies = [
        start_copy(
            w_ref.at[replica],
            out_ref.at[place, replica],
            sent.at[step],
            received.at[step],
            next_on("shard", step),
        )
        for step in range(1, shards)
    ]
    out_ref[place] = w_ref[...]
    passed = []
    for step in range(1, shards):
        copies[step - 1].wait_recv()
        source = out_ref.at[lax.rem(place + shards - step, shards), replica]
        for far in range(1, reps):
            passed.append(
                start_copy(
                    source,
                    source,
                    sent_on.at[step, far],
                    received_on.at[step, far],
                    next_on("rep", far),
                )
            )
    for copy in copies:
        copy.wait_send()
    for copy in passed:
        copy.wait()


def weight_gather(weight):
    shards, reps = lax.axis_size("shard"), lax.axis_size("rep")
    depth, columns = weight.shape
    parts = weight.reshape(reps, depth // reps, columns)
    gathered = call_kernel(
        functools.partial(weight_gather_kernel, shards, reps),
        9,
        jax.ShapeDtypeStruct((shards, *parts.shape), weight.dtype),
        [
            pltpu.SemaphoreType.DMA((shards,)),
            pltpu.SemaphoreType.DMA((shards,)),
            pltpu.SemaphoreType.DMA((shards, reps)),
            pltpu.SemaphoreType.DMA((shards, reps)),
        ],
        (parts,),
        50,
    )
    return gathered.reshape(shards * depth, columns)


def gradient_sum_kernel(
    shards,
    reps,
    grad_ref,
    out_ref,
    arrived,
    staged,
    landed,
    summed,
    sent,
    received,
    sent_far,
    received_far,
    sent_on,
    received_on,
):
    greet((("shard", shards), ("rep", reps)))
    place = lax.axis_index("shard")
    replica = lax.axis_index("rep")
    rows = grad_ref.shape[2]
    order = list(range(1, shards)) + [0]
    first = {}
    for step in order:
        target = lax.rem(place + step, shards)
        for far in range(1, reps):
            first[step, far] = start_copy(
                grad_ref.at[target, lax.rem(replica + far, reps)],
                arrived.at[far - 1, step],
                sent.at[step, far],
                received.at[step, far],
                next_on("rep", far),
            )

    def replica_sum(step, some):
        target = lax.rem(place + step, shards)
        total = grad_ref[target, replica, some, :].astype(jnp.float32)
        for far in range(1, reps):
            total = total + arrived[far - 1, step, some, :].astype(jnp.float32)
        return total

    second = []
    for step in order:
        for far in range(1, reps):
            first[step, far].wait_recv()
        if step:

            def stage(some, step=step):
                staged[step - 1, some, :] = replica_sum(step, some).astype(jnp.bfloat16)

            by_rows(rows, stage)
            second.append(
                start_copy(
                    staged.at[step - 1],
                    landed.at[step - 1],
                    sent_far.at[step],
                    received_far.at[step],
                    next_on("shard", step),
                )
            )
    for copy in second:
        copy.wait()

    def finish(some):
        total = replica_sum(0, some)
        for step in range(1, shards):
            total = total + landed[step - 1, some, :].astype(jnp.float32)
        summed[some, :] = total.astype(jnp.bfloat16)

    by_rows(rows, finish)
    third = [
        start_copy(
            summed,
            out_ref.at[replica],
            sent_on.at[far],
            received_on.at[far],
            next_on("rep", far),
        )
        for far in range(1, reps)
    ]
    out_ref[replica] = summed[...]
    for copy in first.values():
        copy.wait_send()
    for copy in third:
        copy.wait()


def gradient_sum(grad):
    shards, reps = lax.axis_size("shard"), lax.axis_size("rep")
    columns = grad.shape[1]
    depth = grad.shape[0] // shards
    piece = (depth // reps, columns)
    summed = call_kernel(
        functools.partial(gradient_sum_kernel, shards, reps),
        10,
        jax.ShapeDtypeStruct((reps, *piece), grad.dtype),
        [
            pltpu.VMEM((reps - 1, shards, *piece), grad.dtype),
            pltpu.VMEM((shards - 1, *piece), grad.dtype),
            pltpu.VMEM((shards - 1, *piece), grad.dtype),
            pltpu.VMEM(piece, grad.dtype),
            pltpu.SemaphoreType.DMA((shards, reps)),
            pltpu.SemaphoreType.DMA((shards, reps)),
            pltpu.SemaphoreType.DMA((shards,)),
            pltpu.SemaphoreType.DMA((shards,)),
            pltpu.SemaphoreType.DMA((reps,)),
            pltpu.SemaphoreType.DMA((reps,)),
        ],
        (grad.reshape(shards, reps, *piece),),
        90,
    )
    return summed.reshape(depth, columns)


def sum_kernel(sizes, x_ref, out_ref, *scratch):
    greet(sizes)
    held = x_ref
    for place, (axis, count) in enumerate(sizes):
        total_ref, arrived, sent, received = scratch[4 * place : 4 * place + 4]
        copies = [
            start_copy(
                held, arrived.at[step - 1], sent.at[step], received.at[step], next_on(axis, step)
            )
            for step in range(1, count)
        ]
        for copy in copies:
            copy.wait()
        total = held[...]
        for step in range(1, count):
            total = total + arrived[step - 1]
        total_ref[...] = total
        held = total_ref
    out_ref[...] = held[...]


def sum_everywhere(values, axes, name):
    sizes = tuple((axis, lax.axis_size(axis)) for axis in axes)
    scratch = []
    for _, count in sizes:
        scratch.extend(
            [
                pltpu.VMEM(values.shape, jnp.float32),
                pltpu.VMEM((max(count - 1, 1), *values.shape), jnp.float32),
                pltpu.SemaphoreType.DMA((count,)),
                pltpu.SemaphoreType.DMA((count,)),
            ]
        )
    return call_kernel(
        functools.partial(sum_kernel, sizes),
        name,
        jax.ShapeDtypeStruct(values.shape, jnp.float32),
        scratch,
        (values,),
        8,
    )


def peer_pairs(count, step):
    if count & (count - 1) == 0:
        return [(i, i ^ step) for i in range(count)]
    return [((i + step) % count, i) for i in range(count)]


def replica_blocks(part):
    count = lax.axis_size("rep")
    me = lax.axis_index("rep")
    blocks = [part]
    for step in range(1, count):
        blocks.append(lax.ppermute(part, "rep", peer_pairs(count, step)))
    held = jnp.stack(blocks)
    places = []
    for index in range(count):
        if count & (count - 1) == 0:
            slot = lax.bitwise_xor(jnp.int32(index), me)
        else:
            slot = lax.rem(index - me + count, count)
        places.append(lax.dynamic_index_in_dim(held, slot, 0, keepdims=False))
    return places


def rolled(values, shift, dim):
    extent = values.shape[dim]
    return lax.dynamic_slice_in_dim(
        jnp.concatenate([values, values], axis=dim), shift, extent, axis=dim
    )


def gathered(weight):
    return lax.all_gather(weight, "shard", axis=0, tiled=True)


def scattered(grad, axes="shard"):
    return lax.psum_scatter(grad, axes, scatter_dimension=0, tiled=True)


def join_blocks(blocks, width):
    block = blocks[0].shape[-1]
    parts = []
    for index, part in enumerate(blocks):
        skip = max(index * block - (width - block), 0)
        if skip < block:
            parts.append(part[..., skip:])
    return jnp.concatenate(parts, axis=-1).astype(jnp.float32)


def body(
    x_in,
    query_key_value_weight,
    qkv_bias,
    output_weight,
    feedforward_entry_matrix,
    down_weight,
    norm_gains,
    piece_starts,
    seq_lengths,
    grad_out,
):
    seqs, span, width = x_in.shape
    shards = lax.axis_size("shard")
    place = lax.axis_index("shard")
    cores = lax.axis_size("tp")
    core = lax.axis_index("tp")
    reps = lax.axis_size("rep")
    length = span * shards
    half = span // cores
    rows = seqs * span
    own_rows = seqs * half
    depth = width // shards
    group_index = QUERY_HEADS // KEY_VALUE_HEADS
    joined_width = query_key_value_weight.shape[2]
    local_groups = joined_width // ((group_index + 2) * HEAD_SIZE)
    heads_width = output_weight.shape[2]
    hidden_width = down_weight.shape[2]
    block = -(-hidden_width // (reps * LANES)) * LANES
    first_owned = lax.axis_index("rep") * block
    first_unit = jnp.minimum(first_owned, hidden_width - block)
    owned = first_unit + jnp.arange(block, dtype=jnp.int32) >= first_owned
    root = math.sqrt(HEAD_SIZE)
    inner_pos = rolled(jnp.arange(span, dtype=jnp.int32), core * half, 0)
    own_pos = place * span + inner_pos
    all_pos = jnp.concatenate(
        [lax.rem(place + step, shards) * span + inner_pos for step in range(shards)]
    )
    cosine, sine = rope_tables(own_pos)
    cos_query = cosine[None, :, None, None, :]
    sin_query = sine[None, :, None, None, :]
    cos_key = cosine[None, :, None, :]
    sin_key = sine[None, :, None, :]
    own_ids = piece_ids(jnp.broadcast_to(own_pos, (seqs, span)), piece_starts)
    all_ids = piece_ids(jnp.broadcast_to(all_pos, (seqs, length)), piece_starts)
    same_piece = (own_ids[:, :, None] == all_ids[:, None, :]) & (own_ids[:, :, None] > 0)
    seen = (all_pos[None, None, :] < seq_lengths[:, None, None]) & (
        (all_pos[None, None, :] <= own_pos[None, :, None]) | same_piece
    )

    def own_block(weight):
        part = lax.dynamic_slice_in_dim(weight, first_unit, block, axis=weight.ndim - 1)
        return lax.optimization_barrier(jnp.where(owned, part, jnp.zeros_like(part)))

    def core_gather(values, name):
        tall = ring_gather(values, "tp", name, 6).reshape(cores, seqs, half, -1)
        return jnp.moveaxis(tall, 0, 1).reshape(rows, -1)

    def core_scatter(values):
        blocks = jnp.moveaxis(values.reshape(seqs, cores, half, -1), 1, 0)
        blocks = blocks.reshape(cores, own_rows, -1)
        return ring_scatter(blocks[1:].astype(jnp.bfloat16), blocks[0], "tp", 4, 8)

    gains_all = norm_gains.astype(jnp.float32)
    x_tall = rolled(x_in, core * half, 1).astype(jnp.float32)
    residual_state = x_tall[:, :half].reshape(own_rows, width)
    x_tall = x_tall.reshape(rows, width)
    first_normed = (x_tall * norm_scale(x_tall) * gains_all[0, 0]).astype(jnp.bfloat16)
    saved = []
    entry_blocks = own_block(feedforward_entry_matrix)
    down_blocks = own_block(down_weight)
    near_rows = reps * own_rows
    both_width = joined_width + heads_width
    full_both = weight_gather(
        jnp.concatenate(
            [
                weight[index]
                for index in range(LAYERS)
                for weight in (query_key_value_weight, output_weight)
            ],
            axis=1,
        )
    )
    for index in range(LAYERS):
        start = index * both_width
        full_qkv = full_both[:, start : start + joined_width]
        full_out = full_both[:, start + joined_width : start + both_width]
        part_entry = gathered(entry_blocks[index].reshape(depth, 2 * block))
        part_down = gathered(down_blocks[index])
        gains = gains_all[index]
        scale_one = norm_scale(residual_state)
        if index:
            first_normed = core_gather(
                (residual_state * scale_one * gains[0]).astype(jnp.bfloat16), 3
            )
        joined_output = product(first_normed, full_qkv) + qkv_bias[index].astype(jnp.float32)
        joined_output = joined_output.reshape(seqs, span, local_groups, group_index + 2, HEAD_SIZE)
        query_rows = rotate(joined_output[:, :, :, :group_index], cos_query, sin_query).astype(
            jnp.bfloat16
        )
        keys = rotate(joined_output[:, :, :, group_index], cos_key, sin_key).astype(jnp.bfloat16)
        content_entries = joined_output[:, :, :, group_index + 1].astype(jnp.bfloat16)
        pair = jnp.stack([keys, content_entries]).reshape(-1, HEAD_SIZE)
        pair_all = ring_gather(pair, "shard", 5, 12)
        pair_all = pair_all.reshape(shards, 2, seqs, span, local_groups, HEAD_SIZE)
        pair_all = jnp.moveaxis(pair_all, 0, 2).reshape(2, seqs, length, local_groups, HEAD_SIZE)
        keys_all, values_all = pair_all[0], pair_all[1]
        attention_logits = masked_scores(query_rows, keys_all, seen, root)
        log_total = jax.nn.logsumexp(attention_logits, axis=-1, keepdims=True)
        shares = jnp.exp(attention_logits - log_total).astype(jnp.bfloat16)
        mixed_output = jnp.einsum(
            "sgjqk,skgd->sqgjd", shares, values_all, preferred_element_type=jnp.float32
        )
        mixed_output = mixed_output.astype(jnp.bfloat16).reshape(rows, heads_width)
        middle_state = residual_state + core_scatter(right_product(mixed_output, full_out))
        scale_two = norm_scale(middle_state)
        plane_rows = plane_gather((middle_state * scale_two * gains[1]).astype(jnp.bfloat16))
        gate = product(plane_rows, part_entry[:, :block])
        upper = product(plane_rows, part_entry[:, block:])
        hidden_state = (jax.nn.silu(gate) * upper).astype(jnp.bfloat16)
        saved.append(
            (
                residual_state,
                scale_one,
                first_normed,
                query_rows,
                keys_all,
                values_all,
                log_total,
                mixed_output,
                middle_state,
                scale_two,
                plane_rows,
                gate,
                upper,
                hidden_state,
                full_qkv,
                full_out,
                part_entry,
                part_down,
            )
        )
        residual_state = middle_state + plane_scatter(
            right_product(hidden_state[near_rows:], part_down).astype(jnp.bfloat16),
            right_product(hidden_state[:near_rows], part_down),
        )
    out_own = residual_state.astype(jnp.bfloat16)
    grad_tall = rolled(grad_out, core * half, 1)[:, :half]
    flow = grad_tall.astype(jnp.float32).reshape(own_rows, width)
    up_pieces = [None] * LAYERS
    gate_pieces = [None] * LAYERS
    down_pieces = [None] * LAYERS
    qkv_pieces = [None] * LAYERS
    gain_grads = [None] * LAYERS
    bias_grads = [None] * LAYERS
    pending = None
    for index in reversed(range(LAYERS)):
        (
            residual_state,
            scale_one,
            first_normed,
            query_rows,
            keys_all,
            values_all,
            log_total,
            mixed_output,
            middle_state,
            scale_two,
            plane_rows,
            gate,
            upper,
            hidden_state,
            full_qkv,
            full_out,
            part_entry,
            part_down,
        ) = saved[index]
        gains = gains_all[index]
        plane_grad = plane_gather(flow.astype(jnp.bfloat16))
        hidden_grad = product(plane_grad, part_down)
        down_total = left_product(plane_grad, hidden_state)
        hidden_grad, down_total = lax.optimization_barrier((hidden_grad, down_total))
        down_own = scattered(down_total)
        sigmoid = jax.nn.sigmoid(gate)
        gate_grad = hidden_grad * upper * (sigmoid + gate * sigmoid * (1.0 - sigmoid))
        up_grad = hidden_grad * (gate * sigmoid)
        entry_grad = jnp.concatenate([gate_grad, up_grad], axis=1).astype(jnp.bfloat16)
        gate_total = left_product(plane_rows, entry_grad[:, :block])
        up_total = left_product(plane_rows, entry_grad[:, block:])
        entry_grad, gate_total, up_total = lax.optimization_barrier(
            (entry_grad, gate_total, up_total)
        )
        own_parts = (down_own, scattered(gate_total), scattered(up_total))
        far_product = right_product(entry_grad[near_rows:], part_entry).astype(jnp.bfloat16)
        near_product = right_product(entry_grad[:near_rows], part_entry)
        normed_two_grad = plane_scatter(far_product, near_product)
        middle_grad, gain_two = norm_back(middle_state, scale_two, gains[1], normed_two_grad)
        middle_grad = flow + middle_grad
        out_grad = core_gather(middle_grad.astype(jnp.bfloat16), 3)
        mixed_grad = product(out_grad, full_out).astype(jnp.bfloat16)
        mixed_grad, pending = lax.optimization_barrier((mixed_grad, pending))
        if pending is not None:
            down_pieces[index + 1], gate_pieces[index + 1], up_pieces[index + 1], wide = [
                replica_blocks(part) for part in pending
            ]
            qkv_pieces[index + 1] = jnp.concatenate(wide, axis=0).astype(jnp.float32)
        pending = own_parts
        mixed_grad = mixed_grad.reshape(seqs, span, local_groups, group_index, HEAD_SIZE)
        attention_logits = masked_scores(query_rows, keys_all, seen, root)
        exact = jnp.exp(attention_logits - log_total)
        shares = exact.astype(jnp.bfloat16)
        share_grad = jnp.einsum(
            "sqgjd,skgd->sgjqk", mixed_grad, values_all, preferred_element_type=jnp.float32
        )
        centre = jnp.sum(exact * share_grad, axis=-1, keepdims=True)
        score_grad = (exact * (share_grad - centre)).astype(jnp.bfloat16)
        query_grad = (
            jnp.einsum(
                "sgjqk,skgd->sqgjd", score_grad, keys_all, preferred_element_type=jnp.float32
            )
            / root
        )
        key_grad = (
            jnp.einsum(
                "sgjqk,sqgjd->skgd", score_grad, query_rows, preferred_element_type=jnp.float32
            )
            / root
        )
        value_grad = jnp.einsum(
            "sgjqk,sqgjd->skgd", shares, mixed_grad, preferred_element_type=jnp.float32
        )
        pair = jnp.stack([key_grad, value_grad])
        pair = pair.reshape(2, seqs, shards, span, local_groups, HEAD_SIZE)
        pair = jnp.moveaxis(pair, 2, 0).reshape(shards, -1, HEAD_SIZE)
        pair_own = ring_scatter(pair[1:].astype(jnp.bfloat16), pair[0], "shard", 6, 14)
        pair_own = pair_own.reshape(2, seqs, span, local_groups, HEAD_SIZE)
        key_own, value_own = pair_own[0], pair_own[1]
        unrotated_asks = rotate_back(query_grad, cos_query, sin_query)
        key_raw = rotate_back(key_own, cos_key, sin_key)
        joined_grad = jnp.concatenate(
            [unrotated_asks, key_raw[:, :, :, None], value_own[:, :, :, None]], axis=3
        )
        joined_grad = joined_grad.reshape(rows, joined_width).astype(jnp.bfloat16)
        bias_grads[index] = jnp.sum(joined_grad, axis=0, dtype=jnp.float32)
        normed_one_grad = core_scatter(right_product(joined_grad, full_qkv))
        input_grad, gain_one = norm_back(residual_state, scale_one, gains[0], normed_one_grad)
        gain_grads[index] = jnp.stack([gain_one, gain_two])
        flow = middle_grad + input_grad
        both = jnp.concatenate(
            [left_product(first_normed, joined_grad), left_product(out_grad, mixed_output)], axis=1
        )
        if index:
            wide = both.reshape(shards, reps, depth // reps, both_width).swapaxes(0, 1)
            wide = scattered(wide.reshape(shards * depth, both_width), "rep")
            pending = (*pending, scattered(wide))
        else:
            both, *ready = lax.optimization_barrier((both, *pending[:2]))
            pending = (*ready, pending[2])
            both_sum = gradient_sum(both)
            qkv_pieces[index] = both_sum.astype(jnp.float32)
    down_pieces[0], gate_pieces[0], up_pieces[0] = [replica_blocks(part) for part in pending]
    grad_gate_up = []
    for gates, ups in zip(gate_pieces, up_pieces):
        pairs = [
            lax.optimization_barrier(jnp.concatenate(pair, axis=1)).reshape(depth, 2, block)
            for pair in zip(gates, ups)
        ]
        grad_gate_up.append(join_blocks(pairs, hidden_width))
    grad_gate_up = jnp.stack(grad_gate_up)
    grad_down = jnp.stack([join_blocks(blocks, hidden_width) for blocks in down_pieces])
    grad_both = jnp.stack(qkv_pieces)
    grad_qkv = grad_both[:, :, :joined_width]
    grad_out_proj = grad_both[:, :, joined_width:]
    bias = jnp.stack(bias_grads)
    slots = jnp.arange(cores, dtype=jnp.int32)[:, None, None] == core
    bias_slots = jnp.where(slots, bias[None], 0.0)
    gains_own = jnp.stack(gain_grads)
    small = jnp.concatenate([gains_own.reshape(-1), bias_slots.reshape(-1)])
    small, _ = lax.optimization_barrier((small, both_sum))
    small = sum_everywhere(small.reshape(-1, LANES), ("rep", "shard", "tp"), 7).reshape(-1)
    gains_total = small[: gains_own.size].reshape(gains_own.shape)
    bias_slots = small[gains_own.size :].reshape(bias_slots.shape)
    bias_total = lax.dynamic_index_in_dim(bias_slots, core, 0, keepdims=False)

    def whole_rows(values, name):
        tall = core_gather(values, name).reshape(seqs, span, width)
        return rolled(tall, lax.rem(cores - core, cores) * half, 1)

    return (
        whole_rows(out_own, 3),
        whole_rows(flow, 8),
        grad_qkv,
        bias_total,
        grad_out_proj,
        grad_gate_up,
        grad_down,
        gains_total,
    )


def solution(mesh):
    return jax.shard_map(
        body,
        mesh=mesh,
        in_specs=(
            P("rep", "shard", None),
            P(None, "shard", "tp"),
            P(None, "tp"),
            P(None, "shard", "tp"),
            P(None, "shard", None, "tp"),
            P(None, "shard", "tp"),
            P(),
            P("rep", None),
            P("rep"),
            P("rep", "shard", None),
        ),
        out_specs=(
            P("rep", "shard", None),
            P("rep", "shard", None),
            P(None, "shard", "tp"),
            P(None, "tp"),
            P(None, "shard", "tp"),
            P(None, "shard", None, "tp"),
            P(None, "shard", "tp"),
            P(),
        ),
        check_vma=False,
    )
```

```python
import functools
import math

import jax
import jax.numpy as jnp
from jax import lax
from jax.experimental import pallas as pl
from jax.experimental.pallas import tpu as pltpu
from jax.sharding import PartitionSpec as P


QUERY_HEADS = 12
KEY_VALUE_HEADS = 2
HEAD_SIZE = 128
LAYERS = 2
PIECE = 256
PIECES = 2
LANES = 128


EPS = 1e-06
THETA = 1000000.0


def rope_tables(positions):
    freq = jnp.exp(
        jnp.arange(HEAD_SIZE // 2, dtype=jnp.float32) * (-2.0 * math.log(THETA) / HEAD_SIZE)
    )
    angle = positions.astype(jnp.float32)[:, None] * freq[None, :]
    angle = jnp.concatenate([angle, angle], axis=1)
    return (jnp.cos(angle), jnp.sin(angle))


def rotate(content_entries, cosine, sine):
    half = content_entries.shape[-1] // 2
    turned = jnp.concatenate([-content_entries[..., half:], content_entries[..., :half]], axis=-1)
    return content_entries * cosine + turned * sine


def rotate_back(grads, cosine, sine):
    half = grads.shape[-1] // 2
    shifted = grads * sine
    return grads * cosine + jnp.concatenate([shifted[..., half:], -shifted[..., :half]], axis=-1)


def piece_ids(positions, starts):
    inside = (positions[..., :, None] >= starts[..., None, :]) & (
        positions[..., :, None] < starts[..., None, :] + PIECE
    )
    labels = jnp.arange(1, PIECES + 1, dtype=jnp.int32)
    return jnp.sum(jnp.where(inside, labels, 0), axis=-1)


def norm_scale(content_entries):
    return lax.rsqrt(jnp.mean(content_entries * content_entries, axis=-1, keepdims=True) + EPS)


def norm_back(content_entries, scale, gain, grad_normed):
    inner = jnp.mean(grad_normed * gain * content_entries, axis=-1, keepdims=True)
    grad_values = scale * gain * grad_normed - content_entries * (scale * scale * scale) * inner
    gain_grad = jnp.sum(grad_normed * content_entries * scale, axis=0)
    return (grad_values, gain_grad)


def masked_scores(query_rows, keys_all, seen, root):
    raw = (
        jnp.einsum("sqgjd,skgd->sgjqk", query_rows, keys_all, preferred_element_type=jnp.float32)
        / root
    )
    return jnp.where(seen[:, None, None], raw, -1e30)


MESH = pl.DeviceIdType.MESH
FAST_BYTES_PER_US = 3_000_000


def left_product(left, right):
    return lax.dot_general(
        left, right, (((0,), (0,)), ((), ())), preferred_element_type=jnp.float32
    ).astype(jnp.bfloat16)


def right_product(left, right):
    return lax.dot_general(
        left, right, (((1,), (1,)), ((), ())), preferred_element_type=jnp.float32
    )


def product(left, right):
    return jnp.dot(left, right, preferred_element_type=jnp.float32)


def next_on(axis, step):
    return {axis: lax.rem(lax.axis_index(axis) + step, lax.axis_size(axis))}


def greet(sizes):
    barrier = pltpu.get_barrier_semaphore()
    for axis, count in sizes:
        for step in range(1, count):
            pl.semaphore_signal(
                barrier, inc=1, device_id=next_on(axis, step), device_id_type=MESH
            )
    pl.semaphore_wait(barrier, sum(count - 1 for _, count in sizes))


def greet_devices(devices):
    barrier = pltpu.get_barrier_semaphore()
    for device in devices:
        pl.semaphore_signal(barrier, inc=1, device_id=device, device_id_type=MESH)
    pl.semaphore_wait(barrier, len(devices))


def square_peers():
    me = lax.axis_index("rep")
    return me, me + 1 - 2 * lax.rem(me, 2), lax.rem(me + 2, 4)


def slot_of(peer, me):
    return lax.rem(peer - me + 4, 4)


def start_copy(source, target, sent, received, device):
    copy = pltpu.make_async_remote_copy(
        src_ref=source,
        dst_ref=target,
        send_sem=sent,
        recv_sem=received,
        device_id=device,
        device_id_type=MESH,
    )
    copy.start()
    return copy


def by_rows(rows, update, base=0):
    size = next((size for size in (32, 16) if rows % size == 0), rows)

    def step(index, carry):
        update(pl.ds(pl.multiple_of(base + index * size, 16), size))
        return carry

    lax.fori_loop(0, rows // size, step, 0)


def call_kernel(kernel, name, out_shape, scratch, operands, micros):
    return pl.pallas_call(
        kernel,
        out_shape=out_shape,
        in_specs=[pl.BlockSpec(memory_space=pltpu.VMEM)] * len(operands),
        out_specs=pl.BlockSpec(memory_space=pltpu.VMEM),
        scratch_shapes=scratch,
        compiler_params=pltpu.CompilerParams(
            collective_id=name, has_side_effects=True, vmem_limit_bytes=40 * 1024 * 1024
        ),
        cost_estimate=pl.CostEstimate(
            flops=0, bytes_accessed=int(micros * FAST_BYTES_PER_US), transcendentals=0
        ),
    )(*operands)


def ring_gather_kernel(axis, count, x_ref, out_ref, sent, received):
    greet(((axis, count),))
    copies = [
        start_copy(
            x_ref,
            out_ref.at[count - step],
            sent.at[step],
            received.at[count - step],
            next_on(axis, step),
        )
        for step in range(1, count)
    ]
    out_ref[0] = x_ref[...]
    for copy in copies:
        copy.wait()


def ring_gather(values, axis, name, micros):
    count = lax.axis_size(axis)
    if count == 1:
        return values[None]
    return call_kernel(
        functools.partial(ring_gather_kernel, axis, count),
        name,
        jax.ShapeDtypeStruct((count, *values.shape), values.dtype),
        [pltpu.SemaphoreType.DMA((count,)), pltpu.SemaphoreType.DMA((count,))],
        (values,),
        micros,
    )


def ring_scatter_kernel(axis, count, far_ref, near_ref, out_ref, arrived, sent, received):
    greet(((axis, count),))
    copies = [
        start_copy(
            far_ref.at[step - 1],
            arrived.at[step - 1],
            sent.at[step],
            received.at[step],
            next_on(axis, step),
        )
        for step in range(1, count)
    ]
    for copy in copies:
        copy.wait()

    def add(some):
        total = near_ref[some, :]
        for step in range(1, count):
            total = total + arrived[step - 1, some, :].astype(jnp.float32)
        out_ref[some, :] = total

    by_rows(near_ref.shape[0], add)


def ring_scatter(far, near, axis, name, micros):
    count = lax.axis_size(axis)
    if count == 1:
        return near
    return call_kernel(
        functools.partial(ring_scatter_kernel, axis, count),
        name,
        jax.ShapeDtypeStruct(near.shape, jnp.float32),
        [
            pltpu.VMEM(far.shape, far.dtype),
            pltpu.SemaphoreType.DMA((count,)),
            pltpu.SemaphoreType.DMA((count,)),
        ],
        (far, near),
        micros,
    )


def plane_gather_kernel(reps, cores, x_ref, out_ref, sent, received, sent_on, received_on):
    greet((("rep", reps), ("tp", cores)))
    copies = [
        start_copy(
            x_ref,
            out_ref.at[0, reps - step],
            sent.at[step],
            received.at[reps - step],
            next_on("rep", step),
        )
        for step in range(1, reps)
    ]
    passed = []

    def pass_on(source, slot):
        for step in range(1, cores):
            passed.append(
                start_copy(
                    source,
                    out_ref.at[cores - step, slot],
                    sent_on.at[step, slot],
                    received_on.at[cores - step, slot],
                    next_on("tp", step),
                )
            )

    pass_on(x_ref, 0)
    out_ref[0, 0] = x_ref[...]
    for copy, step in zip(copies, range(1, reps)):
        copy.wait_recv()
        pass_on(out_ref.at[0, reps - step], reps - step)
    for copy in copies:
        copy.wait_send()
    for copy in passed:
        copy.wait()


def square_gather_kernel(cores, x_ref, out_ref, sent, received, sent_on, received_on):
    me, beside, above = square_peers()
    ways = {"beside": {"rep": beside}, "above": {"rep": above}}
    greet_devices(list(ways.values()) + [next_on("tp", step) for step in range(1, cores)])
    half = x_ref.shape[0] // 2
    low, high = pl.ds(0, half), pl.ds(half, half)
    by_side = start_copy(
        x_ref, out_ref.at[0, slot_of(me, beside)], sent.at[0], received.at[0], ways["beside"]
    )
    by_top = start_copy(
        x_ref, out_ref.at[0, slot_of(me, above)], sent.at[1], received.at[1], ways["above"]
    )
    passed = []

    def pass_on(source, slot, role):
        for step in range(1, cores):
            passed.append(
                start_copy(
                    source,
                    out_ref.at[cores - step, slot],
                    sent_on.at[step, role],
                    received_on.at[cores - step, role],
                    next_on("tp", step),
                )
            )

    pass_on(x_ref, 0, 0)
    out_ref[0, 0] = x_ref[...]
    side_slot, top_slot = slot_of(beside, me), slot_of(above, me)
    by_side.wait_recv()
    upward = start_copy(
        out_ref.at[0, side_slot, low],
        out_ref.at[0, slot_of(beside, above), low],
        sent.at[2],
        received.at[2],
        ways["above"],
    )
    pass_on(out_ref.at[0, side_slot], side_slot, 1)
    by_top.wait_recv()
    sideward = start_copy(
        out_ref.at[0, top_slot, high],
        out_ref.at[0, slot_of(above, beside), high],
        sent.at[3],
        received.at[3],
        ways["beside"],
    )
    pass_on(out_ref.at[0, top_slot], top_slot, 2)
    upward.wait_recv()
    sideward.wait_recv()
    far_slot = 4 - side_slot
    pass_on(out_ref.at[0, far_slot], far_slot, 3)
    for copy in (by_side, by_top, upward, sideward):
        copy.wait_send()
    for copy in passed:
        copy.wait()


def in_square(reps, rows):
    return reps == 4 and rows % 32 == 0


def plane_gather(rows):
    reps, cores = lax.axis_size("rep"), lax.axis_size("tp")
    gathered = call_kernel(
        (
            functools.partial(square_gather_kernel, cores)
            if in_square(reps, rows.shape[0])
            else functools.partial(plane_gather_kernel, reps, cores)
        ),
        1,
        jax.ShapeDtypeStruct((cores, reps, *rows.shape), rows.dtype),
        [
            pltpu.SemaphoreType.DMA((reps,)),
            pltpu.SemaphoreType.DMA((reps,)),
            pltpu.SemaphoreType.DMA((cores, reps)),
            pltpu.SemaphoreType.DMA((cores, reps)),
        ],
        (rows,),
        30,
    )
    return gathered.reshape(cores * reps * rows.shape[0], rows.shape[1])


def plane_scatter_kernel(
    reps,
    cores,
    far_ref,
    near_ref,
    out_ref,
    arrived,
    staged,
    landed,
    sent,
    received,
    sent_on,
    received_on,
):
    greet((("rep", reps), ("tp", cores)))
    rows = near_ref.shape[1]
    order = list(range(1, reps)) + [0]
    first = {}
    for slot in order:
        for step in range(1, cores):
            first[step, slot] = start_copy(
                far_ref.at[step - 1, slot],
                arrived.at[step - 1, slot],
                sent.at[step, slot],
                received.at[step, slot],
                next_on("tp", step),
            )

    def near_sum(slot, some):
        total = near_ref[slot, some, :]
        for step in range(1, cores):
            total = total + arrived[step - 1, slot, some, :].astype(jnp.float32)
        return total

    second = []
    for slot in order:
        for step in range(1, cores):
            first[step, slot].wait_recv()
        if slot:

            def stage(some, slot=slot):
                staged[slot - 1, some, :] = near_sum(slot, some).astype(jnp.bfloat16)

            by_rows(rows, stage)
            second.append(
                start_copy(
                    staged.at[slot - 1],
                    landed.at[slot - 1],
                    sent_on.at[slot],
                    received_on.at[slot],
                    next_on("rep", slot),
                )
            )
    for copy in first.values():
        copy.wait_send()
    for copy in second:
        copy.wait()

    def finish(some):
        total = near_sum(0, some)
        for slot in range(1, reps):
            total = total + landed[slot - 1, some, :].astype(jnp.float32)
        out_ref[some, :] = total

    by_rows(rows, finish)


def square_scatter_kernel(
    cores,
    far_ref,
    near_ref,
    out_ref,
    arrived,
    staged,
    landed,
    crossed,
    sent,
    received,
    sent_on,
    received_on,
):
    me, beside, above = square_peers()
    ways = {"beside": {"rep": beside}, "above": {"rep": above}}
    greet_devices(list(ways.values()) + [next_on("tp", step) for step in range(1, cores)])
    half = near_ref.shape[1] // 2
    low, high = pl.ds(0, half), pl.ds(half, half)
    side_slot, top_slot = slot_of(beside, me), slot_of(above, me)
    slots = (4 - side_slot, side_slot, top_slot, 0)
    first = {}
    for role, slot in enumerate(slots):
        for step in range(1, cores):
            first[role, step] = start_copy(
                far_ref.at[step - 1, slot],
                arrived.at[step - 1, role],
                sent.at[step, role],
                received.at[step, role],
                next_on("tp", step),
            )

    def near_sum(role, some):
        total = near_ref[slots[role], some, :]
        for step in range(1, cores):
            total = total + arrived[step - 1, role, some, :].astype(jnp.float32)
        return total

    def await_role(role):
        for step in range(1, cores):
            first[role, step].wait_recv()

    def stage(role, base, extra=None):
        def fill(some):
            total = near_sum(role, some)
            if extra is not None:
                inner = pl.ds(some.start - base, some.size)
                total = total + crossed[extra, inner, :].astype(jnp.float32)
            staged[role, some, :] = total.astype(jnp.bfloat16)

        by_rows(half, fill, base)

    def send(role, rows, target, index, way):
        return start_copy(
            staged.at[role, rows], target, sent_on.at[index], received_on.at[index], ways[way]
        )

    await_role(0)
    stage(0, 0)
    corner_low = send(0, low, crossed.at[0], 0, "beside")
    stage(0, half)
    corner_high = send(0, high, crossed.at[1], 1, "above")
    await_role(1)
    stage(1, 0)
    side_low = send(1, low, landed.at[0, low], 2, "beside")
    await_role(2)
    stage(2, half)
    top_high = send(2, high, landed.at[1, high], 3, "above")
    corner_low.wait_recv()
    stage(2, 0, 0)
    top_low = send(2, low, landed.at[1, low], 4, "above")
    corner_high.wait_recv()
    stage(1, half, 1)
    side_high = send(1, high, landed.at[0, high], 5, "beside")
    await_role(3)
    for copy in (side_low, top_high, top_low, side_high):
        copy.wait_recv()

    def finish(some):
        total = near_sum(3, some)
        for way in range(2):
            total = total + landed[way, some, :].astype(jnp.float32)
        out_ref[some, :] = total

    by_rows(near_ref.shape[1], finish)
    for copy in (corner_low, corner_high, side_low, top_high, top_low, side_high):
        copy.wait_send()
    for copy in first.values():
        copy.wait_send()


def plane_scatter(far, near):
    reps, cores = lax.axis_size("rep"), lax.axis_size("tp")
    rows = near.shape[0] // reps
    far = far.reshape(cores - 1, reps, rows, far.shape[1])
    near = near.reshape(reps, rows, near.shape[1])
    if in_square(reps, rows):
        return call_kernel(
            functools.partial(square_scatter_kernel, cores),
            2,
            jax.ShapeDtypeStruct(near.shape[1:], jnp.float32),
            [
                pltpu.VMEM(far.shape, jnp.bfloat16),
                pltpu.VMEM((3, *near.shape[1:]), jnp.bfloat16),
                pltpu.VMEM((2, *near.shape[1:]), jnp.bfloat16),
                pltpu.VMEM((2, rows // 2, near.shape[2]), jnp.bfloat16),
                pltpu.SemaphoreType.DMA((cores, 4)),
                pltpu.SemaphoreType.DMA((cores, 4)),
                pltpu.SemaphoreType.DMA((6,)),
                pltpu.SemaphoreType.DMA((6,)),
            ],
            (far, near),
            28,
        )
    return call_kernel(
        functools.partial(plane_scatter_kernel, reps, cores),
        2,
        jax.ShapeDtypeStruct(near.shape[1:], jnp.float32),
        [
            pltpu.VMEM(far.shape, jnp.bfloat16),
            pltpu.VMEM((reps - 1, *near.shape[1:]), jnp.bfloat16),
            pltpu.VMEM((reps - 1, *near.shape[1:]), jnp.bfloat16),
            pltpu.SemaphoreType.DMA((cores, reps)),
            pltpu.SemaphoreType.DMA((cores, reps)),
            pltpu.SemaphoreType.DMA((reps,)),
            pltpu.SemaphoreType.DMA((reps,)),
        ],
        (far, near),
        35,
    )


def weight_gather_kernel(
    shards, reps, w_ref, out_ref, sent, received, sent_on, received_on
):
    greet((("shard", shards), ("rep", reps)))
    place = lax.axis_index("shard")
    replica = lax.axis_index("rep")
    copies = [
        start_copy(
            w_ref.at[replica],
            out_ref.at[place, replica],
            sent.at[step],
            received.at[step],
            next_on("shard", step),
        )
        for step in range(1, shards)
    ]
    out_ref[place] = w_ref[...]
    passed = []
    for step in range(1, shards):
        copies[step - 1].wait_recv()
        source = out_ref.at[lax.rem(place + shards - step, shards), replica]
        for far in range(1, reps):
            passed.append(
                start_copy(
                    source,
                    source,
                    sent_on.at[step, far],
                    received_on.at[step, far],
                    next_on("rep", far),
                )
            )
    for copy in copies:
        copy.wait_send()
    for copy in passed:
        copy.wait()


def weight_gather(weight):
    shards, reps = lax.axis_size("shard"), lax.axis_size("rep")
    depth, columns = weight.shape
    parts = weight.reshape(reps, depth // reps, columns)
    gathered = call_kernel(
        functools.partial(weight_gather_kernel, shards, reps),
        9,
        jax.ShapeDtypeStruct((shards, *parts.shape), weight.dtype),
        [
            pltpu.SemaphoreType.DMA((shards,)),
            pltpu.SemaphoreType.DMA((shards,)),
            pltpu.SemaphoreType.DMA((shards, reps)),
            pltpu.SemaphoreType.DMA((shards, reps)),
        ],
        (parts,),
        50,
    )
    return gathered.reshape(shards * depth, columns)


def gradient_sum_kernel(
    shards,
    reps,
    grad_ref,
    out_ref,
    arrived,
    staged,
    landed,
    summed,
    sent,
    received,
    sent_far,
    received_far,
    sent_on,
    received_on,
):
    greet((("shard", shards), ("rep", reps)))
    place = lax.axis_index("shard")
    replica = lax.axis_index("rep")
    rows = grad_ref.shape[2]
    order = list(range(1, shards)) + [0]
    first = {}
    for step in order:
        target = lax.rem(place + step, shards)
        for far in range(1, reps):
            first[step, far] = start_copy(
                grad_ref.at[target, lax.rem(replica + far, reps)],
                arrived.at[far - 1, step],
                sent.at[step, far],
                received.at[step, far],
                next_on("rep", far),
            )

    def replica_sum(step, some):
        target = lax.rem(place + step, shards)
        total = grad_ref[target, replica, some, :].astype(jnp.float32)
        for far in range(1, reps):
            total = total + arrived[far - 1, step, some, :].astype(jnp.float32)
        return total

    second = []
    for step in order:
        for far in range(1, reps):
            first[step, far].wait_recv()
        if step:

            def stage(some, step=step):
                staged[step - 1, some, :] = replica_sum(step, some).astype(jnp.bfloat16)

            by_rows(rows, stage)
            second.append(
                start_copy(
                    staged.at[step - 1],
                    landed.at[step - 1],
                    sent_far.at[step],
                    received_far.at[step],
                    next_on("shard", step),
                )
            )
    for copy in second:
        copy.wait()

    def finish(some):
        total = replica_sum(0, some)
        for step in range(1, shards):
            total = total + landed[step - 1, some, :].astype(jnp.float32)
        summed[some, :] = total.astype(jnp.bfloat16)

    by_rows(rows, finish)
    third = [
        start_copy(
            summed,
            out_ref.at[replica],
            sent_on.at[far],
            received_on.at[far],
            next_on("rep", far),
        )
        for far in range(1, reps)
    ]
    out_ref[replica] = summed[...]
    for copy in first.values():
        copy.wait_send()
    for copy in third:
        copy.wait()


def gradient_sum(grad):
    shards, reps = lax.axis_size("shard"), lax.axis_size("rep")
    columns = grad.shape[1]
    depth = grad.shape[0] // shards
    piece = (depth // reps, columns)
    summed = call_kernel(
        functools.partial(gradient_sum_kernel, shards, reps),
        10,
        jax.ShapeDtypeStruct((reps, *piece), grad.dtype),
        [
            pltpu.VMEM((reps - 1, shards, *piece), grad.dtype),
            pltpu.VMEM((shards - 1, *piece), grad.dtype),
            pltpu.VMEM((shards - 1, *piece), grad.dtype),
            pltpu.VMEM(piece, grad.dtype),
            pltpu.SemaphoreType.DMA((shards, reps)),
            pltpu.SemaphoreType.DMA((shards, reps)),
            pltpu.SemaphoreType.DMA((shards,)),
            pltpu.SemaphoreType.DMA((shards,)),
            pltpu.SemaphoreType.DMA((reps,)),
            pltpu.SemaphoreType.DMA((reps,)),
        ],
        (grad.reshape(shards, reps, *piece),),
        90,
    )
    return summed.reshape(depth, columns)


def sum_kernel(sizes, x_ref, out_ref, *scratch):
    greet(sizes)
    held = x_ref
    for place, (axis, count) in enumerate(sizes):
        total_ref, arrived, sent, received = scratch[4 * place : 4 * place + 4]
        copies = [
            start_copy(
                held, arrived.at[step - 1], sent.at[step], received.at[step], next_on(axis, step)
            )
            for step in range(1, count)
        ]
        for copy in copies:
            copy.wait()
        total = held[...]
        for step in range(1, count):
            total = total + arrived[step - 1]
        total_ref[...] = total
        held = total_ref
    out_ref[...] = held[...]


def sum_everywhere(values, axes, name):
    sizes = tuple((axis, lax.axis_size(axis)) for axis in axes)
    scratch = []
    for _, count in sizes:
        scratch.extend(
            [
                pltpu.VMEM(values.shape, jnp.float32),
                pltpu.VMEM((max(count - 1, 1), *values.shape), jnp.float32),
                pltpu.SemaphoreType.DMA((count,)),
                pltpu.SemaphoreType.DMA((count,)),
            ]
        )
    return call_kernel(
        functools.partial(sum_kernel, sizes),
        name,
        jax.ShapeDtypeStruct(values.shape, jnp.float32),
        scratch,
        (values,),
        8,
    )


def peer_pairs(count, step):
    if count & (count - 1) == 0:
        return [(i, i ^ step) for i in range(count)]
    return [((i + step) % count, i) for i in range(count)]


def from_replicas(part):
    count = lax.axis_size("rep")
    return [part] + [
        lax.ppermute(part, "rep", peer_pairs(count, step)) for step in range(1, count)
    ]


def in_order(blocks):
    count = lax.axis_size("rep")
    me = lax.axis_index("rep")
    held = jnp.stack(blocks)
    places = []
    for index in range(count):
        if count & (count - 1) == 0:
            slot = lax.bitwise_xor(jnp.int32(index), me)
        else:
            slot = lax.rem(index - me + count, count)
        places.append(lax.dynamic_index_in_dim(held, slot, 0, keepdims=False))
    return places


def rolled(values, shift, dim):
    extent = values.shape[dim]
    return lax.dynamic_slice_in_dim(
        jnp.concatenate([values, values], axis=dim), shift, extent, axis=dim
    )


def gathered(weight):
    return lax.all_gather(weight, "shard", axis=0, tiled=True)


def scattered(grad, axes="shard"):
    return lax.psum_scatter(grad, axes, scatter_dimension=0, tiled=True)


def join_blocks(blocks, width):
    block = blocks[0].shape[-1]
    parts = []
    for index, part in enumerate(blocks):
        skip = max(index * block - (width - block), 0)
        if skip < block:
            parts.append(part[..., skip:])
    return jnp.concatenate(parts, axis=-1).astype(jnp.float32)


def body(
    x_in,
    query_key_value_weight,
    qkv_bias,
    output_weight,
    feedforward_entry_matrix,
    down_weight,
    norm_gains,
    piece_starts,
    seq_lengths,
    grad_out,
):
    seqs, span, width = x_in.shape
    shards = lax.axis_size("shard")
    place = lax.axis_index("shard")
    cores = lax.axis_size("tp")
    core = lax.axis_index("tp")
    reps = lax.axis_size("rep")
    length = span * shards
    half = span // cores
    rows = seqs * span
    own_rows = seqs * half
    depth = width // shards
    group_index = QUERY_HEADS // KEY_VALUE_HEADS
    joined_width = query_key_value_weight.shape[2]
    local_groups = joined_width // ((group_index + 2) * HEAD_SIZE)
    heads_width = output_weight.shape[2]
    hidden_width = down_weight.shape[2]
    block = -(-hidden_width // (reps * LANES)) * LANES
    first_owned = lax.axis_index("rep") * block
    first_unit = jnp.minimum(first_owned, hidden_width - block)
    owned = first_unit + jnp.arange(block, dtype=jnp.int32) >= first_owned
    root = math.sqrt(HEAD_SIZE)
    inner_pos = rolled(jnp.arange(span, dtype=jnp.int32), core * half, 0)
    own_pos = place * span + inner_pos
    all_pos = jnp.concatenate(
        [lax.rem(place + step, shards) * span + inner_pos for step in range(shards)]
    )
    cosine, sine = rope_tables(own_pos)
    cos_query = cosine[None, :, None, None, :]
    sin_query = sine[None, :, None, None, :]
    cos_key = cosine[None, :, None, :]
    sin_key = sine[None, :, None, :]
    own_ids = piece_ids(jnp.broadcast_to(own_pos, (seqs, span)), piece_starts)
    all_ids = piece_ids(jnp.broadcast_to(all_pos, (seqs, length)), piece_starts)
    same_piece = (own_ids[:, :, None] == all_ids[:, None, :]) & (own_ids[:, :, None] > 0)
    seen = (all_pos[None, None, :] < seq_lengths[:, None, None]) & (
        (all_pos[None, None, :] <= own_pos[None, :, None]) | same_piece
    )

    def own_block(weight):
        part = lax.dynamic_slice_in_dim(weight, first_unit, block, axis=weight.ndim - 1)
        return lax.optimization_barrier(jnp.where(owned, part, jnp.zeros_like(part)))

    def core_gather(values, name):
        tall = ring_gather(values, "tp", name, 6).reshape(cores, seqs, half, -1)
        return jnp.moveaxis(tall, 0, 1).reshape(rows, -1)

    def core_scatter(values):
        blocks = jnp.moveaxis(values.reshape(seqs, cores, half, -1), 1, 0)
        blocks = blocks.reshape(cores, own_rows, -1)
        return ring_scatter(blocks[1:].astype(jnp.bfloat16), blocks[0], "tp", 4, 8)

    gains_all = norm_gains.astype(jnp.float32)
    x_tall = rolled(x_in, core * half, 1).astype(jnp.float32)
    residual_state = x_tall[:, :half].reshape(own_rows, width)
    x_tall = x_tall.reshape(rows, width)
    first_normed = (x_tall * norm_scale(x_tall) * gains_all[0, 0]).astype(jnp.bfloat16)
    saved = []
    entry_blocks = own_block(feedforward_entry_matrix)
    down_blocks = own_block(down_weight)
    near_rows = reps * own_rows
    both_width = joined_width + heads_width
    full_both = weight_gather(
        jnp.concatenate(
            [
                weight[index]
                for index in range(LAYERS)
                for weight in (query_key_value_weight, output_weight)
            ],
            axis=1,
        )
    )
    for index in range(LAYERS):
        start = index * both_width
        full_qkv = full_both[:, start : start + joined_width]
        full_out = full_both[:, start + joined_width : start + both_width]
        entry_block = entry_blocks[index].reshape(depth, 2 * block)
        if index:
            part = jnp.concatenate([entry_block, down_blocks[index]], axis=1)
            part = gathered(part)
            part_entry, part_down = part[:, : 2 * block], part[:, 2 * block :]
        else:
            part_entry = gathered(entry_block)
            part_down = gathered(down_blocks[index])
        gains = gains_all[index]
        scale_one = norm_scale(residual_state)
        if index:
            first_normed = core_gather(
                (residual_state * scale_one * gains[0]).astype(jnp.bfloat16), 3
            )
        joined_output = product(first_normed, full_qkv) + qkv_bias[index].astype(jnp.float32)
        joined_output = joined_output.reshape(seqs, span, local_groups, group_index + 2, HEAD_SIZE)
        query_rows = rotate(joined_output[:, :, :, :group_index], cos_query, sin_query).astype(
            jnp.bfloat16
        )
        keys = rotate(joined_output[:, :, :, group_index], cos_key, sin_key).astype(jnp.bfloat16)
        content_entries = joined_output[:, :, :, group_index + 1].astype(jnp.bfloat16)
        pair = jnp.stack([keys, content_entries]).reshape(-1, HEAD_SIZE)
        pair_all = ring_gather(pair, "shard", 5, 12)
        pair_all = pair_all.reshape(shards, 2, seqs, span, local_groups, HEAD_SIZE)
        pair_all = jnp.moveaxis(pair_all, 0, 2).reshape(2, seqs, length, local_groups, HEAD_SIZE)
        keys_all, values_all = pair_all[0], pair_all[1]
        attention_logits = masked_scores(query_rows, keys_all, seen, root)
        log_total = jax.nn.logsumexp(attention_logits, axis=-1, keepdims=True)
        shares = jnp.exp(attention_logits - log_total).astype(jnp.bfloat16)
        mixed_output = jnp.einsum(
            "sgjqk,skgd->sqgjd", shares, values_all, preferred_element_type=jnp.float32
        )
        mixed_output = mixed_output.astype(jnp.bfloat16).reshape(rows, heads_width)
        middle_state = residual_state + core_scatter(right_product(mixed_output, full_out))
        scale_two = norm_scale(middle_state)
        plane_rows = plane_gather((middle_state * scale_two * gains[1]).astype(jnp.bfloat16))
        gate = product(plane_rows, part_entry[:, :block])
        upper = product(plane_rows, part_entry[:, block:])
        hidden_state = (jax.nn.silu(gate) * upper).astype(jnp.bfloat16)
        saved.append(
            (
                residual_state,
                scale_one,
                first_normed,
                query_rows,
                keys_all,
                values_all,
                log_total,
                mixed_output,
                middle_state,
                scale_two,
                plane_rows,
                gate,
                upper,
                hidden_state,
                full_qkv,
                full_out,
                part_entry,
                part_down,
            )
        )
        residual_state = middle_state + plane_scatter(
            right_product(hidden_state[near_rows:], part_down).astype(jnp.bfloat16),
            right_product(hidden_state[:near_rows], part_down),
        )
    out_own = residual_state.astype(jnp.bfloat16)
    grad_tall = rolled(grad_out, core * half, 1)[:, :half]
    flow = grad_tall.astype(jnp.float32).reshape(own_rows, width)
    up_pieces = [None] * LAYERS
    gate_pieces = [None] * LAYERS
    down_pieces = [None] * LAYERS
    qkv_pieces = [None] * LAYERS
    gain_grads = [None] * LAYERS
    bias_grads = [None] * LAYERS
    pending = None
    for index in reversed(range(LAYERS)):
        (
            residual_state,
            scale_one,
            first_normed,
            query_rows,
            keys_all,
            values_all,
            log_total,
            mixed_output,
            middle_state,
            scale_two,
            plane_rows,
            gate,
            upper,
            hidden_state,
            full_qkv,
            full_out,
            part_entry,
            part_down,
        ) = saved[index]
        gains = gains_all[index]
        plane_grad = plane_gather(flow.astype(jnp.bfloat16))
        down_total = left_product(plane_grad, hidden_state)
        plane_grad, down_total = lax.optimization_barrier((plane_grad, down_total))
        if pending is not None:
            plane_grad, part = lax.optimization_barrier((plane_grad, pending[0]))
            gate_pieces[index + 1] = from_replicas(part)
        hidden_grad = product(plane_grad, part_down)
        down_own = scattered(down_total)
        sigmoid = jax.nn.sigmoid(gate)
        gate_grad = hidden_grad * upper * (sigmoid + gate * sigmoid * (1.0 - sigmoid))
        up_grad = hidden_grad * (gate * sigmoid)
        entry_grad = jnp.concatenate([gate_grad, up_grad], axis=1).astype(jnp.bfloat16)
        gate_total = left_product(plane_rows, entry_grad[:, :block])
        up_total = left_product(plane_rows, entry_grad[:, block:])
        entry_grad, gate_total, up_total = lax.optimization_barrier(
            (entry_grad, gate_total, up_total)
        )
        if pending is not None:
            entry_grad, part = lax.optimization_barrier((entry_grad, pending[1]))
            up_pieces[index + 1] = from_replicas(part)
        own_parts = (scattered(gate_total), scattered(up_total))
        far_product = right_product(entry_grad[near_rows:], part_entry).astype(jnp.bfloat16)
        near_product = right_product(entry_grad[:near_rows], part_entry)
        normed_two_grad = plane_scatter(far_product, near_product)
        middle_grad, gain_two = norm_back(middle_state, scale_two, gains[1], normed_two_grad)
        middle_grad = flow + middle_grad
        out_grad = core_gather(middle_grad.astype(jnp.bfloat16), 3)
        mixed_grad = product(out_grad, full_out).astype(jnp.bfloat16)
        if pending is not None:
            mixed_grad, wide = lax.optimization_barrier((mixed_grad, pending[2]))
            qkv_pieces[index + 1] = from_replicas(wide)
        pending = own_parts
        mixed_grad = mixed_grad.reshape(seqs, span, local_groups, group_index, HEAD_SIZE)
        attention_logits = masked_scores(query_rows, keys_all, seen, root)
        exact = jnp.exp(attention_logits - log_total)
        shares = exact.astype(jnp.bfloat16)
        share_grad = jnp.einsum(
            "sqgjd,skgd->sgjqk", mixed_grad, values_all, preferred_element_type=jnp.float32
        )
        centre = jnp.sum(exact * share_grad, axis=-1, keepdims=True)
        score_grad = (exact * (share_grad - centre)).astype(jnp.bfloat16)
        query_grad = (
            jnp.einsum(
                "sgjqk,skgd->sqgjd", score_grad, keys_all, preferred_element_type=jnp.float32
            )
            / root
        )
        key_grad = (
            jnp.einsum(
                "sgjqk,sqgjd->skgd", score_grad, query_rows, preferred_element_type=jnp.float32
            )
            / root
        )
        value_grad = jnp.einsum(
            "sgjqk,sqgjd->skgd", shares, mixed_grad, preferred_element_type=jnp.float32
        )
        pair = jnp.stack([key_grad, value_grad])
        pair = pair.reshape(2, seqs, shards, span, local_groups, HEAD_SIZE)
        pair = jnp.moveaxis(pair, 2, 0).reshape(shards, -1, HEAD_SIZE)
        pair_own = ring_scatter(pair[1:].astype(jnp.bfloat16), pair[0], "shard", 6, 14)
        pair_own, down_own = lax.optimization_barrier((pair_own, down_own))
        down_pieces[index] = from_replicas(down_own)
        pair_own = pair_own.reshape(2, seqs, span, local_groups, HEAD_SIZE)
        key_own, value_own = pair_own[0], pair_own[1]
        unrotated_asks = rotate_back(query_grad, cos_query, sin_query)
        key_raw = rotate_back(key_own, cos_key, sin_key)
        joined_grad = jnp.concatenate(
            [unrotated_asks, key_raw[:, :, :, None], value_own[:, :, :, None]], axis=3
        )
        joined_grad = joined_grad.reshape(rows, joined_width).astype(jnp.bfloat16)
        bias_grads[index] = jnp.sum(joined_grad, axis=0, dtype=jnp.float32)
        normed_one_grad = core_scatter(right_product(joined_grad, full_qkv))
        input_grad, gain_one = norm_back(residual_state, scale_one, gains[0], normed_one_grad)
        gain_grads[index] = jnp.stack([gain_one, gain_two])
        flow = middle_grad + input_grad
        both = jnp.concatenate(
            [left_product(first_normed, joined_grad), left_product(out_grad, mixed_output)], axis=1
        )
        if index:
            wide = both.reshape(shards, reps, depth // reps, both_width).swapaxes(0, 1)
            wide = scattered(wide.reshape(shards * depth, both_width), "rep")
            pending = (*pending, scattered(wide))
        else:
            both_sum, *pending = lax.optimization_barrier((gradient_sum(both), *pending))
    both_sum, *late = lax.optimization_barrier(
        (both_sum, gate_pieces[1:], up_pieces[1:], down_pieces[1:], qkv_pieces[1:])
    )
    gate_pieces[1:], up_pieces[1:], down_pieces[1:], qkv_pieces[1:] = late
    gate_pieces[0], up_pieces[0] = [from_replicas(part) for part in pending]
    gate_pieces, up_pieces, down_pieces = [
        [in_order(blocks) for blocks in pieces]
        for pieces in (gate_pieces, up_pieces, down_pieces)
    ]
    qkv_pieces[1:] = [
        jnp.concatenate(in_order(blocks), axis=0).astype(jnp.float32) for blocks in qkv_pieces[1:]
    ]
    grad_gate_up = []
    for gates, ups in zip(gate_pieces, up_pieces):
        pairs = [
            lax.optimization_barrier(jnp.concatenate(pair, axis=1)).reshape(depth, 2, block)
            for pair in zip(gates, ups)
        ]
        grad_gate_up.append(join_blocks(pairs, hidden_width))
    grad_gate_up = jnp.stack(grad_gate_up)
    grad_down = jnp.stack([join_blocks(blocks, hidden_width) for blocks in down_pieces])
    bias = jnp.stack(bias_grads)
    slots = jnp.arange(cores, dtype=jnp.int32)[:, None, None] == core
    bias_slots = jnp.where(slots, bias[None], 0.0)
    gains_own = jnp.stack(gain_grads)
    small = jnp.concatenate([gains_own.reshape(-1), bias_slots.reshape(-1)])
    small, both_sum = lax.optimization_barrier((small, both_sum))
    qkv_pieces[0] = both_sum.astype(jnp.float32)
    small = sum_everywhere(small.reshape(-1, LANES), ("rep", "shard", "tp"), 7).reshape(-1)
    grad_both = jnp.stack(qkv_pieces)
    grad_qkv = grad_both[:, :, :joined_width]
    grad_out_proj = grad_both[:, :, joined_width:]
    gains_total = small[: gains_own.size].reshape(gains_own.shape)
    bias_slots = small[gains_own.size :].reshape(bias_slots.shape)
    bias_total = lax.dynamic_index_in_dim(bias_slots, core, 0, keepdims=False)

    def whole_rows(values, name):
        tall = core_gather(values, name).reshape(seqs, span, width)
        return rolled(tall, lax.rem(cores - core, cores) * half, 1)

    return (
        whole_rows(out_own, 3),
        whole_rows(flow, 8),
        grad_qkv,
        bias_total,
        grad_out_proj,
        grad_gate_up,
        grad_down,
        gains_total,
    )


def solution(mesh):
    return jax.shard_map(
        body,
        mesh=mesh,
        in_specs=(
            P("rep", "shard", None),
            P(None, "shard", "tp"),
            P(None, "tp"),
            P(None, "shard", "tp"),
            P(None, "shard", None, "tp"),
            P(None, "shard", "tp"),
            P(),
            P("rep", None),
            P("rep"),
            P("rep", "shard", None),
        ),
        out_specs=(
            P("rep", "shard", None),
            P("rep", "shard", None),
            P(None, "shard", "tp"),
            P(None, "tp"),
            P(None, "shard", "tp"),
            P(None, "shard", None, "tp"),
            P(None, "shard", "tp"),
            P(),
        ),
        check_vma=False,
    )
```

```python
import functools
import math

import jax
import jax.numpy as jnp
from jax import lax
from jax.experimental import pallas as pl
from jax.experimental.pallas import tpu as pltpu
from jax.sharding import PartitionSpec as P


QUERY_HEADS = 12
KEY_VALUE_HEADS = 2
HEAD_SIZE = 128
LAYERS = 2
PIECE = 256
PIECES = 2
LANES = 128


EPS = 1e-06
THETA = 1000000.0


def rope_tables(positions):
    freq = jnp.exp(
        jnp.arange(HEAD_SIZE // 2, dtype=jnp.float32) * (-2.0 * math.log(THETA) / HEAD_SIZE)
    )
    angle = positions.astype(jnp.float32)[:, None] * freq[None, :]
    angle = jnp.concatenate([angle, angle], axis=1)
    return (jnp.cos(angle), jnp.sin(angle))


def rotate(content_entries, cosine, sine):
    half = content_entries.shape[-1] // 2
    turned = jnp.concatenate([-content_entries[..., half:], content_entries[..., :half]], axis=-1)
    return content_entries * cosine + turned * sine


def rotate_back(grads, cosine, sine):
    half = grads.shape[-1] // 2
    shifted = grads * sine
    return grads * cosine + jnp.concatenate([shifted[..., half:], -shifted[..., :half]], axis=-1)


def piece_ids(positions, starts):
    inside = (positions[..., :, None] >= starts[..., None, :]) & (
        positions[..., :, None] < starts[..., None, :] + PIECE
    )
    labels = jnp.arange(1, PIECES + 1, dtype=jnp.int32)
    return jnp.sum(jnp.where(inside, labels, 0), axis=-1)


def norm_scale(content_entries):
    return lax.rsqrt(jnp.mean(content_entries * content_entries, axis=-1, keepdims=True) + EPS)


def norm_back(content_entries, scale, gain, grad_normed):
    inner = jnp.mean(grad_normed * gain * content_entries, axis=-1, keepdims=True)
    grad_values = scale * gain * grad_normed - content_entries * (scale * scale * scale) * inner
    gain_grad = jnp.sum(grad_normed * content_entries * scale, axis=0)
    return (grad_values, gain_grad)


def masked_scores(query_rows, keys_all, seen, root):
    raw = (
        jnp.einsum("sqgjd,skgd->sgjqk", query_rows, keys_all, preferred_element_type=jnp.float32)
        / root
    )
    return jnp.where(seen[:, None, None], raw, -1e30)


MESH = pl.DeviceIdType.MESH
FAST_BYTES_PER_US = 3_000_000


def left_product(left, right):
    return lax.dot_general(
        left, right, (((0,), (0,)), ((), ())), preferred_element_type=jnp.float32
    ).astype(jnp.bfloat16)


def right_product(left, right):
    return lax.dot_general(
        left, right, (((1,), (1,)), ((), ())), preferred_element_type=jnp.float32
    )


def product(left, right):
    return jnp.dot(left, right, preferred_element_type=jnp.float32)


def next_on(axis, step):
    return {axis: lax.rem(lax.axis_index(axis) + step, lax.axis_size(axis))}


def greet(sizes):
    barrier = pltpu.get_barrier_semaphore()
    for axis, count in sizes:
        for step in range(1, count):
            pl.semaphore_signal(
                barrier, inc=1, device_id=next_on(axis, step), device_id_type=MESH
            )
    pl.semaphore_wait(barrier, sum(count - 1 for _, count in sizes))


def greet_devices(devices):
    barrier = pltpu.get_barrier_semaphore()
    for device in devices:
        pl.semaphore_signal(barrier, inc=1, device_id=device, device_id_type=MESH)
    pl.semaphore_wait(barrier, len(devices))


def square_peers():
    me = lax.axis_index("rep")
    return me, me + 1 - 2 * lax.rem(me, 2), lax.rem(me + 2, 4)


def slot_of(peer, me):
    return lax.rem(peer - me + 4, 4)


def start_copy(source, target, sent, received, device):
    copy = pltpu.make_async_remote_copy(
        src_ref=source,
        dst_ref=target,
        send_sem=sent,
        recv_sem=received,
        device_id=device,
        device_id_type=MESH,
    )
    copy.start()
    return copy


def by_rows(rows, update, base=0):
    size = next((size for size in (32, 16) if rows % size == 0), rows)

    def step(index, carry):
        update(pl.ds(pl.multiple_of(base + index * size, 16), size))
        return carry

    lax.fori_loop(0, rows // size, step, 0)


def call_kernel(kernel, name, out_shape, scratch, operands, micros):
    return pl.pallas_call(
        kernel,
        out_shape=out_shape,
        in_specs=[pl.BlockSpec(memory_space=pltpu.VMEM)] * len(operands),
        out_specs=pl.BlockSpec(memory_space=pltpu.VMEM),
        scratch_shapes=scratch,
        compiler_params=pltpu.CompilerParams(
            collective_id=name, has_side_effects=True, vmem_limit_bytes=40 * 1024 * 1024
        ),
        cost_estimate=pl.CostEstimate(
            flops=0, bytes_accessed=int(micros * FAST_BYTES_PER_US), transcendentals=0
        ),
    )(*operands)


def ring_gather_kernel(axis, count, x_ref, out_ref, sent, received):
    greet(((axis, count),))
    copies = [
        start_copy(
            x_ref,
            out_ref.at[count - step],
            sent.at[step],
            received.at[count - step],
            next_on(axis, step),
        )
        for step in range(1, count)
    ]
    out_ref[0] = x_ref[...]
    for copy in copies:
        copy.wait()


def ring_gather(values, axis, name, micros):
    count = lax.axis_size(axis)
    if count == 1:
        return values[None]
    return call_kernel(
        functools.partial(ring_gather_kernel, axis, count),
        name,
        jax.ShapeDtypeStruct((count, *values.shape), values.dtype),
        [pltpu.SemaphoreType.DMA((count,)), pltpu.SemaphoreType.DMA((count,))],
        (values,),
        micros,
    )


def ring_scatter_kernel(axis, count, far_ref, near_ref, out_ref, arrived, sent, received):
    greet(((axis, count),))
    copies = [
        start_copy(
            far_ref.at[step - 1],
            arrived.at[step - 1],
            sent.at[step],
            received.at[step],
            next_on(axis, step),
        )
        for step in range(1, count)
    ]
    for copy in copies:
        copy.wait()

    def add(some):
        total = near_ref[some, :]
        for step in range(1, count):
            total = total + arrived[step - 1, some, :].astype(jnp.float32)
        out_ref[some, :] = total

    by_rows(near_ref.shape[0], add)


def ring_scatter(far, near, axis, name, micros):
    count = lax.axis_size(axis)
    if count == 1:
        return near
    return call_kernel(
        functools.partial(ring_scatter_kernel, axis, count),
        name,
        jax.ShapeDtypeStruct(near.shape, jnp.float32),
        [
            pltpu.VMEM(far.shape, far.dtype),
            pltpu.SemaphoreType.DMA((count,)),
            pltpu.SemaphoreType.DMA((count,)),
        ],
        (far, near),
        micros,
    )


def plane_gather_kernel(reps, cores, x_ref, out_ref, sent, received, sent_on, received_on):
    greet((("rep", reps), ("tp", cores)))
    copies = [
        start_copy(
            x_ref,
            out_ref.at[0, reps - step],
            sent.at[step],
            received.at[reps - step],
            next_on("rep", step),
        )
        for step in range(1, reps)
    ]
    passed = []

    def pass_on(source, slot):
        for step in range(1, cores):
            passed.append(
                start_copy(
                    source,
                    out_ref.at[cores - step, slot],
                    sent_on.at[step, slot],
                    received_on.at[cores - step, slot],
                    next_on("tp", step),
                )
            )

    pass_on(x_ref, 0)
    out_ref[0, 0] = x_ref[...]
    for copy, step in zip(copies, range(1, reps)):
        copy.wait_recv()
        pass_on(out_ref.at[0, reps - step], reps - step)
    for copy in copies:
        copy.wait_send()
    for copy in passed:
        copy.wait()


def square_gather_kernel(cores, x_ref, out_ref, sent, received, sent_on, received_on):
    me, beside, above = square_peers()
    ways = {"beside": {"rep": beside}, "above": {"rep": above}}
    greet_devices(list(ways.values()) + [next_on("tp", step) for step in range(1, cores)])
    half = x_ref.shape[0] // 2
    low, high = pl.ds(0, half), pl.ds(half, half)
    by_side = start_copy(
        x_ref, out_ref.at[0, slot_of(me, beside)], sent.at[0], received.at[0], ways["beside"]
    )
    by_top = start_copy(
        x_ref, out_ref.at[0, slot_of(me, above)], sent.at[1], received.at[1], ways["above"]
    )
    passed = []

    def pass_on(source, slot, role):
        for step in range(1, cores):
            passed.append(
                start_copy(
                    source,
                    out_ref.at[cores - step, slot],
                    sent_on.at[step, role],
                    received_on.at[cores - step, role],
                    next_on("tp", step),
                )
            )

    pass_on(x_ref, 0, 0)
    out_ref[0, 0] = x_ref[...]
    side_slot, top_slot = slot_of(beside, me), slot_of(above, me)
    by_side.wait_recv()
    upward = start_copy(
        out_ref.at[0, side_slot, low],
        out_ref.at[0, slot_of(beside, above), low],
        sent.at[2],
        received.at[2],
        ways["above"],
    )
    pass_on(out_ref.at[0, side_slot], side_slot, 1)
    by_top.wait_recv()
    sideward = start_copy(
        out_ref.at[0, top_slot, high],
        out_ref.at[0, slot_of(above, beside), high],
        sent.at[3],
        received.at[3],
        ways["beside"],
    )
    pass_on(out_ref.at[0, top_slot], top_slot, 2)
    upward.wait_recv()
    sideward.wait_recv()
    far_slot = 4 - side_slot
    pass_on(out_ref.at[0, far_slot], far_slot, 3)
    for copy in (by_side, by_top, upward, sideward):
        copy.wait_send()
    for copy in passed:
        copy.wait()


def in_square(reps, rows):
    return reps == 4 and rows % 32 == 0


def plane_gather(rows):
    reps, cores = lax.axis_size("rep"), lax.axis_size("tp")
    gathered = call_kernel(
        (
            functools.partial(square_gather_kernel, cores)
            if in_square(reps, rows.shape[0])
            else functools.partial(plane_gather_kernel, reps, cores)
        ),
        1,
        jax.ShapeDtypeStruct((cores, reps, *rows.shape), rows.dtype),
        [
            pltpu.SemaphoreType.DMA((reps,)),
            pltpu.SemaphoreType.DMA((reps,)),
            pltpu.SemaphoreType.DMA((cores, reps)),
            pltpu.SemaphoreType.DMA((cores, reps)),
        ],
        (rows,),
        30,
    )
    return gathered.reshape(cores * reps * rows.shape[0], rows.shape[1])


def plane_scatter_kernel(
    reps,
    cores,
    far_ref,
    near_ref,
    out_ref,
    arrived,
    staged,
    landed,
    sent,
    received,
    sent_on,
    received_on,
):
    greet((("rep", reps), ("tp", cores)))
    rows = near_ref.shape[1]
    order = list(range(1, reps)) + [0]
    first = {}
    for slot in order:
        for step in range(1, cores):
            first[step, slot] = start_copy(
                far_ref.at[step - 1, slot],
                arrived.at[step - 1, slot],
                sent.at[step, slot],
                received.at[step, slot],
                next_on("tp", step),
            )

    def near_sum(slot, some):
        total = near_ref[slot, some, :]
        for step in range(1, cores):
            total = total + arrived[step - 1, slot, some, :].astype(jnp.float32)
        return total

    second = []
    for slot in order:
        for step in range(1, cores):
            first[step, slot].wait_recv()
        if slot:

            def stage(some, slot=slot):
                staged[slot - 1, some, :] = near_sum(slot, some).astype(jnp.bfloat16)

            by_rows(rows, stage)
            second.append(
                start_copy(
                    staged.at[slot - 1],
                    landed.at[slot - 1],
                    sent_on.at[slot],
                    received_on.at[slot],
                    next_on("rep", slot),
                )
            )
    for copy in first.values():
        copy.wait_send()
    for copy in second:
        copy.wait()

    def finish(some):
        total = near_sum(0, some)
        for slot in range(1, reps):
            total = total + landed[slot - 1, some, :].astype(jnp.float32)
        out_ref[some, :] = total

    by_rows(rows, finish)


def square_scatter_kernel(
    cores,
    far_ref,
    near_ref,
    out_ref,
    arrived,
    staged,
    landed,
    crossed,
    sent,
    received,
    sent_on,
    received_on,
):
    me, beside, above = square_peers()
    ways = {"beside": {"rep": beside}, "above": {"rep": above}}
    greet_devices(list(ways.values()) + [next_on("tp", step) for step in range(1, cores)])
    half = near_ref.shape[1] // 2
    low, high = pl.ds(0, half), pl.ds(half, half)
    side_slot, top_slot = slot_of(beside, me), slot_of(above, me)
    slots = (4 - side_slot, side_slot, top_slot, 0)
    first = {}
    for role, slot in enumerate(slots):
        for step in range(1, cores):
            first[role, step] = start_copy(
                far_ref.at[step - 1, slot],
                arrived.at[step - 1, role],
                sent.at[step, role],
                received.at[step, role],
                next_on("tp", step),
            )

    def near_sum(role, some):
        total = near_ref[slots[role], some, :]
        for step in range(1, cores):
            total = total + arrived[step - 1, role, some, :].astype(jnp.float32)
        return total

    def await_role(role):
        for step in range(1, cores):
            first[role, step].wait_recv()

    def stage(role, base, extra=None):
        def fill(some):
            total = near_sum(role, some)
            if extra is not None:
                inner = pl.ds(some.start - base, some.size)
                total = total + crossed[extra, inner, :].astype(jnp.float32)
            staged[role, some, :] = total.astype(jnp.bfloat16)

        by_rows(half, fill, base)

    def send(role, rows, target, index, way):
        return start_copy(
            staged.at[role, rows], target, sent_on.at[index], received_on.at[index], ways[way]
        )

    await_role(0)
    stage(0, 0)
    corner_low = send(0, low, crossed.at[0], 0, "beside")
    stage(0, half)
    corner_high = send(0, high, crossed.at[1], 1, "above")
    await_role(1)
    stage(1, 0)
    side_low = send(1, low, landed.at[0, low], 2, "beside")
    await_role(2)
    stage(2, half)
    top_high = send(2, high, landed.at[1, high], 3, "above")
    corner_low.wait_recv()
    stage(2, 0, 0)
    top_low = send(2, low, landed.at[1, low], 4, "above")
    corner_high.wait_recv()
    stage(1, half, 1)
    side_high = send(1, high, landed.at[0, high], 5, "beside")
    await_role(3)
    for copy in (side_low, top_high, top_low, side_high):
        copy.wait_recv()

    def finish(some):
        total = near_sum(3, some)
        for way in range(2):
            total = total + landed[way, some, :].astype(jnp.float32)
        out_ref[some, :] = total

    by_rows(near_ref.shape[1], finish)
    for copy in (corner_low, corner_high, side_low, top_high, top_low, side_high):
        copy.wait_send()
    for copy in first.values():
        copy.wait_send()


def plane_scatter(far, near):
    reps, cores = lax.axis_size("rep"), lax.axis_size("tp")
    rows = near.shape[0] // reps
    far = far.reshape(cores - 1, reps, rows, far.shape[1])
    near = near.reshape(reps, rows, near.shape[1])
    if in_square(reps, rows):
        return call_kernel(
            functools.partial(square_scatter_kernel, cores),
            2,
            jax.ShapeDtypeStruct(near.shape[1:], jnp.float32),
            [
                pltpu.VMEM(far.shape, jnp.bfloat16),
                pltpu.VMEM((3, *near.shape[1:]), jnp.bfloat16),
                pltpu.VMEM((2, *near.shape[1:]), jnp.bfloat16),
                pltpu.VMEM((2, rows // 2, near.shape[2]), jnp.bfloat16),
                pltpu.SemaphoreType.DMA((cores, 4)),
                pltpu.SemaphoreType.DMA((cores, 4)),
                pltpu.SemaphoreType.DMA((6,)),
                pltpu.SemaphoreType.DMA((6,)),
            ],
            (far, near),
            28,
        )
    return call_kernel(
        functools.partial(plane_scatter_kernel, reps, cores),
        2,
        jax.ShapeDtypeStruct(near.shape[1:], jnp.float32),
        [
            pltpu.VMEM(far.shape, jnp.bfloat16),
            pltpu.VMEM((reps - 1, *near.shape[1:]), jnp.bfloat16),
            pltpu.VMEM((reps - 1, *near.shape[1:]), jnp.bfloat16),
            pltpu.SemaphoreType.DMA((cores, reps)),
            pltpu.SemaphoreType.DMA((cores, reps)),
            pltpu.SemaphoreType.DMA((reps,)),
            pltpu.SemaphoreType.DMA((reps,)),
        ],
        (far, near),
        35,
    )


def weight_gather_kernel(
    shards, reps, w_ref, out_ref, sent, received, sent_on, received_on
):
    greet((("shard", shards), ("rep", reps)))
    place = lax.axis_index("shard")
    replica = lax.axis_index("rep")
    copies = [
        start_copy(
            w_ref.at[replica],
            out_ref.at[place, replica],
            sent.at[step],
            received.at[step],
            next_on("shard", step),
        )
        for step in range(1, shards)
    ]
    out_ref[place] = w_ref[...]
    passed = []
    for step in range(1, shards):
        copies[step - 1].wait_recv()
        source = out_ref.at[lax.rem(place + shards - step, shards), replica]
        for far in range(1, reps):
            passed.append(
                start_copy(
                    source,
                    source,
                    sent_on.at[step, far],
                    received_on.at[step, far],
                    next_on("rep", far),
                )
            )
    for copy in copies:
        copy.wait_send()
    for copy in passed:
        copy.wait()


def weight_gather(weight):
    shards, reps = lax.axis_size("shard"), lax.axis_size("rep")
    depth, columns = weight.shape
    parts = weight.reshape(reps, depth // reps, columns)
    gathered = call_kernel(
        functools.partial(weight_gather_kernel, shards, reps),
        9,
        jax.ShapeDtypeStruct((shards, *parts.shape), weight.dtype),
        [
            pltpu.SemaphoreType.DMA((shards,)),
            pltpu.SemaphoreType.DMA((shards,)),
            pltpu.SemaphoreType.DMA((shards, reps)),
            pltpu.SemaphoreType.DMA((shards, reps)),
        ],
        (parts,),
        50,
    )
    return gathered.reshape(shards * depth, columns)


def gradient_sum_kernel(
    shards,
    reps,
    grad_ref,
    out_ref,
    arrived,
    staged,
    landed,
    summed,
    sent,
    received,
    sent_far,
    received_far,
    sent_on,
    received_on,
):
    greet((("shard", shards), ("rep", reps)))
    place = lax.axis_index("shard")
    replica = lax.axis_index("rep")
    rows = grad_ref.shape[2]
    order = list(range(1, shards)) + [0]
    first = {}
    for step in order:
        target = lax.rem(place + step, shards)
        for far in range(1, reps):
            first[step, far] = start_copy(
                grad_ref.at[target, lax.rem(replica + far, reps)],
                arrived.at[far - 1, step],
                sent.at[step, far],
                received.at[step, far],
                next_on("rep", far),
            )

    def replica_sum(step, some):
        target = lax.rem(place + step, shards)
        total = grad_ref[target, replica, some, :].astype(jnp.float32)
        for far in range(1, reps):
            total = total + arrived[far - 1, step, some, :].astype(jnp.float32)
        return total

    second = []
    for step in order:
        for far in range(1, reps):
            first[step, far].wait_recv()
        if step:

            def stage(some, step=step):
                staged[step - 1, some, :] = replica_sum(step, some).astype(jnp.bfloat16)

            by_rows(rows, stage)
            second.append(
                start_copy(
                    staged.at[step - 1],
                    landed.at[step - 1],
                    sent_far.at[step],
                    received_far.at[step],
                    next_on("shard", step),
                )
            )
    for copy in second:
        copy.wait()

    def finish(some):
        total = replica_sum(0, some)
        for step in range(1, shards):
            total = total + landed[step - 1, some, :].astype(jnp.float32)
        summed[some, :] = total.astype(jnp.bfloat16)

    by_rows(rows, finish)
    third = [
        start_copy(
            summed,
            out_ref.at[replica],
            sent_on.at[far],
            received_on.at[far],
            next_on("rep", far),
        )
        for far in range(1, reps)
    ]
    out_ref[replica] = summed[...]
    for copy in first.values():
        copy.wait_send()
    for copy in third:
        copy.wait()


def gradient_sum(grad):
    shards, reps = lax.axis_size("shard"), lax.axis_size("rep")
    columns = grad.shape[1]
    depth = grad.shape[0] // shards
    piece = (depth // reps, columns)
    summed = call_kernel(
        functools.partial(gradient_sum_kernel, shards, reps),
        10,
        jax.ShapeDtypeStruct((reps, *piece), grad.dtype),
        [
            pltpu.VMEM((reps - 1, shards, *piece), grad.dtype),
            pltpu.VMEM((shards - 1, *piece), grad.dtype),
            pltpu.VMEM((shards - 1, *piece), grad.dtype),
            pltpu.VMEM(piece, grad.dtype),
            pltpu.SemaphoreType.DMA((shards, reps)),
            pltpu.SemaphoreType.DMA((shards, reps)),
            pltpu.SemaphoreType.DMA((shards,)),
            pltpu.SemaphoreType.DMA((shards,)),
            pltpu.SemaphoreType.DMA((reps,)),
            pltpu.SemaphoreType.DMA((reps,)),
        ],
        (grad.reshape(shards, reps, *piece),),
        90,
    )
    return summed.reshape(depth, columns)


def sum_kernel(sizes, x_ref, out_ref, *scratch):
    greet(sizes)
    held = x_ref
    for place, (axis, count) in enumerate(sizes):
        total_ref, arrived, sent, received = scratch[4 * place : 4 * place + 4]
        copies = [
            start_copy(
                held, arrived.at[step - 1], sent.at[step], received.at[step], next_on(axis, step)
            )
            for step in range(1, count)
        ]
        for copy in copies:
            copy.wait()
        total = held[...]
        for step in range(1, count):
            total = total + arrived[step - 1]
        total_ref[...] = total
        held = total_ref
    out_ref[...] = held[...]


def sum_everywhere(values, axes, name):
    sizes = tuple((axis, lax.axis_size(axis)) for axis in axes)
    scratch = []
    for _, count in sizes:
        scratch.extend(
            [
                pltpu.VMEM(values.shape, jnp.float32),
                pltpu.VMEM((max(count - 1, 1), *values.shape), jnp.float32),
                pltpu.SemaphoreType.DMA((count,)),
                pltpu.SemaphoreType.DMA((count,)),
            ]
        )
    return call_kernel(
        functools.partial(sum_kernel, sizes),
        name,
        jax.ShapeDtypeStruct(values.shape, jnp.float32),
        scratch,
        (values,),
        8,
    )


def peer_pairs(count, step):
    if count & (count - 1) == 0:
        return [(i, i ^ step) for i in range(count)]
    return [((i + step) % count, i) for i in range(count)]


def from_replicas(part):
    count = lax.axis_size("rep")
    return [part] + [
        lax.ppermute(part, "rep", peer_pairs(count, step)) for step in range(1, count)
    ]


def in_order(blocks):
    count = lax.axis_size("rep")
    me = lax.axis_index("rep")
    held = jnp.stack(blocks)
    places = []
    for index in range(count):
        if count & (count - 1) == 0:
            slot = lax.bitwise_xor(jnp.int32(index), me)
        else:
            slot = lax.rem(index - me + count, count)
        places.append(lax.dynamic_index_in_dim(held, slot, 0, keepdims=False))
    return places


def rolled(values, shift, dim):
    extent = values.shape[dim]
    return lax.dynamic_slice_in_dim(
        jnp.concatenate([values, values], axis=dim), shift, extent, axis=dim
    )


def gathered(weight):
    return lax.all_gather(weight, "shard", axis=0, tiled=True)


def scattered(grad, axes="shard"):
    return lax.psum_scatter(grad, axes, scatter_dimension=0, tiled=True)


def join_blocks(blocks, width):
    block = blocks[0].shape[-1]
    parts = []
    for index, part in enumerate(blocks):
        skip = max(index * block - (width - block), 0)
        if skip < block:
            parts.append(part[..., skip:])
    return jnp.concatenate(parts, axis=-1).astype(jnp.float32)


def body(
    x_in,
    query_key_value_weight,
    qkv_bias,
    output_weight,
    feedforward_entry_matrix,
    down_weight,
    norm_gains,
    piece_starts,
    seq_lengths,
    grad_out,
):
    seqs, span, width = x_in.shape
    shards = lax.axis_size("shard")
    place = lax.axis_index("shard")
    cores = lax.axis_size("tp")
    core = lax.axis_index("tp")
    reps = lax.axis_size("rep")
    length = span * shards
    half = span // cores
    rows = seqs * span
    own_rows = seqs * half
    depth = width // shards
    group_index = QUERY_HEADS // KEY_VALUE_HEADS
    joined_width = query_key_value_weight.shape[2]
    local_groups = joined_width // ((group_index + 2) * HEAD_SIZE)
    heads_width = output_weight.shape[2]
    hidden_width = down_weight.shape[2]
    block = -(-hidden_width // (reps * LANES)) * LANES
    first_owned = lax.axis_index("rep") * block
    first_unit = jnp.minimum(first_owned, hidden_width - block)
    owned = first_unit + jnp.arange(block, dtype=jnp.int32) >= first_owned
    root = math.sqrt(HEAD_SIZE)
    inner_pos = rolled(jnp.arange(span, dtype=jnp.int32), core * half, 0)
    own_pos = place * span + inner_pos
    all_pos = jnp.concatenate(
        [lax.rem(place + step, shards) * span + inner_pos for step in range(shards)]
    )
    cosine, sine = rope_tables(own_pos)
    cos_query = cosine[None, :, None, None, :]
    sin_query = sine[None, :, None, None, :]
    cos_key = cosine[None, :, None, :]
    sin_key = sine[None, :, None, :]
    own_ids = piece_ids(jnp.broadcast_to(own_pos, (seqs, span)), piece_starts)
    all_ids = piece_ids(jnp.broadcast_to(all_pos, (seqs, length)), piece_starts)
    same_piece = (own_ids[:, :, None] == all_ids[:, None, :]) & (own_ids[:, :, None] > 0)
    seen = (all_pos[None, None, :] < seq_lengths[:, None, None]) & (
        (all_pos[None, None, :] <= own_pos[None, :, None]) | same_piece
    )

    def own_block(weight):
        part = lax.dynamic_slice_in_dim(weight, first_unit, block, axis=weight.ndim - 1)
        return lax.optimization_barrier(jnp.where(owned, part, jnp.zeros_like(part)))

    def core_gather(values, name):
        tall = ring_gather(values, "tp", name, 6).reshape(cores, seqs, half, -1)
        return jnp.moveaxis(tall, 0, 1).reshape(rows, -1)

    def core_scatter(values):
        blocks = jnp.moveaxis(values.reshape(seqs, cores, half, -1), 1, 0)
        blocks = blocks.reshape(cores, own_rows, -1)
        return ring_scatter(blocks[1:].astype(jnp.bfloat16), blocks[0], "tp", 4, 8)

    gains_all = norm_gains.astype(jnp.float32)
    x_tall = rolled(x_in, core * half, 1).astype(jnp.float32)
    residual_state = x_tall[:, :half].reshape(own_rows, width)
    x_tall = x_tall.reshape(rows, width)
    first_normed = (x_tall * norm_scale(x_tall) * gains_all[0, 0]).astype(jnp.bfloat16)
    saved = []
    entry_blocks = own_block(feedforward_entry_matrix)
    down_blocks = own_block(down_weight)
    near_rows = reps * own_rows
    both_width = joined_width + heads_width
    full_both = weight_gather(
        jnp.concatenate(
            [
                weight[index]
                for index in range(LAYERS)
                for weight in (query_key_value_weight, output_weight)
            ],
            axis=1,
        )
    )
    for index in range(LAYERS):
        start = index * both_width
        full_qkv = full_both[:, start : start + joined_width]
        full_out = full_both[:, start + joined_width : start + both_width]
        entry_block = entry_blocks[index].reshape(depth, 2 * block)
        if index:
            part = jnp.concatenate([entry_block, down_blocks[index]], axis=1)
            part = gathered(part)
            part_entry, part_down = part[:, : 2 * block], part[:, 2 * block :]
        else:
            part_entry = gathered(entry_block)
            part_down = gathered(down_blocks[index])
        gains = gains_all[index]
        scale_one = norm_scale(residual_state)
        if index:
            first_normed = core_gather(
                (residual_state * scale_one * gains[0]).astype(jnp.bfloat16), 3
            )
        joined_output = product(first_normed, full_qkv) + qkv_bias[index].astype(jnp.float32)
        joined_output = joined_output.reshape(seqs, span, local_groups, group_index + 2, HEAD_SIZE)
        query_rows = rotate(joined_output[:, :, :, :group_index], cos_query, sin_query).astype(
            jnp.bfloat16
        )
        keys = rotate(joined_output[:, :, :, group_index], cos_key, sin_key).astype(jnp.bfloat16)
        content_entries = joined_output[:, :, :, group_index + 1].astype(jnp.bfloat16)
        pair = jnp.stack([keys, content_entries]).reshape(-1, HEAD_SIZE)
        pair_all = ring_gather(pair, "shard", 5, 12)
        pair_all = pair_all.reshape(shards, 2, seqs, span, local_groups, HEAD_SIZE)
        pair_all = jnp.moveaxis(pair_all, 0, 2).reshape(2, seqs, length, local_groups, HEAD_SIZE)
        keys_all, values_all = pair_all[0], pair_all[1]
        attention_logits = masked_scores(query_rows, keys_all, seen, root)
        log_total = jax.nn.logsumexp(attention_logits, axis=-1, keepdims=True)
        shares = jnp.exp(attention_logits - log_total).astype(jnp.bfloat16)
        mixed_output = jnp.einsum(
            "sgjqk,skgd->sqgjd", shares, values_all, preferred_element_type=jnp.float32
        )
        mixed_output = mixed_output.astype(jnp.bfloat16).reshape(rows, heads_width)
        middle_state = residual_state + core_scatter(right_product(mixed_output, full_out))
        scale_two = norm_scale(middle_state)
        plane_rows = plane_gather((middle_state * scale_two * gains[1]).astype(jnp.bfloat16))
        gate = product(plane_rows, part_entry[:, :block])
        upper = product(plane_rows, part_entry[:, block:])
        hidden_state = (jax.nn.silu(gate) * upper).astype(jnp.bfloat16)
        saved.append(
            (
                residual_state,
                scale_one,
                first_normed,
                query_rows,
                keys_all,
                values_all,
                log_total,
                mixed_output,
                middle_state,
                scale_two,
                plane_rows,
                gate,
                upper,
                hidden_state,
                full_qkv,
                full_out,
                part_entry,
                part_down,
            )
        )
        residual_state = middle_state + plane_scatter(
            right_product(hidden_state[near_rows:], part_down).astype(jnp.bfloat16),
            right_product(hidden_state[:near_rows], part_down),
        )
    out_own = residual_state.astype(jnp.bfloat16)
    grad_tall = rolled(grad_out, core * half, 1)[:, :half]
    flow = grad_tall.astype(jnp.float32).reshape(own_rows, width)
    up_pieces = [None] * LAYERS
    gate_pieces = [None] * LAYERS
    down_pieces = [None] * LAYERS
    qkv_pieces = [None] * LAYERS
    gain_grads = [None] * LAYERS
    bias_grads = [None] * LAYERS
    pending = None
    for index in reversed(range(LAYERS)):
        (
            residual_state,
            scale_one,
            first_normed,
            query_rows,
            keys_all,
            values_all,
            log_total,
            mixed_output,
            middle_state,
            scale_two,
            plane_rows,
            gate,
            upper,
            hidden_state,
            full_qkv,
            full_out,
            part_entry,
            part_down,
        ) = saved[index]
        gains = gains_all[index]
        plane_grad = plane_gather(flow.astype(jnp.bfloat16))
        down_total = left_product(plane_grad, hidden_state)
        plane_grad, down_total = lax.optimization_barrier((plane_grad, down_total))
        if pending is not None:
            plane_grad, part = lax.optimization_barrier((plane_grad, pending[0]))
            up_pieces[index + 1] = from_replicas(part)
        hidden_grad = product(plane_grad, part_down)
        down_own = scattered(down_total)
        sigmoid = jax.nn.sigmoid(gate)
        gate_grad = hidden_grad * upper * (sigmoid + gate * sigmoid * (1.0 - sigmoid))
        up_grad = hidden_grad * (gate * sigmoid)
        entry_grad = jnp.concatenate([gate_grad, up_grad], axis=1).astype(jnp.bfloat16)
        gate_total = left_product(plane_rows, entry_grad[:, :block])
        up_total = left_product(plane_rows, entry_grad[:, block:])
        entry_grad, gate_total, up_total = lax.optimization_barrier(
            (entry_grad, gate_total, up_total)
        )
        own_parts = (scattered(gate_total), scattered(up_total))
        far_product = right_product(entry_grad[near_rows:], part_entry).astype(jnp.bfloat16)
        near_product = right_product(entry_grad[:near_rows], part_entry)
        normed_two_grad = plane_scatter(far_product, near_product)
        middle_grad, gain_two = norm_back(middle_state, scale_two, gains[1], normed_two_grad)
        middle_grad = flow + middle_grad
        out_grad = core_gather(middle_grad.astype(jnp.bfloat16), 3)
        mixed_grad = product(out_grad, full_out).astype(jnp.bfloat16)
        if pending is not None:
            mixed_grad, wide = lax.optimization_barrier((mixed_grad, pending[1]))
            qkv_pieces[index + 1] = from_replicas(wide)
        if index:
            mixed_grad, down_own = lax.optimization_barrier((mixed_grad, down_own))
            down_pieces[index] = from_replicas(down_own)
        mixed_grad = mixed_grad.reshape(seqs, span, local_groups, group_index, HEAD_SIZE)
        attention_logits = masked_scores(query_rows, keys_all, seen, root)
        exact = jnp.exp(attention_logits - log_total)
        shares = exact.astype(jnp.bfloat16)
        share_grad = jnp.einsum(
            "sqgjd,skgd->sgjqk", mixed_grad, values_all, preferred_element_type=jnp.float32
        )
        centre = jnp.sum(exact * share_grad, axis=-1, keepdims=True)
        score_grad = (exact * (share_grad - centre)).astype(jnp.bfloat16)
        query_grad = (
            jnp.einsum(
                "sgjqk,skgd->sqgjd", score_grad, keys_all, preferred_element_type=jnp.float32
            )
            / root
        )
        key_grad = (
            jnp.einsum(
                "sgjqk,sqgjd->skgd", score_grad, query_rows, preferred_element_type=jnp.float32
            )
            / root
        )
        value_grad = jnp.einsum(
            "sgjqk,sqgjd->skgd", shares, mixed_grad, preferred_element_type=jnp.float32
        )
        pair = jnp.stack([key_grad, value_grad])
        pair = pair.reshape(2, seqs, shards, span, local_groups, HEAD_SIZE)
        pair = jnp.moveaxis(pair, 2, 0).reshape(shards, -1, HEAD_SIZE)
        pair_own = ring_scatter(pair[1:].astype(jnp.bfloat16), pair[0], "shard", 6, 14)
        if index:
            pair_own, part = lax.optimization_barrier((pair_own, own_parts[0]))
            gate_pieces[index] = from_replicas(part)
            pending = own_parts[1:]
        else:
            pair_own, down_own = lax.optimization_barrier((pair_own, down_own))
            down_pieces[index] = from_replicas(down_own)
            pending = own_parts
        pair_own = pair_own.reshape(2, seqs, span, local_groups, HEAD_SIZE)
        key_own, value_own = pair_own[0], pair_own[1]
        unrotated_asks = rotate_back(query_grad, cos_query, sin_query)
        key_raw = rotate_back(key_own, cos_key, sin_key)
        joined_grad = jnp.concatenate(
            [unrotated_asks, key_raw[:, :, :, None], value_own[:, :, :, None]], axis=3
        )
        joined_grad = joined_grad.reshape(rows, joined_width).astype(jnp.bfloat16)
        bias_grads[index] = jnp.sum(joined_grad, axis=0, dtype=jnp.float32)
        normed_one_grad = core_scatter(right_product(joined_grad, full_qkv))
        input_grad, gain_one = norm_back(residual_state, scale_one, gains[0], normed_one_grad)
        gain_grads[index] = jnp.stack([gain_one, gain_two])
        flow = middle_grad + input_grad
        both = jnp.concatenate(
            [left_product(first_normed, joined_grad), left_product(out_grad, mixed_output)], axis=1
        )
        if index:
            wide = both.reshape(shards, reps, depth // reps, both_width).swapaxes(0, 1)
            wide = scattered(wide.reshape(shards * depth, both_width), "rep")
            pending = (*pending, scattered(wide))
        else:
            both_sum, *pending = lax.optimization_barrier((gradient_sum(both), *pending))
    both_sum, *late = lax.optimization_barrier(
        (both_sum, gate_pieces[1:], up_pieces[1:], down_pieces[1:], qkv_pieces[1:])
    )
    gate_pieces[1:], up_pieces[1:], down_pieces[1:], qkv_pieces[1:] = late
    bias = jnp.stack(bias_grads)
    slots = jnp.arange(cores, dtype=jnp.int32)[:, None, None] == core
    bias_slots = jnp.where(slots, bias[None], 0.0)
    gains_own = jnp.stack(gain_grads)
    small = jnp.concatenate([gains_own.reshape(-1), bias_slots.reshape(-1)])
    small, both_sum = lax.optimization_barrier((small, both_sum))
    qkv_pieces[0] = both_sum.astype(jnp.float32)
    small = sum_everywhere(small.reshape(-1, LANES), ("rep", "shard", "tp"), 7).reshape(-1)
    small, *pending = lax.optimization_barrier((small, *pending))
    gate_pieces[0], up_pieces[0] = [from_replicas(part) for part in pending]
    gate_pieces, up_pieces, down_pieces = [
        [in_order(blocks) for blocks in pieces]
        for pieces in (gate_pieces, up_pieces, down_pieces)
    ]
    qkv_pieces[1:] = [
        jnp.concatenate(in_order(blocks), axis=0).astype(jnp.float32) for blocks in qkv_pieces[1:]
    ]
    grad_gate_up = []
    for gates, ups in zip(gate_pieces, up_pieces):
        pairs = [
            lax.optimization_barrier(jnp.concatenate(pair, axis=1)).reshape(depth, 2, block)
            for pair in zip(gates, ups)
        ]
        grad_gate_up.append(join_blocks(pairs, hidden_width))
    grad_gate_up = jnp.stack(grad_gate_up)
    grad_down = jnp.stack([join_blocks(blocks, hidden_width) for blocks in down_pieces])
    grad_both = jnp.stack(qkv_pieces)
    grad_qkv = grad_both[:, :, :joined_width]
    grad_out_proj = grad_both[:, :, joined_width:]
    gains_total = small[: gains_own.size].reshape(gains_own.shape)
    bias_slots = small[gains_own.size :].reshape(bias_slots.shape)
    bias_total = lax.dynamic_index_in_dim(bias_slots, core, 0, keepdims=False)

    def whole_rows(values, name):
        tall = core_gather(values, name).reshape(seqs, span, width)
        return rolled(tall, lax.rem(cores - core, cores) * half, 1)

    return (
        whole_rows(out_own, 3),
        whole_rows(flow, 8),
        grad_qkv,
        bias_total,
        grad_out_proj,
        grad_gate_up,
        grad_down,
        gains_total,
    )


def solution(mesh):
    return jax.shard_map(
        body,
        mesh=mesh,
        in_specs=(
            P("rep", "shard", None),
            P(None, "shard", "tp"),
            P(None, "tp"),
            P(None, "shard", "tp"),
            P(None, "shard", None, "tp"),
            P(None, "shard", "tp"),
            P(),
            P("rep", None),
            P("rep"),
            P("rep", "shard", None),
        ),
        out_specs=(
            P("rep", "shard", None),
            P("rep", "shard", None),
            P(None, "shard", "tp"),
            P(None, "tp"),
            P(None, "shard", "tp"),
            P(None, "shard", None, "tp"),
            P(None, "shard", "tp"),
            P(),
        ),
        check_vma=False,
    )
```
